512 devices in a mesh: row: 32 (over y_lo, x, core), col: 8 (over z), dp: 2 (over y_hi).
Axes of the slice: x: 4, y: 8 (y_hi: 2, y_lo: 4; y = y_hi * 4 + y_lo), z: 8, core: 2. Of those that a mesh axis runs over, the one named last changes fastest.
Arguments:
- pixels: bfloat16 [2, 3, 1024, 1024], P('dp', None, 'row', 'col'), may hold values from -6 to 6
- cotangent: bfloat16 [2, 256, 256, 1024], P('dp', 'row', 'col'), may hold values from -6 to 6
- embed_weight: bfloat16 [48, 1024], replicated, may hold values from -0.875 to 0.875
- embed_bias: float32 [1024], replicated, may hold values from -4 to 4
- layer_norm_gain: float32 [1024], replicated, may hold values from 0.5 to 1.5
- qkv_weight: bfloat16 [1024, 2304], P('row', ('col', 'dp')), may hold values from -0.1875 to 0.1875
- out_weight: bfloat16 [768, 1024], P('row', ('col', 'dp')), may hold values from -0.21875 to 0.21875
- bias_table: float32 [12, 225], replicated, may hold values from -4 to 404
- rel_index: int32 [64, 64], replicated, may hold values from 0 to 224
- shifts: int32 [2, 2], P('dp'), may hold values from 1 to 7
Outputs:
- out_weight_grad: float32 [768, 1024], P('row', ('col', 'dp'))
- embed_weight_grad: float32 [48, 1024], replicated
- embed_bias_grad: float32 [1024], replicated
- norm_gain_grad: float32 [1024], replicated
- bias_table_grad: float32 [12, 225], replicated
The draws below stay inside these ranges and needn't reach their ends.
Inputs may be any that keep to these rules, and one draw needn't show every extreme that they name: `rel_index`: each entry names one of the 225 columns of bias_table.
All inputs are finite; a program needn't handle non-finite values.
Results may differ from the reference program's by a relative error of at most 0.023.
Values may be sent and summed in bfloat16 or wider, within the bound.
No kernel may reach another device: no remote copies, remote signals or barrier semaphores. Data moves between devices by JAX's collectives and lax.ppermute only.
A program may use at most 64 MiB of HBM per device.

```python
import jax
import jax.numpy as jnp
from jax import lax

D = 1024
HEADS = 12
WIN = 8
PATCH = 4
CHAN = 3
HD = 768
TABLE = 225
KDIM = 48
BATCH = 2
GRID_ROWS = 256
GRID_COLS = 256
PIX_ROWS = 1024
PIX_COLS = 1024


def draw_bias_table(key, part):
    key_base = jax.random.fold_in(key, 11)
    base_draw = jax.random.normal(key_base, (HEADS, TABLE), jnp.float32)
    return jnp.clip(base_draw, -4.0, 4.0)


def with_ends(entries, own_key, smallest, top_value):
    place = [jax.random.randint(jax.random.fold_in(own_key, axis), (), 0, length) for axis, length in enumerate(entries.shape)]
    longest = entries.shape.index(max(entries.shape))
    next_to = place[:longest] + [(place[longest] + 1) % entries.shape[longest]] + place[longest + 1:]
    return entries.at[tuple(place)].set(smallest).at[tuple(next_to)].set(top_value)


def block_levels(key, extent, shards, least, largest):
    factor_of = 1.0
    for dim, shards_of in shards:
        draws = jax.random.uniform(jax.random.fold_in(jax.random.fold_in(key, 6), dim), (shards_of,), jnp.float32, least / len(shards), largest / len(shards))
        factor_of = factor_of * jnp.repeat(jnp.exp(draws), extent[dim] // shards_of).reshape((-1,) + (1,) * (len(extent) - 1 - dim))
    return factor_of


def gaussian(own_key, dims, spread, most, pieces=(), kind=jnp.bfloat16):
    entries = spread * jax.random.normal(own_key, dims, jnp.float32)
    if pieces:
        entries = entries * block_levels(own_key, dims, pieces, -0.22, 0.18)
    return jnp.clip(entries, -most, most).astype(kind)


def setup_inputs(seed: int = 0) -> dict:
    splits = jax.random.split(jax.random.key(seed), 11)
    return {
        "pixels": gaussian(splits[0], (BATCH, CHAN, PIX_ROWS, PIX_COLS), 1.0, 6.0, ((0, 2), (2, 32), (3, 8))),
        "cotangent": gaussian(splits[1], (BATCH, GRID_ROWS, GRID_COLS, D), 1.0, 6.0, ((0, 2), (1, 32), (2, 8))),
        "embed_weight": gaussian(splits[2], (KDIM, D), KDIM ** -0.5, 0.875),
        "embed_bias": gaussian(splits[3], (D,), 1.0, 4.0, (), jnp.float32),
        "layer_norm_gain": jnp.clip(1.0 + 0.1 * jax.random.normal(splits[4], (D,), jnp.float32), 0.5, 1.5),
        "qkv_weight": gaussian(splits[5], (D, 3 * HD), D ** -0.5, 0.1875, ((0, 32), (1, 16))),
        "out_weight": gaussian(splits[6], (HD, D), HD ** -0.5, 0.21875, ((0, 32), (1, 16))),
        "bias_table": draw_bias_table(jax.random.fold_in(splits[10], 71), 0),
        "rel_index": with_ends(jax.random.randint(splits[8], (WIN * WIN, WIN * WIN), 0, TABLE), jax.random.fold_in(splits[8], 1), 0, TABLE - 1).astype(jnp.int32),
        "shifts": with_ends(jax.random.randint(splits[9], (BATCH, 2), 1, WIN), jax.random.fold_in(splits[9], 1), 1, WIN - 1).astype(jnp.int32),
    }


norm_epsilon = 1e-05

def make_patches(pixel_block):
    images, channels, pixel_rows, pixel_cols = pixel_block.shape
    grid_rows = pixel_rows // PATCH
    grid_cols = pixel_cols // PATCH
    shaped = pixel_block.reshape(images, channels, grid_rows, PATCH, grid_cols, PATCH)
    return shaped.transpose(0, 2, 4, 1, 3, 5).reshape(images, grid_rows, grid_cols, channels * PATCH * PATCH)

def window_split(block):
    rows_all, cols_all, features = block.shape
    shaped = block.reshape(rows_all // WIN, WIN, cols_all // WIN, WIN, features)
    return shaped.transpose(0, 2, 1, 3, 4).reshape(-1, WIN * WIN, features)

def window_join(windows, rows_all, cols_all):
    features = windows.shape[-1]
    shaped = windows.reshape(rows_all // WIN, cols_all // WIN, WIN, WIN, features)
    return shaped.transpose(0, 2, 1, 3, 4).reshape(rows_all, cols_all, features)

def window_grads(cell_windows, cot_windows, labels, layer_norm_gain, qkv_weight, out_weight, bias_full):
    window_count, cell_count, features = cell_windows.shape
    head_count = bias_full.shape[0]
    inner_width = out_weight.shape[0]
    head_size = inner_width // head_count
    score_scale = head_size ** (-0.5)
    flat_rows = cell_windows.reshape(-1, features).astype(jnp.float32)
    average = lax.optimization_barrier(jnp.mean(flat_rows, axis=-1, keepdims=True))
    centered_input = flat_rows - average
    inverse_deviation = lax.rsqrt(lax.optimization_barrier(jnp.mean(centered_input * centered_input, axis=-1, keepdims=True)) + norm_epsilon)
    standardized_rows = centered_input * inverse_deviation
    normalized_rows = (standardized_rows * layer_norm_gain).astype(jnp.bfloat16)
    projected = jnp.dot(normalized_rows, qkv_weight, preferred_element_type=jnp.float32).astype(jnp.bfloat16)
    head_shape = (window_count, cell_count, head_count, head_size)
    query_rows = projected[:, :inner_width].reshape(head_shape).astype(jnp.float32)
    key_vectors = projected[:, inner_width:2 * inner_width].reshape(head_shape).astype(jnp.float32)
    value_rows = projected[:, 2 * inner_width:].reshape(head_shape).astype(jnp.float32)
    scores = jnp.einsum('wmhd,wnhd->whmn', query_rows, key_vectors) * score_scale + bias_full[None]
    same_region = labels[:, None, :, None] == labels[:, None, None, :]
    scores = jnp.where(same_region, scores, -1e+30)
    row_peak = lax.optimization_barrier(jnp.max(scores, axis=-1, keepdims=True))
    exp_scores = jnp.exp(scores - row_peak)
    attention_weights = exp_scores / lax.optimization_barrier(jnp.sum(exp_scores, axis=-1, keepdims=True))
    reduced_probability = attention_weights.astype(jnp.bfloat16)
    attended = jnp.einsum('whmn,wnhd->wmhd', reduced_probability.astype(jnp.float32), value_rows).astype(jnp.bfloat16)
    cot_rows = cot_windows.reshape(-1, features)
    d_attended = jnp.dot(cot_rows, out_weight.T, preferred_element_type=jnp.float32).astype(jnp.bfloat16)
    d_heads = d_attended.reshape(head_shape).astype(jnp.float32)
    d_prob = jnp.einsum('wmhd,wnhd->whmn', d_heads, value_rows)
    d_values = jnp.einsum('whmn,wmhd->wnhd', reduced_probability.astype(jnp.float32), d_heads).astype(jnp.bfloat16)
    d_scores = attention_weights * (d_prob - lax.optimization_barrier(jnp.sum(attention_weights * d_prob, axis=-1, keepdims=True)))
    table_part = lax.optimization_barrier(jnp.sum(d_scores, axis=0))
    d_low = d_scores.astype(jnp.bfloat16).astype(jnp.float32)
    d_queries = (jnp.einsum('whmn,wnhd->wmhd', d_low, key_vectors) * score_scale).astype(jnp.bfloat16)
    d_keys = (jnp.einsum('whmn,wmhd->wnhd', d_low, query_rows) * score_scale).astype(jnp.bfloat16)
    total_row_count = flat_rows.shape[0]
    d_projected = jnp.concatenate([d_queries.reshape(total_row_count, inner_width), d_keys.reshape(total_row_count, inner_width), d_values.reshape(total_row_count, inner_width)], axis=1)
    normalized_gradient = jnp.dot(d_projected, qkv_weight.T, preferred_element_type=jnp.float32)
    gain_contribution = lax.optimization_barrier(jnp.sum(normalized_gradient * standardized_rows, axis=0))
    scaled_rows = normalized_gradient * layer_norm_gain
    branch_gradient = inverse_deviation * (scaled_rows - lax.optimization_barrier(jnp.mean(scaled_rows, axis=-1, keepdims=True)) - standardized_rows * lax.optimization_barrier(jnp.mean(scaled_rows * standardized_rows, axis=-1, keepdims=True)))
    attended_rows = attended.reshape(total_row_count, inner_width)
    return (branch_gradient.astype(jnp.bfloat16), attended_rows, gain_contribution, table_part)

def reference(pixels, cotangent, embed_weight, embed_bias, layer_norm_gain, qkv_weight, out_weight, bias_table, rel_index, shifts):
    images, grid_rows, grid_cols, features = cotangent.shape
    head_count = bias_table.shape[0]
    table_size = bias_table.shape[1]
    inner_width = out_weight.shape[0]
    patch_width = embed_weight.shape[0]
    selector = (rel_index.reshape(-1)[:, None] == jnp.arange(table_size, dtype=jnp.int32)[None, :]).astype(jnp.float32)
    bias_full = jnp.dot(selector, bias_table.T, precision=lax.Precision.HIGHEST).T.reshape(head_count, WIN * WIN, WIN * WIN)
    patches_all = make_patches(pixels)
    band_count = grid_rows // WIN

    def per_image(carry, inputs):
        out_grad, embed_grad, bias_grad, gain_grad, table_grad = carry
        patches, cot_image, shift_pair = inputs
        tokens = (jnp.dot(patches, embed_weight, preferred_element_type=jnp.float32) + embed_bias).astype(jnp.bfloat16)
        shifted = jnp.roll(jnp.roll(tokens, -shift_pair[0], axis=0), -shift_pair[1], axis=1)
        shifted_cot = jnp.roll(jnp.roll(cot_image, -shift_pair[0], axis=0), -shift_pair[1], axis=1)
        band_tokens = shifted.reshape(band_count, WIN, grid_cols, features)
        band_cots = shifted_cot.reshape(band_count, WIN, grid_cols, features)

        def per_band(inner, band_inputs):
            band_out, band_gain, band_table = inner
            band_x, band_c, band_index = band_inputs
            row_ids = band_index * WIN + jnp.arange(WIN, dtype=jnp.int32)
            col_ids = jnp.arange(grid_cols, dtype=jnp.int32)
            row_part = (row_ids[:, None] >= grid_rows - shift_pair[0]).astype(jnp.int32)
            col_part = (col_ids[None, :] >= grid_cols - shift_pair[1]).astype(jnp.int32)
            region = 2 * row_part + col_part
            labels = window_split(region[:, :, None])[:, :, 0]
            cell_windows = window_split(band_x)
            cot_windows = window_split(band_c)
            branch_gradient, attended_rows, gain_contribution, table_part = window_grads(cell_windows, cot_windows, labels, layer_norm_gain, qkv_weight, out_weight, bias_full)
            band_out = band_out + lax.dot_general(attended_rows, cot_windows.reshape(-1, features), (((0,), (0,)), ((), ())), preferred_element_type=jnp.float32)
            joined = window_join(branch_gradient.reshape(-1, WIN * WIN, features), WIN, grid_cols)
            return ((band_out, band_gain + gain_contribution, band_table + table_part), joined)
        band_ids = jnp.arange(band_count, dtype=jnp.int32)
        (out_grad, gain_grad, table_grad), d_bands = lax.scan(per_band, (out_grad, gain_grad, table_grad), (band_tokens, band_cots, band_ids))
        branch_gradient = d_bands.reshape(grid_rows, grid_cols, features)
        d_back = jnp.roll(jnp.roll(branch_gradient, shift_pair[0], axis=0), shift_pair[1], axis=1)
        patch_rows = patches.reshape(-1, patch_width)
        cot_rows = cot_image.reshape(-1, features)
        back_rows = d_back.reshape(-1, features)
        contract = (((0,), (0,)), ((), ()))
        embed_grad = embed_grad + lax.dot_general(patch_rows, cot_rows, contract, preferred_element_type=jnp.float32) + lax.dot_general(patch_rows, back_rows, contract, preferred_element_type=jnp.float32)
        bias_grad = bias_grad + lax.optimization_barrier(jnp.sum(cot_rows, axis=0, dtype=jnp.float32)) + lax.optimization_barrier(jnp.sum(back_rows, axis=0, dtype=jnp.float32))
        return ((out_grad, embed_grad, bias_grad, gain_grad, table_grad), None)
    initial = (jnp.zeros((inner_width, features), jnp.float32), jnp.zeros((patch_width, features), jnp.float32), jnp.zeros((features,), jnp.float32), jnp.zeros((features,), jnp.float32), jnp.zeros((head_count, WIN * WIN, WIN * WIN), jnp.float32))
    totals, unused = lax.scan(per_image, initial, (patches_all, cotangent, shifts))
    out_grad, embed_grad, bias_grad, gain_grad, table_grad = totals
    table_result = jnp.dot(table_grad.reshape(head_count, -1), selector, precision=lax.Precision.HIGHEST)
    return (out_grad, embed_grad, bias_grad, gain_grad, table_result)
```

```python
import jax
import jax.numpy as jnp
from jax import lax
from jax.sharding import PartitionSpec as P

WIN = 8
PATCH = 4


norm_epsilon = 1e-05


def laid_out(blocks, dim):
    blocks = jnp.moveaxis(blocks, 0, dim)
    lengths = blocks.shape
    return blocks.reshape(*lengths[:dim], lengths[dim] * lengths[dim + 1], *lengths[dim + 2 :])


def exchange(blocks, axis):
    return lax.all_to_all(blocks, axis, split_axis=0, concat_axis=0, tiled=True)


def spread(line, axis):
    copies = jnp.broadcast_to(line[None], (lax.axis_size(axis), *line.shape))
    return exchange(copies, axis)


def gather_together(arrays, axis, dims):
    line = jnp.concatenate([a.reshape(-1) for a in arrays])
    lines, at, gathered = (spread(line, axis), 0, [])
    for a, dim in zip(arrays, dims):
        blocks = lines[:, at : at + a.size].reshape(-1, *a.shape)
        gathered.append(laid_out(blocks, dim))
        at += a.size
    return tuple(gathered)


def from_behind(value, axis, steps):
    count = lax.axis_size(axis)
    pairs = [(source, (source + steps) % count) for source in range(count)]
    return lax.ppermute(value, axis, pairs)


def in_blocks(x, dim, length):
    before, after = (x.shape[:dim], x.shape[dim + 1 :])
    return jnp.moveaxis(x.reshape(*before, length, -1, *after), dim, 0)


def summed_on_arrival(x, axis, dim):
    blocks = in_blocks(x, dim, lax.axis_size(axis))
    arrived = lax.all_to_all(blocks, axis, split_axis=0, concat_axis=0, tiled=True)
    return arrived.astype(jnp.float32).sum(axis=0)


def make_patches(pixel_block):
    images, channels, pixel_rows, pixel_cols = pixel_block.shape
    grid_rows = pixel_rows // PATCH
    grid_cols = pixel_cols // PATCH
    shaped = pixel_block.reshape(images, channels, grid_rows, PATCH, grid_cols, PATCH)
    return shaped.transpose(0, 2, 4, 1, 3, 5).reshape(
        images, grid_rows, grid_cols, channels * PATCH * PATCH
    )


def embed_cells(patches, embed_weight, embed_bias):
    return (jnp.dot(patches, embed_weight, preferred_element_type=jnp.float32) + embed_bias).astype(
        jnp.bfloat16
    )


def window_split(block):
    rows_all, cols_all, features = block.shape
    shaped = block.reshape(rows_all // WIN, WIN, cols_all // WIN, WIN, features)
    return shaped.transpose(0, 2, 1, 3, 4).reshape(-1, WIN * WIN, features)


def window_join(windows, rows_all, cols_all):
    features = windows.shape[-1]
    shaped = windows.reshape(rows_all // WIN, cols_all // WIN, WIN, WIN, features)
    return shaped.transpose(0, 2, 1, 3, 4).reshape(rows_all, cols_all, features)


def splice_after(own_block, borrowed, offsets, along_dim):
    length = own_block.shape[along_dim]

    def single(own_item, borrowed_item, offset):
        joined = jnp.concatenate([own_item, borrowed_item], along_dim - 1)
        return lax.dynamic_slice_in_dim(joined, offset, length, along_dim - 1)

    return jax.vmap(single)(own_block, borrowed, offsets)


def attend_forward(cell_windows, labels, layer_norm_gain, qkv_full, bias_full):
    window_count, cell_count, features = cell_windows.shape
    head_count = bias_full.shape[0]
    inner_width = qkv_full.shape[1] // 3
    head_size = inner_width // head_count
    score_scale = head_size ** (-0.5)
    flat_rows = cell_windows.reshape(-1, features).astype(jnp.float32)
    average = jnp.mean(flat_rows, axis=-1, keepdims=True)
    centered_input = flat_rows - average
    inverse_deviation = lax.rsqrt(
        jnp.mean(centered_input * centered_input, axis=-1, keepdims=True) + norm_epsilon
    )
    standardized_rows = centered_input * inverse_deviation
    normalized_rows = (standardized_rows * layer_norm_gain).astype(jnp.bfloat16)
    projected = jnp.dot(normalized_rows, qkv_full, preferred_element_type=jnp.float32).astype(
        jnp.bfloat16
    )
    head_shape = (window_count, cell_count, head_count, head_size)
    query_rows = projected[:, :inner_width].reshape(head_shape)
    key_vectors = projected[:, inner_width : 2 * inner_width].reshape(head_shape)
    value_rows = projected[:, 2 * inner_width :].reshape(head_shape)
    scores = (
        jnp.einsum("wmhd,wnhd->whmn", query_rows, key_vectors, preferred_element_type=jnp.float32)
        * score_scale
        + bias_full[None]
    )
    same_region = labels[:, None, :, None] == labels[:, None, None, :]
    scores = jnp.where(same_region, scores, -1e30)
    row_peak = jnp.max(scores, axis=-1, keepdims=True)
    exp_scores = jnp.exp(scores - row_peak)
    attention_weights = exp_scores / jnp.sum(exp_scores, axis=-1, keepdims=True)
    reduced_probability = attention_weights.astype(jnp.bfloat16)
    attended = jnp.einsum(
        "whmn,wnhd->wmhd", reduced_probability, value_rows, preferred_element_type=jnp.float32
    ).astype(jnp.bfloat16)
    stored_residuals = (
        standardized_rows,
        inverse_deviation,
        query_rows,
        key_vectors,
        value_rows,
        attention_weights,
        reduced_probability,
    )
    return (stored_residuals, attended.reshape(-1, inner_width))


def attend_backward(stored_residuals, d_attended, layer_norm_gain, qkv_full):
    (
        standardized_rows,
        inverse_deviation,
        query_rows,
        key_vectors,
        value_rows,
        attention_weights,
        reduced_probability,
    ) = stored_residuals
    head_shape = query_rows.shape
    score_scale = head_shape[3] ** (-0.5)
    total_row_count = standardized_rows.shape[0]
    inner_width = head_shape[2] * head_shape[3]
    d_heads = d_attended.reshape(head_shape)
    d_prob = jnp.einsum("wmhd,wnhd->whmn", d_heads, value_rows, preferred_element_type=jnp.float32)
    d_values = jnp.einsum(
        "whmn,wmhd->wnhd", reduced_probability, d_heads, preferred_element_type=jnp.float32
    ).astype(jnp.bfloat16)
    d_scores = attention_weights * (
        d_prob - jnp.sum(attention_weights * d_prob, axis=-1, keepdims=True)
    )
    table_part = jnp.sum(d_scores, axis=0)
    d_low = d_scores.astype(jnp.bfloat16)
    d_queries = (
        jnp.einsum("whmn,wnhd->wmhd", d_low, key_vectors, preferred_element_type=jnp.float32)
        * score_scale
    ).astype(jnp.bfloat16)
    d_keys = (
        jnp.einsum("whmn,wmhd->wnhd", d_low, query_rows, preferred_element_type=jnp.float32)
        * score_scale
    ).astype(jnp.bfloat16)
    d_projected = jnp.concatenate(
        [
            d_queries.reshape(total_row_count, inner_width),
            d_keys.reshape(total_row_count, inner_width),
            d_values.reshape(total_row_count, inner_width),
        ],
        axis=1,
    )
    normalized_gradient = lax.dot_general(
        d_projected, qkv_full, (((1,), (1,)), ((), ())), preferred_element_type=jnp.float32
    )
    gain_contribution = jnp.sum(normalized_gradient * standardized_rows, axis=0)
    scaled_rows = normalized_gradient * layer_norm_gain
    branch_gradient = inverse_deviation * (
        scaled_rows
        - jnp.mean(scaled_rows, axis=-1, keepdims=True)
        - standardized_rows * jnp.mean(scaled_rows * standardized_rows, axis=-1, keepdims=True)
    )
    return (branch_gradient.astype(jnp.bfloat16), gain_contribution, table_part)


def on_device(
    pixels,
    cotangent,
    embed_weight,
    embed_bias,
    layer_norm_gain,
    qkv_weight,
    out_weight,
    bias_table,
    rel_index,
    shifts,
):
    images, rows_dev, cols_dev, features = cotangent.shape
    head_count = bias_table.shape[0]
    grid_rows = rows_dev * lax.axis_size("row")
    grid_cols = cols_dev * lax.axis_size("col")
    row_shift = shifts[:, 0]
    col_shift = shifts[:, 1]
    qkv_columns, out_columns = gather_together((qkv_weight, out_weight), ("col", "dp"), (1, 1))
    rows_qkv, width_qkv = qkv_columns.shape
    out_tall = out_columns.reshape(rows_qkv, -1)
    weights = lax.all_gather(
        jnp.concatenate([qkv_columns, out_tall], axis=1), "row", axis=0, tiled=True
    )
    qkv_full = weights[:, :width_qkv]
    out_full = weights[:, width_qkv:].reshape(-1, features)
    patches = make_patches(pixels)
    below = from_behind((pixels, cotangent), "row", -1)
    moved_pixels = splice_after(pixels, below[0], row_shift * PATCH, 2)
    shifted_cot = splice_after(cotangent, below[1], row_shift, 1)
    beside = from_behind((moved_pixels[:, :, :, : WIN * PATCH], shifted_cot[:, :, :WIN]), "col", -1)
    moved_pixels = splice_after(moved_pixels, beside[0], col_shift * PATCH, 3)
    shifted_cot = splice_after(shifted_cot, beside[1], col_shift, 2)
    moved_patches = make_patches(moved_pixels)
    shifted = embed_cells(moved_patches, embed_weight, embed_bias)
    row_ids = lax.axis_index("row") * rows_dev + jnp.arange(rows_dev, dtype=jnp.int32)
    col_ids = lax.axis_index("col") * cols_dev + jnp.arange(cols_dev, dtype=jnp.int32)
    row_part = (row_ids[None, :] >= grid_rows - row_shift[:, None]).astype(jnp.int32)
    col_part = (col_ids[None, :] >= grid_cols - col_shift[:, None]).astype(jnp.int32)
    region = 2 * row_part[:, :, None] + col_part[:, None, :]
    labels = window_split(region.reshape(images * rows_dev, cols_dev, 1))[:, :, 0]
    cell_windows = window_split(shifted.reshape(images * rows_dev, cols_dev, features))
    cot_flat = window_split(shifted_cot.reshape(images * rows_dev, cols_dev, features)).reshape(
        -1, features
    )
    selector = (
        rel_index.reshape(-1)[:, None] == jnp.arange(bias_table.shape[1], dtype=jnp.int32)[None, :]
    ).astype(jnp.float32)
    bias_full = jnp.dot(selector, bias_table.T, precision=lax.Precision.HIGHEST).T.reshape(
        head_count, WIN * WIN, WIN * WIN
    )
    stored_residuals, attended = attend_forward(
        cell_windows, labels, layer_norm_gain, qkv_full, bias_full
    )
    d_attended = lax.dot_general(
        cot_flat,
        out_full,
        (((1,), (1,)), ((), ())),
        preferred_element_type=jnp.float32,
    ).astype(jnp.bfloat16)
    partial_rows = summed_on_arrival(
        lax.dot_general(
            attended, cot_flat, (((0,), (0,)), ((), ())), preferred_element_type=jnp.float32
        ).astype(jnp.bfloat16),
        "row",
        0,
    )
    d_rows, gain_contribution, table_part = attend_backward(
        stored_residuals, d_attended, layer_norm_gain, qkv_full
    )
    branch_gradient = window_join(
        d_rows.reshape(-1, WIN * WIN, features), images * rows_dev, cols_dev
    ).reshape(images, rows_dev, cols_dev, features)
    patch_rows = patches.reshape(-1, patches.shape[-1])
    cot_rows = cotangent.reshape(-1, features)
    contract = (((0,), (0,)), ((), ()))
    branch_patches = moved_patches.reshape(-1, patches.shape[-1])
    back_rows = branch_gradient.reshape(-1, features)
    embed_grad = lax.dot_general(
        patch_rows, cot_rows, contract, preferred_element_type=jnp.float32
    ) + lax.dot_general(branch_patches, back_rows, contract, preferred_element_type=jnp.float32)
    bias_grad = jnp.sum(cot_rows, axis=0, dtype=jnp.float32) + jnp.sum(
        back_rows, axis=0, dtype=jnp.float32
    )
    table_grad = jnp.dot(
        table_part.reshape(head_count, -1), selector, precision=lax.Precision.HIGHEST
    )
    head_table = table_grad.reshape(-1)
    pieces = [embed_grad.reshape(-1), bias_grad, gain_contribution, head_table]
    line = jnp.concatenate(pieces)
    row_count = lax.axis_size("row")
    piece = -(-line.size // (row_count * 1024)) * 1024
    line = jnp.pad(line, (0, row_count * piece - line.size)).reshape(row_count, piece // 128, 128)
    mine = exchange(line, "row").sum(axis=0).reshape(-1)
    col_blocks = in_blocks(partial_rows, 1, lax.axis_size(("col", "dp")))
    block_shape = col_blocks.shape
    col_blocks = col_blocks.reshape(block_shape[0], -1)
    own = jnp.broadcast_to(mine[None], (block_shape[0], piece))
    both = exchange(jnp.concatenate([own, col_blocks], axis=1), ("col", "dp")).sum(axis=0)
    out_weight_grad = both[piece:].reshape(block_shape[1:])
    total = spread(both[:piece].reshape(piece // 128, 128), "row").reshape(-1)
    results, at = ([], 0)
    for a, shape in zip(pieces, (embed_grad.shape, (features,), (features,), table_grad.shape)):
        results.append(total[at : at + a.size].reshape(shape))
        at += a.size
    return (out_weight_grad, *results)


def solution(mesh):
    return jax.shard_map(
        on_device,
        mesh=mesh,
        in_specs=(
            P("dp", None, "row", "col"),
            P("dp", "row", "col", None),
            P(),
            P(),
            P(),
            P("row", ("col", "dp")),
            P("row", ("col", "dp")),
            P(),
            P(),
            P("dp", None),
        ),
        out_specs=(P("row", ("col", "dp")), P(), P(), P(), P()),
        check_vma=False,
    )
```

```python
import jax
import jax.numpy as jnp
from jax import lax
from jax.experimental import pallas as pl
from jax.experimental.pallas import tpu as pltpu
from jax.sharding import PartitionSpec as P

WIN = 8
PATCH = 4
CELLS = WIN * WIN
norm_epsilon = 1e-05

STEP = 256
PAIR = 128
HEAD = 64
SCALE = HEAD ** (-0.5)


def dot_nn(a, b):
    return lax.dot_general(a, b, (((1,), (0,)), ((), ())), preferred_element_type=jnp.float32)


def dot_nt(a, b):
    return lax.dot_general(a, b, (((1,), (1,)), ((), ())), preferred_element_type=jnp.float32)


def dot_tn(a, b):
    return lax.dot_general(a, b, (((0,), (0,)), ((), ())), preferred_element_type=jnp.float32)


def head_lanes(width):
    lane = lax.broadcasted_iota(jnp.int32, (PAIR, width), 1)
    return [(lane // HEAD) == i for i in range(width // HEAD)]


def slabs(features):
    return [(at, min(PAIR, features - at)) for at in range(0, features, PAIR)]


def choose(masks, parts):
    return parts[0] if len(parts) == 1 else jnp.where(masks[0], parts[0], parts[1])


def forward_kernel(
    normed, cot, wq, wk, wv, bias, lab_col, lab_row, q_out, k_out, v_out, p_out, og_out, att, og_acc
):
    step = pl.program_id(0)
    x = normed[...]
    for weight, out in ((wq, q_out), (wk, k_out), (wv, v_out)):
        out[...] = dot_nn(x, weight[...]).astype(jnp.bfloat16)
    features = q_out.shape[1]
    for pair in range(STEP // PAIR):
        rows = slice(pair * PAIR, (pair + 1) * PAIR)
        same = lab_col[rows, :] == lab_row[pair, 0:1, :]
        for at, width in slabs(features):
            cols = slice(at, at + width)
            masks = head_lanes(width)
            q, k, v = q_out[rows, cols], k_out[rows, cols], v_out[rows, cols]
            parts = []
            for i, mask in enumerate(masks):
                head = at // HEAD + i
                mine = q if len(masks) == 1 else jnp.where(mask, q, jnp.zeros_like(q))
                scores = jnp.where(same, dot_nt(mine, k) * SCALE + bias[head], -1e30)
                peak = jnp.max(scores, axis=-1, keepdims=True)
                e = jnp.exp(scores - peak)
                p = e / jnp.sum(e, axis=-1, keepdims=True)
                p_out[pair, head] = p
                parts.append(dot_nn(p.astype(jnp.bfloat16), v))
            att[rows, cols] = choose(masks, parts).astype(jnp.bfloat16)
    grad = dot_tn(att[...], cot[...])

    @pl.when(step == 0)
    def _():
        og_acc[...] = grad

    @pl.when(step > 0)
    def _():
        og_acc[...] += grad

    @pl.when(step == pl.num_programs(0) - 1)
    def _():
        og_out[...] = og_acc[...].astype(og_out.dtype)


def backward_kernel(
    cot, patches, q_in, k_in, v_in, p_in, xhat, inv, gain, wq, wk, wv, wo,
    embed_out, bias_out, gain_out, table_out, datt, dq, dk, dv, dn, branch
):
    step = pl.program_id(0)
    features = q_in.shape[1]

    @pl.when(step == 0)
    def _():
        embed_out[...] = jnp.zeros_like(embed_out)
        bias_out[...] = jnp.zeros_like(bias_out)
        gain_out[...] = jnp.zeros_like(gain_out)
        table_out[...] = jnp.zeros_like(table_out)

    datt[...] = dot_nt(cot[...], wo[...]).astype(jnp.bfloat16)
    for pair in range(STEP // PAIR):
        rows = slice(pair * PAIR, (pair + 1) * PAIR)
        for at, width in slabs(features):
            cols = slice(at, at + width)
            masks = head_lanes(width)
            q, k, v = q_in[rows, cols], k_in[rows, cols], v_in[rows, cols]
            d_out = datt[rows, cols]
            qs, ks, vs = [], [], []
            for i, mask in enumerate(masks):
                head = at // HEAD + i
                mine = d_out if len(masks) == 1 else jnp.where(mask, d_out, jnp.zeros_like(d_out))
                p = p_in[pair, head]
                d_prob = dot_nt(mine, v)
                vs.append(dot_tn(p.astype(jnp.bfloat16), d_out))
                d_scores = p * (d_prob - jnp.sum(p * d_prob, axis=-1, keepdims=True))
                table_out[head] += d_scores
                low = d_scores.astype(jnp.bfloat16)
                qs.append(dot_nn(low, k))
                ks.append(dot_tn(low, q))
            dq[rows, cols] = (choose(masks, qs) * SCALE).astype(jnp.bfloat16)
            dk[rows, cols] = (choose(masks, ks) * SCALE).astype(jnp.bfloat16)
            dv[rows, cols] = choose(masks, vs).astype(jnp.bfloat16)
    dn[...] = dot_nt(dq[...], wq[...]) + dot_nt(dk[...], wk[...]) + dot_nt(dv[...], wv[...])
    chunk = 16
    width = dn.shape[1]
    gain_row = gain[0:1, :]

    def rows_at(i, carry):
        bias_sum, gain_sum = carry
        rows = pl.ds(pl.multiple_of(i * chunk, chunk), chunk)
        d, x = dn[rows, :], xhat[rows, :]
        gain_sum = gain_sum + (d * x).reshape(chunk // 8, 8, width).sum(axis=0)
        g = d * gain_row
        mean = jnp.mean(g, axis=-1, keepdims=True)
        along = jnp.mean(g * x, axis=-1, keepdims=True)
        out = (inv[rows, 0:1] * (g - mean - x * along)).astype(jnp.bfloat16)
        branch[rows, :] = out
        bias_sum = bias_sum + out.astype(jnp.float32).reshape(chunk // 8, 8, width).sum(axis=0)
        return bias_sum, gain_sum

    zero = jnp.zeros((8, width), jnp.float32)
    bias_sum, gain_sum = lax.fori_loop(0, STEP // chunk, rows_at, (zero, zero))
    bias_out[...] += bias_sum
    gain_out[...] += gain_sum
    embed_out[...] += dot_tn(patches[...], branch[...])


def stepped(shape, lead=False):
    rest = len(shape) - 1
    return pl.BlockSpec(shape, lambda i: (i,) + (0,) * rest)


def whole(shape, index=None):
    index = index or (0,) * len(shape)
    return pl.BlockSpec(shape, lambda i: index)


def params():
    return pltpu.CompilerParams(
        dimension_semantics=("arbitrary",), vmem_limit_bytes=56 * 1024 * 1024
    )


def run_forward(normed, cot, weights, weight_index, features, bias, lab_col, lab_row):
    cells, width = normed.shape
    heads = features // HEAD
    f32, bf16 = jnp.float32, jnp.bfloat16
    w_specs = [whole((width, features), index) for index in weight_index[:3]]
    return pl.pallas_call(
        forward_kernel,
        grid=(cells // STEP,),
        in_specs=[
            stepped((STEP, width)), stepped((STEP, width)), *w_specs,
            whole((heads, PAIR, PAIR)), stepped((STEP, PAIR)), stepped((STEP // PAIR, 8, PAIR)),
        ],
        out_specs=[
            *[stepped((STEP, features))] * 3,
            stepped((STEP // PAIR, heads, PAIR, PAIR)),
            whole((features, width)),
        ],
        out_shape=[
            *[jax.ShapeDtypeStruct((cells, features), bf16)] * 3,
            jax.ShapeDtypeStruct((cells // PAIR, heads, PAIR, PAIR), f32),
            jax.ShapeDtypeStruct((features, width), bf16),
        ],
        scratch_shapes=[pltpu.VMEM((STEP, features), bf16), pltpu.VMEM((features, width), f32)],
        compiler_params=params(), name="forward",
    )(normed, cot, *weights, bias, lab_col, lab_row)


def run_backward(cot, patches, q, k, v, p, xhat, inv, gain, weights, weight_index, wo):
    cells, width = cot.shape
    features = q.shape[1]
    heads = features // HEAD
    f32, bf16 = jnp.float32, jnp.bfloat16
    kd = patches.shape[1]
    w_specs = [whole((width, features), index) for index in weight_index[:3]]
    return pl.pallas_call(
        backward_kernel,
        grid=(cells // STEP,),
        in_specs=[
            stepped((STEP, width)), stepped((STEP, kd)), *[stepped((STEP, features))] * 3,
            stepped((STEP // PAIR, heads, PAIR, PAIR)),
            stepped((STEP, width)), stepped((STEP, PAIR)), whole((8, width)), *w_specs,
            whole((features, width)),
        ],
        out_specs=[whole((kd, width)), whole((8, width)), whole((8, width)), whole((heads, PAIR, PAIR))],
        out_shape=[
            jax.ShapeDtypeStruct((kd, width), f32), jax.ShapeDtypeStruct((8, width), f32),
            jax.ShapeDtypeStruct((8, width), f32), jax.ShapeDtypeStruct((heads, PAIR, PAIR), f32),
        ],
        scratch_shapes=[
            *[pltpu.VMEM((STEP, features), bf16)] * 4,
            pltpu.VMEM((STEP, width), f32), pltpu.VMEM((STEP, width), bf16),
        ],
        compiler_params=params(), name="backward",
    )(cot, patches, q, k, v, p, xhat, inv, gain, *weights, wo)


def exchange(blocks, axis):
    return lax.all_to_all(blocks, axis, split_axis=0, concat_axis=0, tiled=True)


def spread(line, axis):
    copies = jnp.broadcast_to(line[None], (lax.axis_size(axis), *line.shape))
    return exchange(copies, axis)


def from_behind(value, axis, steps):
    count = lax.axis_size(axis)
    pairs = [(source, (source + steps) % count) for source in range(count)]
    return lax.ppermute(value, axis, pairs)


def in_blocks(x, dim, length):
    before, after = (x.shape[:dim], x.shape[dim + 1 :])
    return jnp.moveaxis(x.reshape(*before, length, -1, *after), dim, 0)


def make_patches(pixel_block):
    channels, pixel_rows, pixel_cols = pixel_block.shape
    grid_rows = pixel_rows // PATCH
    grid_cols = pixel_cols // PATCH
    shaped = pixel_block.reshape(channels, grid_rows, PATCH, grid_cols, PATCH)
    return shaped.transpose(1, 3, 0, 2, 4).reshape(grid_rows, grid_cols, channels * PATCH * PATCH)


def window_split(block):
    rows_all, cols_all, features = block.shape
    shaped = block.reshape(rows_all // WIN, WIN, cols_all // WIN, WIN, features)
    return shaped.transpose(0, 2, 1, 3, 4).reshape(-1, features)


def splice_after(own, borrowed, offset, dim):
    joined = jnp.concatenate([own, borrowed], dim)
    return lax.dynamic_slice_in_dim(joined, offset, own.shape[dim], dim)


def on_device(
    pixels,
    cotangent,
    embed_weight,
    embed_bias,
    layer_norm_gain,
    qkv_weight,
    out_weight,
    bias_table,
    rel_index,
    shifts,
):
    cotangent, pixels = cotangent[0], pixels[0]
    rows_dev, cols_dev, width = cotangent.shape
    heads, table_size = bias_table.shape
    features = heads * HEAD
    grid_rows = rows_dev * lax.axis_size("row")
    grid_cols = cols_dev * lax.axis_size("col")
    row_shift, col_shift = shifts[0, 0], shifts[0, 1]
    rows_w = qkv_weight.shape[0]

    line = jnp.concatenate([qkv_weight.reshape(-1), out_weight.reshape(-1)])
    lines = spread(line, ("col", "dp"))
    count = lines.shape[0]
    split = qkv_weight.size
    qkv_rows = jnp.moveaxis(lines[:, :split].reshape(count, *qkv_weight.shape), 0, 1)
    out_rows = jnp.moveaxis(lines[:, split:].reshape(count, *out_weight.shape), 0, 1)
    weights = lax.all_gather(
        jnp.concatenate([qkv_rows.reshape(rows_w, -1), out_rows.reshape(rows_w, -1)], axis=1),
        "row", axis=0, tiled=True,
    )
    wo = weights[:, 3 * features :].reshape(features, width)

    below = from_behind((pixels, cotangent), "row", -1)
    pix = splice_after(pixels, below[0], row_shift * PATCH, 1)
    cot = splice_after(cotangent, below[1], row_shift, 0)
    beside = from_behind((pix[:, :, : WIN * PATCH], cot[:, :WIN]), "col", -1)
    pix = splice_after(pix, beside[0], col_shift * PATCH, 2)
    cot = splice_after(cot, beside[1], col_shift, 1)
    patches = window_split(make_patches(pix))
    cot = window_split(cot)
    cells = cot.shape[0]
    tokens = jnp.dot(patches, embed_weight, preferred_element_type=jnp.float32) + embed_bias
    tokens = tokens.astype(jnp.bfloat16).astype(jnp.float32)
    centered = tokens - jnp.mean(tokens, axis=-1, keepdims=True)
    inv = lax.rsqrt(jnp.mean(centered * centered, axis=-1, keepdims=True) + norm_epsilon)
    xhat = centered * inv
    normed = (xhat * layer_norm_gain).astype(jnp.bfloat16)
    inv = jnp.broadcast_to(inv, (cells, PAIR))

    row_ids = lax.axis_index("row") * rows_dev + jnp.arange(rows_dev, dtype=jnp.int32)
    col_ids = lax.axis_index("col") * cols_dev + jnp.arange(cols_dev, dtype=jnp.int32)
    row_part = (row_ids >= grid_rows - row_shift).astype(jnp.int32)
    col_part = (col_ids >= grid_cols - col_shift).astype(jnp.int32)
    region = window_split((2 * row_part[:, None] + col_part[None, :])[:, :, None])[:, 0]
    label = region + 4 * (jnp.arange(cells, dtype=jnp.int32) // CELLS)
    lab_col = jnp.broadcast_to(label[:, None], (cells, PAIR))
    lab_row = jnp.broadcast_to(label.reshape(-1, 1, PAIR), (cells // PAIR, 8, PAIR))
    selector = (
        rel_index.reshape(-1)[:, None] == jnp.arange(table_size, dtype=jnp.int32)[None, :]
    ).astype(jnp.float32)
    bias = jnp.dot(selector, bias_table.T, precision=lax.Precision.HIGHEST).T
    bias = jnp.tile(bias.reshape(heads, CELLS, CELLS), (1, 2, 2))

    trio = (weights, weights, weights)
    places = ((0, 0), (0, 1), (0, 2))
    q, k, v, prob, out_grad = run_forward(
        normed, cot, trio, places, features, bias, lab_col, lab_row
    )
    arrived = exchange(in_blocks(out_grad, 0, lax.axis_size("row")), "row")
    gain = jnp.broadcast_to(layer_norm_gain[None], (8, width))
    embed_part, bias_part, gain_part, table_part = run_backward(
        cot, patches, q, k, v, prob, xhat, inv, gain, trio, places, wo
    )
    contract = (((0,), (0,)), ((), ()))
    embed_grad = embed_part + lax.dot_general(
        patches, cot, contract, preferred_element_type=jnp.float32
    )
    bias_grad = bias_part.sum(axis=0) + jnp.sum(cot, axis=0, dtype=jnp.float32)
    gain_grad = gain_part.sum(axis=0)
    table_part = table_part[:, :CELLS, :CELLS] + table_part[:, CELLS:, CELLS:]
    table_grad = jnp.dot(
        table_part.reshape(heads, -1), selector, precision=lax.Precision.HIGHEST
    )

    partial_rows = arrived.astype(jnp.float32).sum(axis=0)
    pieces = [embed_grad.reshape(-1), bias_grad, gain_grad, table_grad.reshape(-1)]
    line = jnp.concatenate(pieces)
    row_count = lax.axis_size("row")
    piece = -(-line.size // (row_count * 1024)) * 1024
    line = jnp.pad(line, (0, row_count * piece - line.size)).reshape(row_count, piece // 128, 128)
    mine = exchange(line, "row").sum(axis=0).reshape(-1)
    col_blocks = in_blocks(partial_rows, 1, lax.axis_size(("col", "dp")))
    block_shape = col_blocks.shape
    col_blocks = col_blocks.reshape(block_shape[0], -1)
    own = jnp.broadcast_to(mine[None], (block_shape[0], piece))
    both = exchange(jnp.concatenate([own, col_blocks], axis=1), ("col", "dp")).sum(axis=0)
    out_weight_grad = both[piece:].reshape(block_shape[1:])
    total = spread(both[:piece].reshape(piece // 128, 128), "row").reshape(-1)
    results, at = ([], 0)
    for a, shape in zip(pieces, (embed_grad.shape, (width,), (width,), table_grad.shape)):
        results.append(total[at : at + a.size].reshape(shape))
        at += a.size
    return (out_weight_grad, *results)


def solution(mesh):
    return jax.shard_map(
        on_device,
        mesh=mesh,
        in_specs=(
            P("dp", None, "row", "col"),
            P("dp", "row", "col", None),
            P(),
            P(),
            P(),
            P("row", ("col", "dp")),
            P("row", ("col", "dp")),
            P(),
            P(),
            P("dp", None),
        ),
        out_specs=(P("row", ("col", "dp")), P(), P(), P(), P()),
        check_vma=False,
    )
```

```python
import jax
import jax.numpy as jnp
from jax import lax
from jax.experimental import pallas as pl
from jax.experimental.pallas import tpu as pltpu
from jax.sharding import Mesh, PartitionSpec as P

WIN = 8
PATCH = 4
CELLS = WIN * WIN
norm_epsilon = 1e-05

STEP = 256
PAIR = 128
HEAD = 64
LANES = 128
SCALE = HEAD ** (-0.5)
UNITS = ((0, 128, 256, 0, 2), (384, 448, 512, 128, 1))
QKV = 640


def dot_nn(a, b):
    return lax.dot_general(a, b, (((1,), (0,)), ((), ())), preferred_element_type=jnp.float32)


def dot_nt(a, b):
    return lax.dot_general(a, b, (((1,), (1,)), ((), ())), preferred_element_type=jnp.float32)


def dot_tn(a, b):
    return lax.dot_general(a, b, (((0,), (0,)), ((), ())), preferred_element_type=jnp.float32)


def half_masks(count):
    lane = lax.broadcasted_iota(jnp.int32, (PAIR, count * HEAD), 1)
    return [(lane // HEAD) == i for i in range(count)]


def choose(masks, parts):
    return parts[0] if len(parts) == 1 else jnp.where(masks[0], parts[0], parts[1])


def only(masks, i, x):
    return x if len(masks) == 1 else jnp.where(masks[i], x, jnp.zeros_like(x))


def forward_kernel(
    cot, patches, embed_w, embed_b, gain, weights, bias, lab_col, lab_row,
    proj_out, prob_out, xhat_out, inv_out, grad_out, att, grad_acc
):
    step = pl.program_id(0)
    tokens = dot_nn(patches[...], embed_w[...]) + embed_b[0:1, :]
    tokens = tokens.astype(jnp.bfloat16).astype(jnp.float32)
    centered = tokens - jnp.mean(tokens, axis=-1, keepdims=True)
    inv = lax.rsqrt(jnp.mean(centered * centered, axis=-1, keepdims=True) + norm_epsilon)
    xhat = centered * inv
    xhat_out[...] = xhat
    inv_out[...] = jnp.broadcast_to(inv, inv_out.shape)
    normed = (xhat * gain[0:1, :]).astype(jnp.bfloat16)
    proj_out[...] = dot_nn(normed, weights[:, :QKV]).astype(jnp.bfloat16)
    for pair in range(STEP // PAIR):
        rows = slice(pair * PAIR, (pair + 1) * PAIR)
        same = lab_col[rows, :] == lab_row[pair, 0:1, :]
        for q_at, k_at, v_at, at, count in UNITS:
            width = count * HEAD
            masks = half_masks(count)
            q = proj_out[rows, q_at : q_at + width]
            k = proj_out[rows, k_at : k_at + width]
            v = proj_out[rows, v_at : v_at + width]
            parts = []
            for i in range(count):
                head = at // HEAD + i
                scores = dot_nt(only(masks, i, q), k) * SCALE + bias[head]
                scores = jnp.where(same, scores, -1e30)
                peak = jnp.max(scores, axis=-1, keepdims=True)
                e = jnp.exp(scores - peak)
                prob = e / jnp.sum(e, axis=-1, keepdims=True)
                prob_out[pair, head] = prob
                parts.append(dot_nn(prob.astype(jnp.bfloat16), v))
            att[rows, at : at + width] = choose(masks, parts).astype(jnp.bfloat16)
    grad = dot_tn(att[...], cot[...])

    @pl.when(step == 0)
    def _():
        grad_acc[...] = grad

    @pl.when(step > 0)
    def _():
        grad_acc[...] += grad

    @pl.when(step == pl.num_programs(0) - 1)
    def _():
        grad_out[...] = grad_acc[...].astype(grad_out.dtype)


def backward_kernel(
    cot, patches, proj, prob_in, xhat, inv, gain, weights, wo,
    embed_out, bias_out, gain_out, table_out, datt, dproj, dn, branch
):
    step = pl.program_id(0)

    @pl.when(step == 0)
    def _():
        embed_out[...] = jnp.zeros_like(embed_out)
        bias_out[...] = jnp.zeros_like(bias_out)
        gain_out[...] = jnp.zeros_like(gain_out)
        table_out[...] = jnp.zeros_like(table_out)
        dproj[...] = jnp.zeros_like(dproj)

    datt[...] = dot_nt(cot[...], wo[...]).astype(jnp.bfloat16)
    for pair in range(STEP // PAIR):
        rows = slice(pair * PAIR, (pair + 1) * PAIR)
        for q_at, k_at, v_at, at, count in UNITS:
            width = count * HEAD
            masks = half_masks(count)
            q = proj[rows, q_at : q_at + width]
            k = proj[rows, k_at : k_at + width]
            v = proj[rows, v_at : v_at + width]
            d_out = datt[rows, at : at + width]
            qs, ks, vs = [], [], []
            for i in range(count):
                head = at // HEAD + i
                prob = prob_in[pair, head]
                d_prob = dot_nt(only(masks, i, d_out), v)
                vs.append(dot_tn(prob.astype(jnp.bfloat16), d_out))
                d_scores = prob * (d_prob - jnp.sum(prob * d_prob, axis=-1, keepdims=True))
                table_out[head] += d_scores
                low = d_scores.astype(jnp.bfloat16)
                qs.append(dot_nn(low, k))
                ks.append(dot_tn(low, q))
            dproj[rows, q_at : q_at + width] = (choose(masks, qs) * SCALE).astype(jnp.bfloat16)
            dproj[rows, k_at : k_at + width] = (choose(masks, ks) * SCALE).astype(jnp.bfloat16)
            dproj[rows, v_at : v_at + width] = choose(masks, vs).astype(jnp.bfloat16)
    dn[...] = dot_nt(dproj[...], weights[:, :QKV])
    chunk = 16
    width = dn.shape[1]
    gain_row = gain[0:1, :]

    def rows_at(i, carry):
        bias_sum, gain_sum = carry
        rows = pl.ds(pl.multiple_of(i * chunk, chunk), chunk)
        d, x = dn[rows, :], xhat[rows, :]
        gain_sum = gain_sum + (d * x).reshape(chunk // 8, 8, width).sum(axis=0)
        g = d * gain_row
        mean = jnp.mean(g, axis=-1, keepdims=True)
        along = jnp.mean(g * x, axis=-1, keepdims=True)
        out = (inv[rows, 0:1] * (g - mean - x * along)).astype(jnp.bfloat16)
        branch[rows, :] = out
        bias_sum = bias_sum + out.astype(jnp.float32).reshape(chunk // 8, 8, width).sum(axis=0)
        return bias_sum, gain_sum

    zero = jnp.zeros((8, width), jnp.float32)
    bias_sum, gain_sum = lax.fori_loop(0, STEP // chunk, rows_at, (zero, zero))
    bias_out[...] += bias_sum
    gain_out[...] += gain_sum
    embed_out[...] += dot_tn(patches[...], branch[...])


def stepped(shape, lead=False):
    rest = len(shape) - 1
    return pl.BlockSpec(shape, lambda i: (i,) + (0,) * rest)


def whole(shape, index=None):
    index = index or (0,) * len(shape)
    return pl.BlockSpec(shape, lambda i: index)


def params():
    return pltpu.CompilerParams(
        dimension_semantics=("arbitrary",), vmem_limit_bytes=56 * 1024 * 1024
    )


def run_forward(joined, embed_w, embed_b, gain, weights, bias, lab_col, lab_row):
    cells, width = joined.shape[0], gain.shape[1]
    heads = bias.shape[0]
    features = heads * HEAD
    f32, bf16 = jnp.float32, jnp.bfloat16
    return pl.pallas_call(
        forward_kernel,
        grid=(cells // STEP,),
        in_specs=[
            stepped((STEP, width)),
            pl.BlockSpec((STEP, LANES), lambda i: (i, width // LANES)),
            whole((LANES, width)), whole((8, width)), whole((8, width)), whole(weights.shape),
            whole((heads, PAIR, PAIR)), stepped((STEP, PAIR)), stepped((STEP // PAIR, 8, PAIR)),
        ],
        out_specs=[
            stepped((STEP, QKV)), stepped((STEP // PAIR, heads, PAIR, PAIR)),
            stepped((STEP, width)), stepped((STEP, LANES)), whole((features, width)),
        ],
        out_shape=[
            jax.ShapeDtypeStruct((cells, QKV), bf16),
            jax.ShapeDtypeStruct((cells // PAIR, heads, PAIR, PAIR), f32),
            jax.ShapeDtypeStruct((cells, width), f32),
            jax.ShapeDtypeStruct((cells, LANES), f32),
            jax.ShapeDtypeStruct((features, width), bf16),
        ],
        scratch_shapes=[pltpu.VMEM((STEP, features), bf16), pltpu.VMEM((features, width), f32)],
        compiler_params=params(), name="forward",
        cost_estimate=pl.CostEstimate(
            flops=2 * cells * width * (QKV + features + LANES), transcendentals=cells * heads * PAIR,
            bytes_accessed=cells * width * 8,
        ),
    )(joined, joined, embed_w, embed_b, gain, weights, bias, lab_col, lab_row)


def run_backward(joined, proj, prob, xhat, inv, gain, weights, wo):
    cells, width = xhat.shape
    features = wo.shape[0]
    heads = features // HEAD
    f32, bf16 = jnp.float32, jnp.bfloat16
    return pl.pallas_call(
        backward_kernel,
        grid=(cells // STEP,),
        in_specs=[
            stepped((STEP, width)),
            pl.BlockSpec((STEP, LANES), lambda i: (i, width // LANES)),
            stepped((STEP, QKV)), stepped((STEP // PAIR, heads, PAIR, PAIR)),
            stepped((STEP, width)), stepped((STEP, LANES)), whole((8, width)),
            whole(weights.shape), whole((features, width)),
        ],
        out_specs=[
            whole((LANES, width)), whole((8, width)), whole((8, width)),
            whole((heads, PAIR, PAIR)),
        ],
        out_shape=[
            jax.ShapeDtypeStruct((LANES, width), f32), jax.ShapeDtypeStruct((8, width), f32),
            jax.ShapeDtypeStruct((8, width), f32), jax.ShapeDtypeStruct((heads, PAIR, PAIR), f32),
        ],
        scratch_shapes=[
            pltpu.VMEM((STEP, features), bf16), pltpu.VMEM((STEP, QKV), bf16),
            pltpu.VMEM((STEP, width), f32), pltpu.VMEM((STEP, width), bf16),
        ],
        compiler_params=params(), name="backward",
        cost_estimate=pl.CostEstimate(
            flops=2 * cells * width * (QKV + features + LANES), transcendentals=0,
            bytes_accessed=cells * width * 8,
        ),
    )(joined, joined, proj, prob, xhat, inv, gain, weights, wo)


ROW = ("yl", "x", "core")
COL = ("col", "dp")
CHIP_ROW = ("x", "core")
FAR = ("yl", "col", "dp")


def exchange(blocks, axis):
    return lax.all_to_all(blocks, axis, split_axis=0, concat_axis=0, tiled=True)


def spread(line, axis):
    copies = jnp.broadcast_to(line[None], (lax.axis_size(axis), *line.shape))
    return exchange(copies, axis)


def from_behind(value, axis):
    count = lax.axis_size(axis)
    return lax.ppermute(value, axis, [(source, (source - 1) % count) for source in range(count)])


def swap(value, axis):
    count = lax.axis_size(axis)
    return lax.ppermute(value, axis, [(source, source ^ 1) for source in range(count)])


def make_patches(pixel_block):
    channels, pixel_rows, pixel_cols = pixel_block.shape
    grid_rows = pixel_rows // PATCH
    grid_cols = pixel_cols // PATCH
    shaped = pixel_block.reshape(channels, grid_rows, PATCH, grid_cols, PATCH)
    return shaped.transpose(1, 3, 0, 2, 4).reshape(grid_rows, grid_cols, channels * PATCH * PATCH)


def window_split(block):
    rows_all, cols_all, features = block.shape
    shaped = block.reshape(rows_all // WIN, WIN, cols_all // WIN, WIN, features)
    return shaped.transpose(0, 2, 1, 3, 4).reshape(-1, features)


def splice_after(own, borrowed, offset, dim):
    joined = jnp.concatenate([own, borrowed], dim)
    return lax.dynamic_slice_in_dim(joined, offset, own.shape[dim], dim)


def pack_out(rows):
    tall = rows[:16].reshape(16, 8, LANES).transpose(1, 0, 2).reshape(LANES, LANES)
    low = rows[16:].reshape(8, 8, LANES).transpose(1, 0, 2).reshape(64, 2, 64)
    return jnp.concatenate([low.transpose(1, 0, 2).reshape(LANES, 64), tall], axis=1)


def unpack_out(blocks):
    count = blocks.shape[0]
    tall = blocks[:, :, 64:].reshape(count, 8, 16, LANES).transpose(0, 2, 1, 3)
    low = blocks[:, :, :64].reshape(count, 2, 64, 64).transpose(0, 2, 1, 3)
    low = low.reshape(count, 8, 8, LANES).transpose(0, 2, 1, 3)
    return jnp.concatenate([tall, low], axis=1).reshape(count * 24, 8 * LANES)


def gather_weights(qkv_weight, out_weight, half, heads):
    line = jnp.concatenate([qkv_weight.reshape(-1), out_weight.reshape(-1)])
    lines = spread(line, FAR)
    split = qkv_weight.size
    bands = lax.axis_size("yl")
    cols = lines.shape[0] // bands
    rows_w, rows_o = qkv_weight.shape[0], out_weight.shape[0]
    qkv = lines[:, :split].reshape(bands, cols, *qkv_weight.shape).transpose(0, 2, 1, 3)
    qkv = qkv.reshape(bands * rows_w, 3, -1)
    out = lines[:, split:].reshape(bands, cols, *out_weight.shape).transpose(0, 2, 1, 3)
    out = out.reshape(bands, rows_o, -1)
    features = qkv.shape[2]
    mine = lax.dynamic_slice_in_dim(qkv, half * (features // 2), features // 2, 2)
    out = lax.dynamic_slice_in_dim(out, half * 2, 2, 0)
    group = features // 4
    blocks = []
    for core in range(2):
        part = mine[:, :, core * group : (core + 1) * group]
        pieces = [part[:, i, :LANES] for i in range(3)] + [part[:, i, LANES:] for i in range(3)]
        blocks.append(jnp.concatenate([*pieces, pack_out(out[core])], axis=1))
    both = jnp.stack(blocks)
    chips = lax.axis_size("x")
    sent = jnp.broadcast_to(both[None], (chips, *both.shape)).reshape(2 * chips, *both.shape[1:])
    arrived = exchange(sent, CHIP_ROW)
    wo = unpack_out(arrived[:, :, QKV - 64 :])
    weights = arrived.reshape(2 * chips, bands, rows_w, -1).transpose(1, 0, 2, 3)
    return weights.reshape(bands * 2 * chips * rows_w, -1), wo


def on_device(
    pixels,
    cotangent,
    embed_weight,
    embed_bias,
    layer_norm_gain,
    qkv_weight,
    out_weight,
    bias_table,
    rel_index,
    shifts,
):
    cotangent, pixels = cotangent[0], pixels[0]
    rows_dev, cols_dev, width = cotangent.shape
    all_heads, table_size = bias_table.shape
    heads = all_heads // 4
    grid_rows = rows_dev * lax.axis_size(ROW)
    grid_cols = cols_dev * lax.axis_size("col")
    row_shift, col_shift = shifts[0, 0], shifts[0, 1]
    row_at, col_at, core = lax.axis_index(ROW), lax.axis_index("col"), lax.axis_index("core")
    half = col_at % 2
    group = 2 * half + core

    with jax.named_scope("weights"):
        weights, wo = gather_weights(qkv_weight, out_weight, half, heads)

    depth = embed_weight.shape[0]
    patches = make_patches(pixels)
    patches = jnp.pad(patches, ((0, 0), (0, 0), (0, LANES - depth)))
    block = jnp.concatenate([cotangent, patches], axis=-1)
    block = splice_after(block, from_behind(block[: WIN - 1], ROW), row_shift, 0)
    block = splice_after(block, from_behind(block[:, :WIN], "col"), col_shift, 1)
    own = window_split(block)
    two = jnp.concatenate([own, swap(own, "col")])
    joined = jnp.concatenate([two, swap(two, "core")])
    cells = joined.shape[0]

    labels = []
    for row_flip, col_flip in ((0, 0), (0, 1), (1, 0), (1, 1)):
        row_ids = (row_at ^ row_flip) * rows_dev + jnp.arange(rows_dev, dtype=jnp.int32)
        col_ids = (col_at ^ col_flip) * cols_dev + jnp.arange(cols_dev, dtype=jnp.int32)
        row_part = (row_ids >= grid_rows - row_shift).astype(jnp.int32)
        col_part = (col_ids >= grid_cols - col_shift).astype(jnp.int32)
        region = 2 * row_part[:, None] + col_part[None, :]
        labels.append(window_split(region[:, :, None])[:, 0])
    label = jnp.concatenate(labels) + 4 * (jnp.arange(cells, dtype=jnp.int32) // CELLS)
    lab_col = jnp.broadcast_to(label[:, None], (cells, PAIR))
    lab_row = jnp.broadcast_to(label.reshape(-1, 1, PAIR), (cells // PAIR, 8, PAIR))
    selector = (
        rel_index.reshape(-1)[:, None] == jnp.arange(table_size, dtype=jnp.int32)[None, :]
    ).astype(jnp.float32)
    my_table = lax.dynamic_slice_in_dim(bias_table, group * heads, heads, 0)
    bias = jnp.dot(selector, my_table.T, precision=lax.Precision.HIGHEST).T
    bias = jnp.tile(bias.reshape(heads, CELLS, CELLS), (1, 2, 2))
    embed_w = jnp.pad(embed_weight, ((0, LANES - depth), (0, 0)))
    embed_b = jnp.broadcast_to(embed_bias[None], (8, width))
    gain = jnp.broadcast_to(layer_norm_gain[None], (8, width))
    contract = (((0,), (0,)), ((), ()))
    cot_own, patches_own = own[:, :width], own[:, width:]
    embed_cot = lax.dot_general(patches_own, cot_own, contract, preferred_element_type=jnp.float32)
    bias_cot = jnp.sum(cot_own, axis=0, dtype=jnp.float32)

    proj, prob, xhat, inv, out_grad = run_forward(
        joined, embed_w, embed_b, gain, weights, bias, lab_col, lab_row
    )
    with jax.named_scope("outgrad"):
        count = lax.axis_size(CHIP_ROW)
        arrived = exchange(out_grad.reshape(count, -1, width), CHIP_ROW)
        by_core = arrived.reshape(count // 2, 2, -1, width).astype(jnp.float32).sum(axis=0)
        held = by_core.astype(jnp.bfloat16)
        none = jnp.zeros_like(held)
        bands = [jnp.where(half == i, held, none) for i in range(2)]
        partial_rows = exchange(jnp.concatenate(bands), "yl").astype(jnp.float32).sum(axis=0)
    embed_part, bias_part, gain_part, table_part = run_backward(
        joined, proj, prob, xhat, inv, gain, weights, wo
    )
    embed_grad = (embed_part + embed_cot)[:depth]
    bias_grad = bias_part.sum(axis=0) + bias_cot
    gain_grad = gain_part.sum(axis=0)
    table_part = table_part[:, :CELLS, :CELLS] + table_part[:, CELLS:, CELLS:]
    my_grad = jnp.dot(table_part.reshape(heads, -1), selector, precision=lax.Precision.HIGHEST)
    table_grad = lax.dynamic_update_slice_in_dim(
        jnp.zeros((all_heads, table_size), jnp.float32), my_grad, group * heads, 0
    )

    pieces = [embed_grad.reshape(-1), bias_grad, gain_grad, table_grad.reshape(-1)]
    line = jnp.concatenate(pieces)
    row_count = lax.axis_size(ROW)
    piece = -(-line.size // (row_count * 2048)) * 2048
    line = jnp.pad(line, (0, row_count * piece - line.size)).astype(jnp.bfloat16)
    line = line.reshape(row_count, piece // LANES, LANES)
    mine = exchange(line, ROW).astype(jnp.float32).sum(axis=0).reshape(-1)
    count = lax.axis_size(COL)
    col_blocks = partial_rows.reshape(partial_rows.shape[0], count, -1).transpose(1, 0, 2)
    block_shape = col_blocks.shape
    col_blocks = col_blocks.reshape(count, -1).astype(jnp.bfloat16)
    own = jnp.broadcast_to(mine[None].astype(jnp.bfloat16), (count, piece))
    both = exchange(jnp.concatenate([own, col_blocks], axis=1), COL)
    both = both.astype(jnp.float32).sum(axis=0)
    out_weight_grad = both[piece:].reshape(block_shape[1:])
    total = both[:piece].astype(jnp.bfloat16).reshape(piece // LANES, LANES)
    total = spread(total, ROW).reshape(-1).astype(jnp.float32)
    results, at = ([], 0)
    for a, shape in zip(pieces, (embed_grad.shape, (width,), (width,), table_grad.shape)):
        results.append(total[at : at + a.size].reshape(shape))
        at += a.size
    return (out_weight_grad, *results)


def solution(mesh):
    sizes = mesh.devices.shape
    names = ("yl", "x", "core", "col", "dp")
    fine = Mesh(mesh.devices.reshape(-1, 4, 2, *sizes[1:]), names)
    return jax.shard_map(
        on_device,
        mesh=fine,
        in_specs=(
            P("dp", None, ROW, "col"),
            P("dp", ROW, "col", None),
            P(),
            P(),
            P(),
            P(ROW, COL),
            P(ROW, COL),
            P(),
            P(),
            P("dp", None),
        ),
        out_specs=(P(ROW, COL), P(), P(), P(), P()),
        check_vma=False,
    )
```

```python
import jax
import jax.numpy as jnp
from jax import lax
from jax.experimental import pallas as pl
from jax.experimental.pallas import tpu as pltpu
from jax.sharding import Mesh, PartitionSpec as P

WIN = 8
PATCH = 4
CELLS = WIN * WIN
norm_epsilon = 1e-05

STEP = 256
PAIR = 128
HEAD = 64
LANES = 128
SCALE = HEAD ** (-0.5)
UNITS = ((0, 128, 256, 0, 2), (384, 448, 512, 128, 1))
QKV = 640


def dot_nn(a, b):
    return lax.dot_general(a, b, (((1,), (0,)), ((), ())), preferred_element_type=jnp.float32)


def dot_nt(a, b):
    return lax.dot_general(a, b, (((1,), (1,)), ((), ())), preferred_element_type=jnp.float32)


def dot_tn(a, b):
    return lax.dot_general(a, b, (((0,), (0,)), ((), ())), preferred_element_type=jnp.float32)


def half_masks(count):
    lane = lax.broadcasted_iota(jnp.int32, (PAIR, count * HEAD), 1)
    return [(lane // HEAD) == i for i in range(count)]


def choose(masks, parts):
    return parts[0] if len(parts) == 1 else jnp.where(masks[0], parts[0], parts[1])


def only(masks, i, x):
    return x if len(masks) == 1 else jnp.where(masks[i], x, jnp.zeros_like(x))


def forward_kernel(
    cot, patches, embed_w, embed_b, gain, weights, bias, lab_col, lab_row,
    proj_out, prob_out, xhat_out, inv_out, grad_out, att, grad_acc
):
    step = pl.program_id(0)
    tokens = dot_nn(patches[...], embed_w[...]) + embed_b[0:1, :]
    tokens = tokens.astype(jnp.bfloat16).astype(jnp.float32)
    centered = tokens - jnp.mean(tokens, axis=-1, keepdims=True)
    inv = lax.rsqrt(jnp.mean(centered * centered, axis=-1, keepdims=True) + norm_epsilon)
    xhat = centered * inv
    xhat_out[...] = xhat
    inv_out[...] = jnp.broadcast_to(inv, inv_out.shape)
    normed = (xhat * gain[0:1, :]).astype(jnp.bfloat16)
    proj_out[...] = dot_nn(normed, weights[:, :QKV]).astype(jnp.bfloat16)
    for pair in range(STEP // PAIR):
        rows = slice(pair * PAIR, (pair + 1) * PAIR)
        same = lab_col[rows, :] == lab_row[pair, 0:1, :]
        for q_at, k_at, v_at, at, count in UNITS:
            width = count * HEAD
            masks = half_masks(count)
            q = proj_out[rows, q_at : q_at + width]
            k = proj_out[rows, k_at : k_at + width]
            v = proj_out[rows, v_at : v_at + width]
            parts = []
            for i in range(count):
                head = at // HEAD + i
                scores = dot_nt(only(masks, i, q), k) * SCALE + bias[head]
                scores = jnp.where(same, scores, -1e30)
                peak = jnp.max(scores, axis=-1, keepdims=True)
                e = jnp.exp(scores - peak)
                prob = e / jnp.sum(e, axis=-1, keepdims=True)
                prob_out[pair, head] = prob
                parts.append(dot_nn(prob.astype(jnp.bfloat16), v))
            att[rows, at : at + width] = choose(masks, parts).astype(jnp.bfloat16)
    grad = dot_tn(att[...], cot[...])

    @pl.when(step == 0)
    def _():
        grad_acc[...] = grad

    @pl.when(step > 0)
    def _():
        grad_acc[...] += grad

    @pl.when(step == pl.num_programs(0) - 1)
    def _():
        grad_out[...] = grad_acc[...].astype(grad_out.dtype)


def backward_kernel(
    cot, patches, proj, prob_in, xhat, inv, gain, weights, wo,
    embed_out, bias_out, gain_out, table_out, datt, dproj, dn, branch
):
    step = pl.program_id(0)

    @pl.when(step == 0)
    def _():
        embed_out[...] = jnp.zeros_like(embed_out)
        bias_out[...] = jnp.zeros_like(bias_out)
        gain_out[...] = jnp.zeros_like(gain_out)
        table_out[...] = jnp.zeros_like(table_out)
        dproj[...] = jnp.zeros_like(dproj)

    datt[...] = dot_nt(cot[...], wo[...]).astype(jnp.bfloat16)
    for pair in range(STEP // PAIR):
        rows = slice(pair * PAIR, (pair + 1) * PAIR)
        for q_at, k_at, v_at, at, count in UNITS:
            width = count * HEAD
            masks = half_masks(count)
            q = proj[rows, q_at : q_at + width]
            k = proj[rows, k_at : k_at + width]
            v = proj[rows, v_at : v_at + width]
            d_out = datt[rows, at : at + width]
            qs, ks, vs = [], [], []
            for i in range(count):
                head = at // HEAD + i
                prob = prob_in[pair, head]
                d_prob = dot_nt(only(masks, i, d_out), v)
                vs.append(dot_tn(prob.astype(jnp.bfloat16), d_out))
                d_scores = prob * (d_prob - jnp.sum(prob * d_prob, axis=-1, keepdims=True))
                table_out[head] += d_scores
                low = d_scores.astype(jnp.bfloat16)
                qs.append(dot_nn(low, k))
                ks.append(dot_tn(low, q))
            dproj[rows, q_at : q_at + width] = (choose(masks, qs) * SCALE).astype(jnp.bfloat16)
            dproj[rows, k_at : k_at + width] = (choose(masks, ks) * SCALE).astype(jnp.bfloat16)
            dproj[rows, v_at : v_at + width] = choose(masks, vs).astype(jnp.bfloat16)
    dn[...] = dot_nt(dproj[...], weights[:, :QKV])
    chunk = 16
    width = dn.shape[1]
    gain_row = gain[0:1, :]

    def rows_at(i, carry):
        bias_sum, gain_sum = carry
        rows = pl.ds(pl.multiple_of(i * chunk, chunk), chunk)
        d, x = dn[rows, :], xhat[rows, :]
        gain_sum = gain_sum + (d * x).reshape(chunk // 8, 8, width).sum(axis=0)
        g = d * gain_row
        mean = jnp.mean(g, axis=-1, keepdims=True)
        along = jnp.mean(g * x, axis=-1, keepdims=True)
        out = (inv[rows, 0:1] * (g - mean - x * along)).astype(jnp.bfloat16)
        branch[rows, :] = out
        bias_sum = bias_sum + out.astype(jnp.float32).reshape(chunk // 8, 8, width).sum(axis=0)
        return bias_sum, gain_sum

    zero = jnp.zeros((8, width), jnp.float32)
    bias_sum, gain_sum = lax.fori_loop(0, STEP // chunk, rows_at, (zero, zero))
    bias_out[...] += bias_sum
    gain_out[...] += gain_sum
    embed_out[...] += dot_tn(patches[...], branch[...])


def stepped(shape):
    rest = len(shape) - 1
    return pl.BlockSpec(shape, lambda i: (i,) + (0,) * rest)


def whole(shape, index=None):
    index = index or (0,) * len(shape)
    return pl.BlockSpec(shape, lambda i: index)


def params():
    return pltpu.CompilerParams(
        dimension_semantics=("arbitrary",), vmem_limit_bytes=56 * 1024 * 1024
    )


def run_forward(joined, embed_w, embed_b, gain, weights, bias, lab_col, lab_row):
    cells, width = joined.shape[0], gain.shape[1]
    heads = bias.shape[0]
    features = heads * HEAD
    f32, bf16 = jnp.float32, jnp.bfloat16
    return pl.pallas_call(
        forward_kernel,
        grid=(cells // STEP,),
        in_specs=[
            stepped((STEP, width)),
            pl.BlockSpec((STEP, LANES), lambda i: (i, width // LANES)),
            whole((LANES, width)), whole((8, width)), whole((8, width)), whole(weights.shape),
            whole((heads, PAIR, PAIR)), stepped((STEP, PAIR)), stepped((STEP // PAIR, 8, PAIR)),
        ],
        out_specs=[
            stepped((STEP, QKV)), stepped((STEP // PAIR, heads, PAIR, PAIR)),
            stepped((STEP, width)), stepped((STEP, LANES)), whole((features, width)),
        ],
        out_shape=[
            jax.ShapeDtypeStruct((cells, QKV), bf16),
            jax.ShapeDtypeStruct((cells // PAIR, heads, PAIR, PAIR), f32),
            jax.ShapeDtypeStruct((cells, width), f32),
            jax.ShapeDtypeStruct((cells, LANES), f32),
            jax.ShapeDtypeStruct((features, width), bf16),
        ],
        scratch_shapes=[pltpu.VMEM((STEP, features), bf16), pltpu.VMEM((features, width), f32)],
        compiler_params=params(), name="forward",
        cost_estimate=pl.CostEstimate(
            flops=2 * cells * width * (QKV + features + LANES), transcendentals=cells * heads * PAIR,
            bytes_accessed=cells * width * 8,
        ),
    )(joined, joined, embed_w, embed_b, gain, weights, bias, lab_col, lab_row)


def run_backward(joined, proj, prob, xhat, inv, gain, weights, wo):
    cells, width = xhat.shape
    features = wo.shape[0]
    heads = features // HEAD
    f32, bf16 = jnp.float32, jnp.bfloat16
    return pl.pallas_call(
        backward_kernel,
        grid=(cells // STEP,),
        in_specs=[
            stepped((STEP, width)),
            pl.BlockSpec((STEP, LANES), lambda i: (i, width // LANES)),
            stepped((STEP, QKV)), stepped((STEP // PAIR, heads, PAIR, PAIR)),
            stepped((STEP, width)), stepped((STEP, LANES)), whole((8, width)),
            whole(weights.shape), whole((features, width)),
        ],
        out_specs=[
            whole((LANES, width)), whole((8, width)), whole((8, width)),
            whole((heads, PAIR, PAIR)),
        ],
        out_shape=[
            jax.ShapeDtypeStruct((LANES, width), f32), jax.ShapeDtypeStruct((8, width), f32),
            jax.ShapeDtypeStruct((8, width), f32), jax.ShapeDtypeStruct((heads, PAIR, PAIR), f32),
        ],
        scratch_shapes=[
            pltpu.VMEM((STEP, features), bf16), pltpu.VMEM((STEP, QKV), bf16),
            pltpu.VMEM((STEP, width), f32), pltpu.VMEM((STEP, width), bf16),
        ],
        compiler_params=params(), name="backward",
        cost_estimate=pl.CostEstimate(
            flops=2 * cells * width * (QKV + features + LANES), transcendentals=0,
            bytes_accessed=cells * width * 8,
        ),
    )(joined, joined, proj, prob, xhat, inv, gain, weights, wo)


ROW = ("yl", "x", "core")
COL = ("col", "dp")
PLANE = ("x", "core", "col")
RING = ("yl", "dp")
CHIP_ROW = ("x", "core")
FAR = ("yl", "col", "dp")


def exchange(blocks, axis):
    return lax.all_to_all(blocks, axis, split_axis=0, concat_axis=0, tiled=True)


def spread(line, axis):
    copies = jnp.broadcast_to(line[None], (lax.axis_size(axis), *line.shape))
    return exchange(copies, axis)


def from_behind(value, axis):
    count = lax.axis_size(axis)
    return lax.ppermute(value, axis, [(source, (source - 1) % count) for source in range(count)])


def swap(value, axis):
    count = lax.axis_size(axis)
    return lax.ppermute(value, axis, [(source, source ^ 1) for source in range(count)])


def make_patches(pixel_block):
    channels, pixel_rows, pixel_cols = pixel_block.shape
    grid_rows = pixel_rows // PATCH
    grid_cols = pixel_cols // PATCH
    shaped = pixel_block.reshape(channels, grid_rows, PATCH, grid_cols, PATCH)
    return shaped.transpose(1, 3, 0, 2, 4).reshape(grid_rows, grid_cols, channels * PATCH * PATCH)


def window_split(block):
    rows_all, cols_all, features = block.shape
    shaped = block.reshape(rows_all // WIN, WIN, cols_all // WIN, WIN, features)
    return shaped.transpose(0, 2, 1, 3, 4).reshape(-1, features)


def splice_after(own, borrowed, offset, dim):
    joined = jnp.concatenate([own, borrowed], dim)
    return lax.dynamic_slice_in_dim(joined, offset, own.shape[dim], dim)


def pack_out(rows):
    tall = rows[:16].reshape(16, 8, LANES).transpose(1, 0, 2).reshape(LANES, LANES)
    low = rows[16:].reshape(8, 8, LANES).transpose(1, 0, 2).reshape(64, 2, 64)
    return jnp.concatenate([low.transpose(1, 0, 2).reshape(LANES, 64), tall], axis=1)


def unpack_out(blocks):
    count = blocks.shape[0]
    tall = blocks[:, :, 64:].reshape(count, 8, 16, LANES).transpose(0, 2, 1, 3)
    low = blocks[:, :, :64].reshape(count, 2, 64, 64).transpose(0, 2, 1, 3)
    low = low.reshape(count, 8, 8, LANES).transpose(0, 2, 1, 3)
    return jnp.concatenate([tall, low], axis=1).reshape(count * 24, 8 * LANES)


def gather_weights(qkv_weight, out_weight, half, own):
    split = qkv_weight.size // LANES
    line = jnp.concatenate([qkv_weight.reshape(-1, LANES), out_weight.reshape(-1, LANES)])
    lines = spread(line, FAR)
    bands = lax.axis_size("yl")
    cols = lines.shape[0] // bands
    rows_w, rows_o = qkv_weight.shape[0], out_weight.shape[0]
    qkv = lines[:, :split].reshape(bands, cols, *qkv_weight.shape).transpose(0, 2, 1, 3)
    qkv = qkv.reshape(bands * rows_w, 3, -1)
    out = lines[:, split:].reshape(bands, cols, *out_weight.shape).transpose(0, 2, 1, 3)
    out = out.reshape(bands, rows_o, -1)
    features = qkv.shape[2]
    mine = lax.dynamic_slice_in_dim(qkv, half * (features // 2), features // 2, 2)
    out = lax.dynamic_slice_in_dim(out, half * 2, 2, 0)
    group = features // 4
    blocks = []
    for core in range(2):
        part = mine[:, :, core * group : (core + 1) * group]
        pieces = [part[:, i, :LANES] for i in range(3)] + [part[:, i, LANES:] for i in range(3)]
        blocks.append(jnp.concatenate([*pieces, pack_out(out[core])], axis=1))
    both = jnp.stack(blocks)
    chips = lax.axis_size("x")
    sent = jnp.broadcast_to(both[None], (chips, *both.shape)).reshape(2 * chips, *both.shape[1:])
    sent, own = lax.optimization_barrier((sent, own))
    arrived = exchange(sent, CHIP_ROW)
    wo = unpack_out(arrived[:, :, QKV - 64 :])
    weights = arrived.reshape(2 * chips, bands, rows_w, -1).transpose(1, 0, 2, 3)
    return weights.reshape(bands * 2 * chips * rows_w, -1), wo, own


def on_device(
    pixels,
    cotangent,
    embed_weight,
    embed_bias,
    layer_norm_gain,
    qkv_weight,
    out_weight,
    bias_table,
    rel_index,
    shifts,
):
    cotangent, pixels = cotangent[0], pixels[0]
    rows_dev, cols_dev, width = cotangent.shape
    all_heads, table_size = bias_table.shape
    heads = all_heads // 4
    grid_rows = rows_dev * lax.axis_size(ROW)
    grid_cols = cols_dev * lax.axis_size("col")
    row_shift, col_shift = shifts[0, 0], shifts[0, 1]
    row_at, col_at, core = lax.axis_index(ROW), lax.axis_index("col"), lax.axis_index("core")
    half = col_at % 2
    group = 2 * half + core

    depth = embed_weight.shape[0]
    patches = make_patches(pixels)
    patches = jnp.pad(patches, ((0, 0), (0, 0), (0, LANES - depth)))
    block = jnp.concatenate([cotangent, patches], axis=-1)
    below = from_behind(block[: WIN - 1], ROW)
    block = splice_after(block, below, row_shift, 0)
    block = splice_after(block, from_behind(block[:, :WIN], "col"), col_shift, 1)
    weights, wo, own = gather_weights(qkv_weight, out_weight, half, window_split(block))
    two = jnp.concatenate([own, swap(own, "col")])
    joined = jnp.concatenate([two, swap(two, "core")])
    cells = joined.shape[0]

    labels = []
    for row_flip, col_flip in ((0, 0), (0, 1), (1, 0), (1, 1)):
        row_ids = (row_at ^ row_flip) * rows_dev + jnp.arange(rows_dev, dtype=jnp.int32)
        col_ids = (col_at ^ col_flip) * cols_dev + jnp.arange(cols_dev, dtype=jnp.int32)
        row_part = (row_ids >= grid_rows - row_shift).astype(jnp.int32)
        col_part = (col_ids >= grid_cols - col_shift).astype(jnp.int32)
        region = 2 * row_part[:, None] + col_part[None, :]
        labels.append(window_split(region[:, :, None])[:, 0])
    label = jnp.concatenate(labels) + 4 * (jnp.arange(cells, dtype=jnp.int32) // CELLS)
    lab_col = jnp.broadcast_to(label[:, None], (cells, PAIR))
    lab_row = jnp.broadcast_to(label.reshape(-1, 1, PAIR), (cells // PAIR, 8, PAIR))
    selector = (
        rel_index.reshape(-1)[:, None] == jnp.arange(table_size, dtype=jnp.int32)[None, :]
    ).astype(jnp.float32)
    my_table = lax.dynamic_slice_in_dim(bias_table, group * heads, heads, 0)
    bias = jnp.dot(selector, my_table.T, precision=lax.Precision.HIGHEST).T
    bias = jnp.tile(bias.reshape(heads, CELLS, CELLS), (1, 2, 2))
    embed_w = jnp.pad(embed_weight, ((0, LANES - depth), (0, 0)))
    embed_b = jnp.broadcast_to(embed_bias[None], (8, width))
    gain = jnp.broadcast_to(layer_norm_gain[None], (8, width))
    contract = (((0,), (0,)), ((), ()))
    cot_own, patches_own = own[:, :width], own[:, width:]
    embed_cot = lax.dot_general(patches_own, cot_own, contract, preferred_element_type=jnp.float32)
    bias_cot = jnp.sum(cot_own, axis=0, dtype=jnp.float32)

    proj, prob, xhat, inv, out_grad = run_forward(
        joined, embed_w, embed_b, gain, weights, bias, lab_col, lab_row
    )
    count = lax.axis_size(CHIP_ROW)
    arrived = exchange(out_grad.reshape(count, -1, width), CHIP_ROW)
    embed_part, bias_part, gain_part, table_part = run_backward(
        joined, proj, prob, xhat, inv, gain, weights, wo
    )
    embed_grad = (embed_part + embed_cot)[:depth]
    bias_grad = bias_part.sum(axis=0) + bias_cot
    gain_grad = gain_part.sum(axis=0)
    table_part = table_part[:, :CELLS, :CELLS] + table_part[:, CELLS:, CELLS:]
    my_grad = jnp.dot(table_part.reshape(heads, -1), selector, precision=lax.Precision.HIGHEST)
    table_grad = lax.dynamic_update_slice_in_dim(
        jnp.zeros((all_heads, table_size), jnp.float32), my_grad, group * heads, 0
    )

    pieces = [embed_grad.reshape(-1), bias_grad, gain_grad, table_grad.reshape(-1)]
    line = jnp.concatenate(pieces)
    plane, ring, deep = lax.axis_size(PLANE), lax.axis_size(RING), lax.axis_size("col")
    piece = -(-line.size // (plane * 1024)) * 1024
    tiles = piece // LANES
    line = jnp.pad(line, (0, plane * piece - line.size)).astype(jnp.bfloat16)
    line, arrived = lax.optimization_barrier((line, arrived))
    mine = exchange(line.reshape(plane, tiles, LANES), PLANE)
    mine = mine.astype(jnp.float32).sum(axis=0).astype(jnp.bfloat16)
    held = arrived.reshape(count // 2, 2, -1, width).astype(jnp.float32).sum(axis=0)
    held = held.astype(jnp.bfloat16)
    owned = held.shape[1]
    held = held.reshape(2, owned, deep, ring // 4, -1).transpose(0, 3, 2, 1, 4)
    held = held.reshape(2, ring // 4, -1, LANES)
    none = jnp.zeros_like(held)
    bands = jnp.concatenate([jnp.where(half == i, held, none) for i in range(2)])
    bands = bands.reshape(ring, -1, LANES)
    mine = jnp.broadcast_to(mine[None], (ring, tiles, LANES))
    both = exchange(jnp.concatenate([mine, bands], axis=1), RING)
    both = both.astype(jnp.float32).sum(axis=0).astype(jnp.bfloat16)
    mine = jnp.broadcast_to(both[None, :tiles], (plane, tiles, LANES))
    bands = both[tiles:].reshape(1, deep, -1, LANES)
    place = lax.axis_index(CHIP_ROW)
    here = jnp.arange(plane // deep, dtype=jnp.int32)[:, None, None, None] == place
    bands = jnp.where(here, bands, jnp.zeros_like(bands)).reshape(plane, -1, LANES)
    total = exchange(jnp.concatenate([mine, bands], axis=1), PLANE).astype(jnp.float32)
    out_weight_grad = total[:, tiles:].sum(axis=0).reshape(owned, -1)
    total = total[:, :tiles].reshape(-1)
    results, at = ([], 0)
    for a, shape in zip(pieces, (embed_grad.shape, (width,), (width,), table_grad.shape)):
        results.append(total[at : at + a.size].reshape(shape))
        at += a.size
    return (out_weight_grad, *results)


def solution(mesh):
    sizes = mesh.devices.shape
    names = ("yl", "x", "core", "col", "dp")
    fine = Mesh(mesh.devices.reshape(-1, 4, 2, *sizes[1:]), names)
    return jax.shard_map(
        on_device,
        mesh=fine,
        in_specs=(
            P("dp", None, ROW, "col"),
            P("dp", ROW, "col", None),
            P(),
            P(),
            P(),
            P(ROW, COL),
            P(ROW, COL),
            P(),
            P(),
            P("dp", None),
        ),
        out_specs=(P(ROW, COL), P(), P(), P(), P()),
        check_vma=False,
    )
```

```python
import jax
import jax.numpy as jnp
from jax import lax
from jax.experimental import pallas as pl
from jax.experimental.pallas import tpu as pltpu
from jax.sharding import Mesh, PartitionSpec as P

WIN = 8
PATCH = 4
CELLS = WIN * WIN
norm_epsilon = 1e-05

STEP = 256
PAIR = 128
HEAD = 64
LANES = 128
SCALE = HEAD ** (-0.5)
UNITS = ((0, 128, 256, 0, 2), (384, 448, 512, 128, 1))
QKV = 640


def dot_nn(a, b):
    return lax.dot_general(a, b, (((1,), (0,)), ((), ())), preferred_element_type=jnp.float32)


def dot_nt(a, b):
    return lax.dot_general(a, b, (((1,), (1,)), ((), ())), preferred_element_type=jnp.float32)


def dot_tn(a, b):
    return lax.dot_general(a, b, (((0,), (0,)), ((), ())), preferred_element_type=jnp.float32)


def half_masks(count):
    lane = lax.broadcasted_iota(jnp.int32, (PAIR, count * HEAD), 1)
    return [(lane // HEAD) == i for i in range(count)]


def choose(masks, parts):
    return parts[0] if len(parts) == 1 else jnp.where(masks[0], parts[0], parts[1])


def only(masks, i, x):
    return x if len(masks) == 1 else jnp.where(masks[i], x, jnp.zeros_like(x))


def work():
    for pair in range(STEP // PAIR):
        for unit in UNITS:
            yield (pair, slice(pair * PAIR, (pair + 1) * PAIR), *unit)


def assemble(arrived, out):
    sources, rows, _ = arrived.shape
    band = rows // 4
    for source in range(sources):
        for i in range(4):
            at = (i * sources + source) * band
            out[at : at + band, :] = arrived[source, i * band : (i + 1) * band, :QKV]


def assemble_out(arrived, wide, out):
    sources = arrived.shape[0]
    for source in range(sources):
        at = source * 24
        for tile in range(8):
            cols = slice(tile * LANES, (tile + 1) * LANES)
            tall = arrived[source, tile * 16 : (tile + 1) * 16, QKV:]
            wide[at : at + 16, cols] = tall.astype(jnp.float32)
            low = [
                arrived[source, i * 64 + tile * 8 : i * 64 + tile * 8 + 8, QKV - 64 : QKV]
                for i in range(2)
            ]
            wide[at + 16 : at + 24, cols] = jnp.concatenate(low, axis=1).astype(jnp.float32)
    out[...] = wide[...].astype(jnp.bfloat16)


def forward_kernel(
    two, other, embed_w, embed_b, gain, arrived, bias, label,
    proj_out, prob_out, xhat_out, inv_out, grad_out, weights, bias_pair, scores, att, grad_acc
):
    step = pl.program_id(0)
    width = gain.shape[1]

    @pl.when(step == 0)
    def _():
        assemble(arrived, weights)
        for head in range(bias.shape[0]):
            row = jnp.concatenate([bias[head], bias[head]], axis=1)
            bias_pair[head] = jnp.concatenate([row, row], axis=0)

    cells = jnp.where(step < 2, two[...], other[...])
    cot = cells[:, :width]
    tokens = dot_nn(cells[:, width:], embed_w[...]) + embed_b[...]
    tokens = tokens.astype(jnp.bfloat16).astype(jnp.float32)
    centered = tokens - jnp.mean(tokens, axis=-1, keepdims=True)
    inv = lax.rsqrt(jnp.mean(centered * centered, axis=-1, keepdims=True) + norm_epsilon)
    xhat = centered * inv
    xhat_out[...] = xhat
    inv_out[...] = jnp.broadcast_to(inv, inv_out.shape)
    normed = (xhat * gain[...]).astype(jnp.bfloat16)
    proj_out[...] = dot_nn(normed, weights[...]).astype(jnp.bfloat16)
    heads = bias.shape[0]
    for pair, rows, q_at, k_at, v_at, at, count in work():
        q = proj_out[rows, q_at : q_at + count * HEAD]
        k = proj_out[rows, k_at : k_at + count * HEAD]
        for i in range(count):
            scores[pair * heads + at // HEAD + i] = dot_nt(only(half_masks(count), i, q), k)
    for pair in range(STEP // PAIR):
        line = label[pl.ds(step * (STEP // PAIR) + pair, 1), :]
        wide = jnp.broadcast_to(line, (PAIR, PAIR))
        same = wide == wide.T
        for head in range(heads):
            values = scores[pair * heads + head] * SCALE + bias_pair[head]
            values = jnp.where(same, values, -1e30)
            e = jnp.exp(values - jnp.max(values, axis=-1, keepdims=True))
            prob_out[pair, head] = e * (1.0 / jnp.sum(e, axis=-1, keepdims=True))
    for pair, rows, q_at, k_at, v_at, at, count in work():
        v = proj_out[rows, v_at : v_at + count * HEAD]
        parts = [
            dot_nn(prob_out[pair, at // HEAD + i].astype(jnp.bfloat16), v) for i in range(count)
        ]
        att[rows, at : at + count * HEAD] = choose(half_masks(count), parts).astype(jnp.bfloat16)
    grad = dot_tn(att[...], cot)

    @pl.when(step == 0)
    def _():
        grad_acc[...] = grad

    @pl.when(step > 0)
    def _():
        grad_acc[...] += grad

    @pl.when(step == pl.num_programs(0) - 1)
    def _():
        grad_out[...] = grad_acc[...].astype(grad_out.dtype)


def scores_kernel(
    two, other, proj, prob_in, arrived, dproj, table_out, wide, wo, table, datt, d_probs, lows
):
    step = pl.program_id(0)
    width = wo.shape[1]
    heads = prob_in.shape[1]

    @pl.when(step == 0)
    def _():
        assemble_out(arrived, wide, wo)
        table[...] = jnp.zeros_like(table)

    cot = jnp.where(step < 2, two[:, :width], other[:, :width])
    datt[...] = dot_nt(cot, wo[...]).astype(jnp.bfloat16)
    dproj[:, QKV - HEAD :] = jnp.zeros((STEP, HEAD), jnp.bfloat16)
    for pair, rows, q_at, k_at, v_at, at, count in work():
        v = proj[rows, v_at : v_at + count * HEAD]
        d_out = datt[rows, at : at + count * HEAD]
        for i in range(count):
            d_probs[pair * heads + at // HEAD + i] = dot_nt(only(half_masks(count), i, d_out), v)
    for head in range(heads):
        total = table[head]
        for pair in range(STEP // PAIR):
            prob, d_prob = prob_in[pair, head], d_probs[pair * heads + head]
            weighted = prob * d_prob
            d_scores = weighted - prob * jnp.sum(weighted, axis=-1, keepdims=True)
            total = total + d_scores
            lows[pair * heads + head] = d_scores.astype(jnp.bfloat16)
        table[head] = total
    for pair, rows, q_at, k_at, v_at, at, count in work():
        width_in = count * HEAD
        masks = half_masks(count)
        q = proj[rows, q_at : q_at + width_in]
        k = proj[rows, k_at : k_at + width_in]
        d_out = datt[rows, at : at + width_in]
        qs, ks, vs = [], [], []
        for i in range(count):
            head = at // HEAD + i
            low = lows[pair * heads + head]
            qs.append(dot_nn(low, k))
            ks.append(dot_tn(low, q))
            vs.append(dot_tn(prob_in[pair, head].astype(jnp.bfloat16), d_out))
        dproj[rows, q_at : q_at + width_in] = (choose(masks, qs) * SCALE).astype(jnp.bfloat16)
        dproj[rows, k_at : k_at + width_in] = (choose(masks, ks) * SCALE).astype(jnp.bfloat16)
        dproj[rows, v_at : v_at + width_in] = choose(masks, vs).astype(jnp.bfloat16)

    @pl.when(step == pl.num_programs(0) - 1)
    def _():
        for head in range(heads):
            full = table[head]
            table_out[head] = full[:CELLS, :CELLS] + full[CELLS:, CELLS:]


def norm_kernel(
    two, other, dproj, xhat, inv, gain, arrived, line_out, weights, dn, branch, embed, bias, gains
):
    step = pl.program_id(0)
    width = gain.shape[1]
    chunk = 32
    cells = jnp.where(step < 2, two[...], other[...])
    patches = cells[:, width:]

    @pl.when(step == 0)
    def _():
        assemble(arrived, weights)
        cot = cells[:, :width]
        embed[...] = dot_tn(patches, cot)
        bias[...] = cot.astype(jnp.float32).reshape(STEP // 8, 8, width).sum(axis=0)
        gains[...] = jnp.zeros_like(gains)

    dn[...] = dot_nt(dproj[...], weights[...])
    bias_sum, gain_sum = bias[...], gains[...]
    for i in range(STEP // chunk):
        rows = slice(i * chunk, (i + 1) * chunk)
        d, x = dn[rows, :], xhat[rows, :]
        gain_sum = gain_sum + (d * x).reshape(chunk // 8, 8, width).sum(axis=0)
        g = d * gain[...]
        mean = jnp.mean(g, axis=-1, keepdims=True)
        along = jnp.mean(g * x, axis=-1, keepdims=True)
        out = (inv[rows, 0:1] * (g - mean - x * along)).astype(jnp.bfloat16)
        branch[rows, :] = out
        bias_sum = bias_sum + out.astype(jnp.float32).reshape(chunk // 8, 8, width).sum(axis=0)
    bias[...] = bias_sum
    gains[...] = gain_sum
    embed[...] += dot_tn(patches, branch[...])

    @pl.when(step == pl.num_programs(0) - 1)
    def _():
        depth = 48
        line_out[:depth, :] = embed[:depth, :].astype(line_out.dtype)
        row = lax.broadcasted_iota(jnp.int32, (16, width), 0)
        sums = jnp.where(row == 0, jnp.sum(bias[...], axis=0, keepdims=True), 0.0)
        sums = jnp.where(row == 1, jnp.sum(gains[...], axis=0, keepdims=True), sums)
        line_out[depth:, :] = sums.astype(line_out.dtype)


def stepped(shape):
    rest = len(shape) - 1
    return pl.BlockSpec(shape, lambda i: (i,) + (0,) * rest)


def whole(shape):
    return pl.BlockSpec(shape, lambda i: (0,) * len(shape))


def cell_specs(width):
    return [
        pl.BlockSpec((STEP, width), lambda i: (jnp.minimum(i, 1), 0)),
        pl.BlockSpec((STEP, width), lambda i: (jnp.maximum(i - 2, 0), 0)),
    ]


def call(kernel, cells, in_specs, out_specs, out_shape, scratch, flops):
    return pl.pallas_call(
        kernel,
        grid=(cells // STEP,),
        in_specs=in_specs,
        out_specs=out_specs,
        out_shape=out_shape,
        scratch_shapes=scratch,
        compiler_params=pltpu.CompilerParams(
            dimension_semantics=("arbitrary",), vmem_limit_bytes=56 * 1024 * 1024
        ),
        cost_estimate=pl.CostEstimate(flops=flops, transcendentals=0, bytes_accessed=8 << 20),
    )


def run_forward(two, other, embed_w, embed_b, gain, arrived, bias, label):
    cells, width = 2 * two.shape[0], gain.shape[1]
    heads = bias.shape[0]
    features = heads * HEAD
    units = heads * (STEP // PAIR)
    f32, bf16 = jnp.float32, jnp.bfloat16
    return call(
        forward_kernel, cells,
        [
            *cell_specs(two.shape[1]), whole((LANES, width)), whole((1, width)), whole((1, width)),
            whole(arrived.shape), whole(bias.shape), whole(label.shape),
        ],
        [
            stepped((STEP, QKV)), stepped((STEP // PAIR, heads, PAIR, PAIR)),
            stepped((STEP, width)), stepped((STEP, LANES)), whole((features, width)),
        ],
        [
            jax.ShapeDtypeStruct((cells, QKV), bf16),
            jax.ShapeDtypeStruct((cells // PAIR, heads, PAIR, PAIR), f32),
            jax.ShapeDtypeStruct((cells, width), f32),
            jax.ShapeDtypeStruct((cells, LANES), f32),
            jax.ShapeDtypeStruct((features, width), bf16),
        ],
        [
            pltpu.VMEM((width, QKV), bf16), pltpu.VMEM((heads, PAIR, PAIR), f32),
            pltpu.VMEM((units, PAIR, PAIR), f32), pltpu.VMEM((STEP, features), bf16),
            pltpu.VMEM((features, width), f32),
        ],
        4 << 30,
    )(two, other, embed_w, embed_b, gain, arrived, bias, label)


def run_scores(two, other, proj, prob, arrived, width):
    cells = proj.shape[0]
    heads = prob.shape[1]
    features = heads * HEAD
    units = heads * (STEP // PAIR)
    f32, bf16 = jnp.float32, jnp.bfloat16
    return call(
        scores_kernel, cells,
        [
            *cell_specs(two.shape[1]), stepped((STEP, QKV)),
            stepped((STEP // PAIR, heads, PAIR, PAIR)), whole(arrived.shape),
        ],
        [stepped((STEP, QKV)), whole((heads, CELLS, CELLS))],
        [
            jax.ShapeDtypeStruct((cells, QKV), bf16),
            jax.ShapeDtypeStruct((heads, CELLS, CELLS), f32),
        ],
        [
            pltpu.VMEM((features, width), f32), pltpu.VMEM((features, width), bf16),
            pltpu.VMEM((heads, PAIR, PAIR), f32), pltpu.VMEM((STEP, features), bf16),
            pltpu.VMEM((units, PAIR, PAIR), f32), pltpu.VMEM((units, PAIR, PAIR), bf16),
        ],
        4 << 30,
    )(two, other, proj, prob, arrived)


def run_norm(two, other, dproj, xhat, inv, gain, arrived):
    cells, width = xhat.shape
    f32, bf16 = jnp.float32, jnp.bfloat16
    return call(
        norm_kernel, cells,
        [
            *cell_specs(two.shape[1]), stepped((STEP, QKV)), stepped((STEP, width)),
            stepped((STEP, LANES)), whole((1, width)), whole(arrived.shape),
        ],
        whole((64, width)),
        jax.ShapeDtypeStruct((64, width), bf16),
        [
            pltpu.VMEM((width, QKV), bf16), pltpu.VMEM((STEP, width), f32),
            pltpu.VMEM((STEP, width), bf16), pltpu.VMEM((LANES, width), f32),
            pltpu.VMEM((8, width), f32), pltpu.VMEM((8, width), f32),
        ],
        4 << 30,
    )(two, other, dproj, xhat, inv, gain, arrived)


ROW = ("yl", "x", "core")
COL = ("col", "dp")
CHIP_ROW = ("x", "core")
FAR = ("yl", "col", "dp")


def exchange(blocks, axis):
    return lax.all_to_all(blocks, axis, split_axis=0, concat_axis=0, tiled=True)


def spread(line, axis):
    copies = jnp.broadcast_to(line[None], (lax.axis_size(axis), *line.shape))
    return exchange(copies, axis)


def from_behind(value, axis):
    count = lax.axis_size(axis)
    return lax.ppermute(value, axis, [(source, (source - 1) % count) for source in range(count)])


def swap(value, axis):
    count = lax.axis_size(axis)
    return lax.ppermute(value, axis, [(source, source ^ 1) for source in range(count)])


def make_patches(pixel_block):
    channels, pixel_rows, pixel_cols = pixel_block.shape
    grid_rows = pixel_rows // PATCH
    grid_cols = pixel_cols // PATCH
    shaped = pixel_block.reshape(channels, grid_rows, PATCH, grid_cols, PATCH)
    return shaped.transpose(1, 3, 0, 2, 4).reshape(grid_rows, grid_cols, channels * PATCH * PATCH)


def window_split(block):
    rows_all, cols_all, features = block.shape
    shaped = block.reshape(rows_all // WIN, WIN, cols_all // WIN, WIN, features)
    return shaped.transpose(0, 2, 1, 3, 4).reshape(-1, features)


def splice_after(own, borrowed, offset, dim):
    joined = jnp.concatenate([own, borrowed], dim)
    return lax.dynamic_slice_in_dim(joined, offset, own.shape[dim], dim)


def pack_out(rows):
    tall = rows[:16].reshape(16, 8, LANES).transpose(1, 0, 2).reshape(LANES, LANES)
    low = rows[16:].reshape(8, 8, LANES).transpose(1, 0, 2).reshape(64, 2, 64)
    return jnp.concatenate([low.transpose(1, 0, 2).reshape(LANES, 64), tall], axis=1)


def gather_weights(qkv_weight, out_weight, half, own):
    split = qkv_weight.size // LANES
    line = jnp.concatenate([qkv_weight.reshape(-1, LANES), out_weight.reshape(-1, LANES)])
    lines = spread(line, FAR)
    bands = lax.axis_size("yl")
    cols = lines.shape[0] // bands
    rows_w, rows_o = qkv_weight.shape[0], out_weight.shape[0]
    qkv = lines[:, :split].reshape(bands, cols, *qkv_weight.shape).transpose(0, 2, 1, 3)
    qkv = qkv.reshape(bands * rows_w, 3, -1)
    out = lines[:, split:].reshape(bands, cols, *out_weight.shape).transpose(0, 2, 1, 3)
    out = out.reshape(bands, rows_o, -1)
    features = qkv.shape[2]
    mine = lax.dynamic_slice_in_dim(qkv, half * (features // 2), features // 2, 2)
    out = lax.dynamic_slice_in_dim(out, half * 2, 2, 0)
    group = features // 4
    blocks = []
    for core in range(2):
        part = mine[:, :, core * group : (core + 1) * group]
        pieces = [part[:, i, :LANES] for i in range(3)] + [part[:, i, LANES:] for i in range(3)]
        blocks.append(jnp.concatenate([*pieces, pack_out(out[core])], axis=1))
    both = jnp.stack(blocks)
    chips = lax.axis_size("x")
    sent = jnp.broadcast_to(both[None], (chips, *both.shape)).reshape(2 * chips, *both.shape[1:])
    sent, own = lax.optimization_barrier((sent, own))
    arrived = exchange(sent, CHIP_ROW)
    return arrived, own


def on_device(
    pixels,
    cotangent,
    embed_weight,
    embed_bias,
    layer_norm_gain,
    qkv_weight,
    out_weight,
    bias_table,
    rel_index,
    shifts,
):
    cotangent, pixels = cotangent[0], pixels[0]
    rows_dev, cols_dev, width = cotangent.shape
    all_heads, table_size = bias_table.shape
    heads = all_heads // 4
    grid_rows = rows_dev * lax.axis_size(ROW)
    grid_cols = cols_dev * lax.axis_size("col")
    row_shift, col_shift = shifts[0, 0], shifts[0, 1]
    row_at, col_at, core = lax.axis_index(ROW), lax.axis_index("col"), lax.axis_index("core")
    half = col_at % 2
    group = 2 * half + core

    depth = embed_weight.shape[0]
    patches = make_patches(pixels)
    patches = jnp.pad(patches, ((0, 0), (0, 0), (0, LANES - depth)))
    block = jnp.concatenate([cotangent, patches], axis=-1)
    below = from_behind(block[: WIN - 1], ROW)
    block = splice_after(block, below, row_shift, 0)
    block = splice_after(block, from_behind(block[:, :WIN], "col"), col_shift, 1)
    arrived, own = gather_weights(qkv_weight, out_weight, half, window_split(block))
    beside = swap(own, "col")
    two = jnp.concatenate([own, beside])
    other = swap(two, "core")
    cells = 2 * two.shape[0]

    labels = []
    for row_flip, col_flip in ((0, 0), (0, 1), (1, 0), (1, 1)):
        row_ids = (row_at ^ row_flip) * rows_dev + jnp.arange(rows_dev, dtype=jnp.int32)
        col_ids = (col_at ^ col_flip) * cols_dev + jnp.arange(cols_dev, dtype=jnp.int32)
        row_part = (row_ids >= grid_rows - row_shift).astype(jnp.int32)
        col_part = (col_ids >= grid_cols - col_shift).astype(jnp.int32)
        region = 2 * row_part[:, None] + col_part[None, :]
        labels.append(window_split(region[:, :, None])[:, 0])
    label = jnp.concatenate(labels) + 4 * (jnp.arange(cells, dtype=jnp.int32) // CELLS)
    label = label.astype(jnp.float32).reshape(-1, PAIR)
    selector = (
        rel_index.reshape(-1)[:, None] == jnp.arange(table_size, dtype=jnp.int32)[None, :]
    ).astype(jnp.float32)
    my_table = lax.dynamic_slice_in_dim(bias_table, group * heads, heads, 0)
    bias = jnp.dot(selector, my_table.T, precision=lax.Precision.HIGHEST).T
    bias = bias.reshape(heads, CELLS, CELLS)
    embed_w = jnp.pad(embed_weight, ((0, LANES - depth), (0, 0)))
    gain = layer_norm_gain[None]

    proj, prob, xhat, inv, out_grad = run_forward(
        two, other, embed_w, embed_bias[None], gain, arrived, bias, label
    )
    count = lax.axis_size(CHIP_ROW)
    held = exchange(out_grad.reshape(count, -1, width), CHIP_ROW)
    dproj, table_part = run_scores(two, other, proj, prob, arrived, width)
    held = held.reshape(count // 2, 2, -1, width).astype(jnp.float32).sum(axis=0)
    held = held.astype(jnp.bfloat16)
    none = jnp.zeros_like(held)
    bands = jnp.concatenate([jnp.where(half == i, held, none) for i in range(2)])
    bands = exchange(bands, "yl")
    line = run_norm(two, other, dproj, xhat, inv, gain, arrived)
    my_grad = jnp.dot(table_part.reshape(heads, -1), selector, precision=lax.Precision.HIGHEST)
    wide = 256
    my_grad = jnp.pad(my_grad, ((0, 0), (0, wide - table_size)))
    table_grad = lax.dynamic_update_slice_in_dim(
        jnp.zeros((all_heads, wide), jnp.float32), my_grad, group * heads, 0
    )
    table_rows = table_grad.astype(jnp.bfloat16).reshape(-1, width)
    line = lax.dynamic_update_slice(line, table_rows, (depth + 2, 0))
    line, bands = lax.optimization_barrier((line, bands))
    chunks = lax.axis_size(ROW)
    tall = line.shape[0]
    tiles = line.reshape(tall // 8, 8, width // LANES, LANES).transpose(0, 2, 1, 3)
    tiles = tiles.reshape(chunks, -1, LANES)
    mine = exchange(tiles, ROW)
    mine = mine.astype(jnp.float32).sum(axis=0).astype(jnp.bfloat16)
    rows_o = bands.shape[1]
    bands = bands.astype(jnp.float32).sum(axis=0).astype(jnp.bfloat16)
    spans = lax.axis_size(COL)
    bands = bands.reshape(rows_o, spans, -1).transpose(1, 0, 2).reshape(spans, -1, LANES)
    held = mine.shape[0]
    mine = jnp.broadcast_to(mine[None], (spans, held, LANES))
    both = exchange(jnp.concatenate([mine, bands], axis=1), COL)
    both = both.astype(jnp.float32).sum(axis=0)
    out_weight_grad = both[held:].reshape(rows_o, -1)
    total = spread(both[:held].astype(jnp.bfloat16), ROW)
    total = total.reshape(tall // 8, width // LANES, 8, LANES).transpose(0, 2, 1, 3)
    total = total.reshape(tall, width).astype(jnp.float32)
    table_grad = total[depth + 2 : depth + 5].reshape(all_heads, wide)[:, :table_size]
    return (out_weight_grad, total[:depth], total[depth], total[depth + 1], table_grad)


def solution(mesh):
    sizes = mesh.devices.shape
    names = ("yl", "x", "core", "col", "dp")
    fine = Mesh(mesh.devices.reshape(-1, 4, 2, *sizes[1:]), names)
    return jax.shard_map(
        on_device,
        mesh=fine,
        in_specs=(
            P("dp", None, ROW, "col"),
            P("dp", ROW, "col", None),
            P(),
            P(),
            P(),
            P(ROW, COL),
            P(ROW, COL),
            P(),
            P(),
            P("dp", None),
        ),
        out_specs=(P(ROW, COL), P(), P(), P(), P()),
        check_vma=False,
    )
```

```python
import jax
import jax.numpy as jnp
from jax import lax
from jax.experimental import pallas as pl
from jax.experimental.pallas import tpu as pltpu
from jax.sharding import Mesh, PartitionSpec as P

WIN = 8
PATCH = 4
CELLS = WIN * WIN
norm_epsilon = 1e-05

STEP = 256
PAIR = 128
HEAD = 64
LANES = 128
SCALE = HEAD ** (-0.5)
UNITS = ((0, 128, 256, 0, 2), (384, 448, 512, 128, 1))
QKV = 640


def dot_nn(a, b):
    return lax.dot_general(a, b, (((1,), (0,)), ((), ())), preferred_element_type=jnp.float32)


def dot_nt(a, b):
    return lax.dot_general(a, b, (((1,), (1,)), ((), ())), preferred_element_type=jnp.float32)


def dot_tn(a, b):
    return lax.dot_general(a, b, (((0,), (0,)), ((), ())), preferred_element_type=jnp.float32)


def half_masks(count):
    lane = lax.broadcasted_iota(jnp.int32, (PAIR, count * HEAD), 1)
    return [(lane // HEAD) == i for i in range(count)]


def choose(masks, parts):
    return parts[0] if len(parts) == 1 else jnp.where(masks[0], parts[0], parts[1])


def only(masks, i, x):
    return x if len(masks) == 1 else jnp.where(masks[i], x, jnp.zeros_like(x))


def work():
    for pair in range(STEP // PAIR):
        for unit in UNITS:
            yield (pair, slice(pair * PAIR, (pair + 1) * PAIR), *unit)


def assemble(arrived, out):
    sources, rows, _ = arrived.shape
    band = rows // 4
    for source in range(sources):
        for i in range(4):
            at = (i * sources + source) * band
            out[at : at + band, :] = arrived[source, i * band : (i + 1) * band, :QKV]


def assemble_out(arrived, wide, out):
    sources = arrived.shape[0]
    for source in range(sources):
        at = source * 24
        for tile in range(8):
            cols = slice(tile * LANES, (tile + 1) * LANES)
            tall = arrived[source, tile * 16 : (tile + 1) * 16, QKV:]
            wide[at : at + 16, cols] = tall.astype(jnp.float32)
            low = [
                arrived[source, i * 64 + tile * 8 : i * 64 + tile * 8 + 8, QKV - 64 : QKV]
                for i in range(2)
            ]
            wide[at + 16 : at + 24, cols] = jnp.concatenate(low, axis=1).astype(jnp.float32)
    out[...] = wide[...].astype(jnp.bfloat16)


def tokens_kernel(two, other, embed_w, embed_b, gain, normed_out, xhat_out, inv_out):
    step = pl.program_id(0)
    patches = jnp.where(step < 2, two[...], other[...])
    tokens = dot_nn(patches, embed_w[...]) + embed_b[...]
    tokens = tokens.astype(jnp.bfloat16).astype(jnp.float32)
    centered = tokens - jnp.mean(tokens, axis=-1, keepdims=True)
    inv = lax.rsqrt(jnp.mean(centered * centered, axis=-1, keepdims=True) + norm_epsilon)
    xhat = centered * inv
    xhat_out[...] = xhat
    inv_out[...] = jnp.broadcast_to(inv, inv_out.shape)
    normed_out[...] = (xhat * gain[...]).astype(jnp.bfloat16)


def forward_kernel(
    two, other, normed, arrived, bias, label,
    proj_out, prob_out, grad_out, weights, bias_pair, scores, att, grad_acc
):
    step = pl.program_id(0)

    @pl.when(step == 0)
    def _():
        assemble(arrived, weights)
        for head in range(bias.shape[0]):
            row = jnp.concatenate([bias[head], bias[head]], axis=1)
            bias_pair[head] = jnp.concatenate([row, row], axis=0)

    cot = jnp.where(step < 2, two[...], other[...])
    proj_out[...] = dot_nn(normed[...], weights[...]).astype(jnp.bfloat16)
    heads = bias.shape[0]
    for pair, rows, q_at, k_at, v_at, at, count in work():
        q = proj_out[rows, q_at : q_at + count * HEAD]
        k = proj_out[rows, k_at : k_at + count * HEAD]
        for i in range(count):
            scores[pair * heads + at // HEAD + i] = dot_nt(only(half_masks(count), i, q), k)
    for pair in range(STEP // PAIR):
        line = label[pl.ds(step * (STEP // PAIR) + pair, 1), :]
        wide = jnp.broadcast_to(line, (PAIR, PAIR))
        same = wide == wide.T
        for head in range(heads):
            values = scores[pair * heads + head] * SCALE + bias_pair[head]
            values = jnp.where(same, values, -1e30)
            e = jnp.exp(values - jnp.max(values, axis=-1, keepdims=True))
            prob_out[pair, head] = e * (1.0 / jnp.sum(e, axis=-1, keepdims=True))
    for pair, rows, q_at, k_at, v_at, at, count in work():
        v = proj_out[rows, v_at : v_at + count * HEAD]
        parts = [
            dot_nn(prob_out[pair, at // HEAD + i].astype(jnp.bfloat16), v) for i in range(count)
        ]
        att[rows, at : at + count * HEAD] = choose(half_masks(count), parts).astype(jnp.bfloat16)
    grad = dot_tn(att[...], cot)

    @pl.when(step == 0)
    def _():
        grad_acc[...] = grad

    @pl.when(step > 0)
    def _():
        grad_acc[...] += grad

    @pl.when(step == pl.num_programs(0) - 1)
    def _():
        grad_out[...] = grad_acc[...].astype(grad_out.dtype)


def scores_kernel(
    two, other, proj, prob_in, arrived, dproj, table_out, wide, wo, table, datt, d_probs, lows
):
    step = pl.program_id(0)
    heads = prob_in.shape[1]

    @pl.when(step == 0)
    def _():
        assemble_out(arrived, wide, wo)
        table[...] = jnp.zeros_like(table)

    cot = jnp.where(step < 2, two[...], other[...])
    datt[...] = dot_nt(cot, wo[...]).astype(jnp.bfloat16)
    dproj[:, QKV - HEAD :] = jnp.zeros((STEP, HEAD), jnp.bfloat16)
    for pair, rows, q_at, k_at, v_at, at, count in work():
        v = proj[rows, v_at : v_at + count * HEAD]
        d_out = datt[rows, at : at + count * HEAD]
        for i in range(count):
            d_probs[pair * heads + at // HEAD + i] = dot_nt(only(half_masks(count), i, d_out), v)
    for head in range(heads):
        total = table[head]
        for pair in range(STEP // PAIR):
            prob, d_prob = prob_in[pair, head], d_probs[pair * heads + head]
            weighted = prob * d_prob
            d_scores = weighted - prob * jnp.sum(weighted, axis=-1, keepdims=True)
            total = total + d_scores
            lows[pair * heads + head] = d_scores.astype(jnp.bfloat16)
        table[head] = total
    for pair, rows, q_at, k_at, v_at, at, count in work():
        width_in = count * HEAD
        masks = half_masks(count)
        q = proj[rows, q_at : q_at + width_in]
        k = proj[rows, k_at : k_at + width_in]
        d_out = datt[rows, at : at + width_in]
        qs, ks, vs = [], [], []
        for i in range(count):
            head = at // HEAD + i
            low = lows[pair * heads + head]
            qs.append(dot_nn(low, k))
            ks.append(dot_tn(low, q))
            vs.append(dot_tn(prob_in[pair, head].astype(jnp.bfloat16), d_out))
        dproj[rows, q_at : q_at + width_in] = (choose(masks, qs) * SCALE).astype(jnp.bfloat16)
        dproj[rows, k_at : k_at + width_in] = (choose(masks, ks) * SCALE).astype(jnp.bfloat16)
        dproj[rows, v_at : v_at + width_in] = choose(masks, vs).astype(jnp.bfloat16)

    @pl.when(step == pl.num_programs(0) - 1)
    def _():
        for head in range(heads):
            full = table[head]
            table_out[head] = full[:CELLS, :CELLS] + full[CELLS:, CELLS:]


def norm_kernel(
    two, other, dproj, xhat, inv, gain, arrived, line_out, weights, dn, branch, embed, bias, gains
):
    step = pl.program_id(0)
    width = gain.shape[1]
    chunk = 32
    cells = jnp.where(step < 2, two[...], other[...])
    patches = cells[:, width:]

    @pl.when(step == 0)
    def _():
        assemble(arrived, weights)
        cot = cells[:, :width]
        embed[...] = dot_tn(patches, cot)
        bias[...] = cot.astype(jnp.float32).reshape(STEP // 8, 8, width).sum(axis=0)
        gains[...] = jnp.zeros_like(gains)

    dn[...] = dot_nt(dproj[...], weights[...])
    bias_sum, gain_sum = bias[...], gains[...]
    for i in range(STEP // chunk):
        rows = slice(i * chunk, (i + 1) * chunk)
        d, x = dn[rows, :], xhat[rows, :]
        gain_sum = gain_sum + (d * x).reshape(chunk // 8, 8, width).sum(axis=0)
        g = d * gain[...]
        mean = jnp.mean(g, axis=-1, keepdims=True)
        along = jnp.mean(g * x, axis=-1, keepdims=True)
        out = (inv[rows, 0:1] * (g - mean - x * along)).astype(jnp.bfloat16)
        branch[rows, :] = out
        bias_sum = bias_sum + out.astype(jnp.float32).reshape(chunk // 8, 8, width).sum(axis=0)
    bias[...] = bias_sum
    gains[...] = gain_sum
    embed[...] += dot_tn(patches, branch[...])

    @pl.when(step == pl.num_programs(0) - 1)
    def _():
        depth = 48
        line_out[:depth, :] = embed[:depth, :].astype(line_out.dtype)
        row = lax.broadcasted_iota(jnp.int32, (16, width), 0)
        sums = jnp.where(row == 0, jnp.sum(bias[...], axis=0, keepdims=True), 0.0)
        sums = jnp.where(row == 1, jnp.sum(gains[...], axis=0, keepdims=True), sums)
        line_out[depth:, :] = sums.astype(line_out.dtype)


def stepped(shape):
    rest = len(shape) - 1
    return pl.BlockSpec(shape, lambda i: (i,) + (0,) * rest)


def whole(shape):
    return pl.BlockSpec(shape, lambda i: (0,) * len(shape))


def cell_specs(width, at=0):
    return [
        pl.BlockSpec((STEP, width), lambda i: (jnp.minimum(i, 1), at)),
        pl.BlockSpec((STEP, width), lambda i: (jnp.maximum(i - 2, 0), at)),
    ]


def call(kernel, cells, in_specs, out_specs, out_shape, scratch, flops):
    return pl.pallas_call(
        kernel,
        grid=(cells // STEP,),
        in_specs=in_specs,
        out_specs=out_specs,
        out_shape=out_shape,
        scratch_shapes=scratch,
        compiler_params=pltpu.CompilerParams(
            dimension_semantics=("arbitrary",), vmem_limit_bytes=56 * 1024 * 1024
        ),
        cost_estimate=pl.CostEstimate(flops=flops, transcendentals=0, bytes_accessed=8 << 20),
    )


def run_tokens(two, other, embed_w, embed_b, gain):
    cells, width = 2 * two.shape[0], gain.shape[1]
    f32, bf16 = jnp.float32, jnp.bfloat16
    return call(
        tokens_kernel, cells,
        [
            *cell_specs(LANES, width // LANES), whole((LANES, width)), whole((1, width)),
            whole((1, width)),
        ],
        [stepped((STEP, width)), stepped((STEP, width)), stepped((STEP, LANES))],
        [
            jax.ShapeDtypeStruct((cells, width), bf16),
            jax.ShapeDtypeStruct((cells, width), f32),
            jax.ShapeDtypeStruct((cells, LANES), f32),
        ],
        [],
        2 << 30,
    )(two, other, embed_w, embed_b, gain)


def run_forward(two, other, normed, arrived, bias, label):
    cells, width = normed.shape
    heads = bias.shape[0]
    features = heads * HEAD
    units = heads * (STEP // PAIR)
    f32, bf16 = jnp.float32, jnp.bfloat16
    return call(
        forward_kernel, cells,
        [
            *cell_specs(width), stepped((STEP, width)),
            whole(arrived.shape), whole(bias.shape), whole(label.shape),
        ],
        [
            stepped((STEP, QKV)), stepped((STEP // PAIR, heads, PAIR, PAIR)),
            whole((features, width)),
        ],
        [
            jax.ShapeDtypeStruct((cells, QKV), bf16),
            jax.ShapeDtypeStruct((cells // PAIR, heads, PAIR, PAIR), f32),
            jax.ShapeDtypeStruct((features, width), bf16),
        ],
        [
            pltpu.VMEM((width, QKV), bf16), pltpu.VMEM((heads, PAIR, PAIR), f32),
            pltpu.VMEM((units, PAIR, PAIR), f32), pltpu.VMEM((STEP, features), bf16),
            pltpu.VMEM((features, width), f32),
        ],
        4 << 30,
    )(two, other, normed, arrived, bias, label)


def run_scores(two, other, proj, prob, arrived, width):
    cells = proj.shape[0]
    heads = prob.shape[1]
    features = heads * HEAD
    units = heads * (STEP // PAIR)
    f32, bf16 = jnp.float32, jnp.bfloat16
    return call(
        scores_kernel, cells,
        [
            *cell_specs(width), stepped((STEP, QKV)),
            stepped((STEP // PAIR, heads, PAIR, PAIR)), whole(arrived.shape),
        ],
        [stepped((STEP, QKV)), whole((heads, CELLS, CELLS))],
        [
            jax.ShapeDtypeStruct((cells, QKV), bf16),
            jax.ShapeDtypeStruct((heads, CELLS, CELLS), f32),
        ],
        [
            pltpu.VMEM((features, width), f32), pltpu.VMEM((features, width), bf16),
            pltpu.VMEM((heads, PAIR, PAIR), f32), pltpu.VMEM((STEP, features), bf16),
            pltpu.VMEM((units, PAIR, PAIR), f32), pltpu.VMEM((units, PAIR, PAIR), bf16),
        ],
        4 << 30,
    )(two, other, proj, prob, arrived)


def run_norm(two, other, dproj, xhat, inv, gain, arrived):
    cells, width = xhat.shape
    f32, bf16 = jnp.float32, jnp.bfloat16
    return call(
        norm_kernel, cells,
        [
            *cell_specs(two.shape[1]), stepped((STEP, QKV)), stepped((STEP, width)),
            stepped((STEP, LANES)), whole((1, width)), whole(arrived.shape),
        ],
        whole((64, width)),
        jax.ShapeDtypeStruct((64, width), bf16),
        [
            pltpu.VMEM((width, QKV), bf16), pltpu.VMEM((STEP, width), f32),
            pltpu.VMEM((STEP, width), bf16), pltpu.VMEM((LANES, width), f32),
            pltpu.VMEM((8, width), f32), pltpu.VMEM((8, width), f32),
        ],
        4 << 30,
    )(two, other, dproj, xhat, inv, gain, arrived)


ROW = ("yl", "x", "core")
COL = ("col", "dp")
RING = ("yl", "dp")
CHIP_ROW = ("x", "core")
FAR = ("yl", "col", "dp")


def exchange(blocks, axis):
    return lax.all_to_all(blocks, axis, split_axis=0, concat_axis=0, tiled=True)


def spread(line, axis):
    copies = jnp.broadcast_to(line[None], (lax.axis_size(axis), *line.shape))
    return exchange(copies, axis)


def from_behind(value, axis):
    count = lax.axis_size(axis)
    return lax.ppermute(value, axis, [(source, (source - 1) % count) for source in range(count)])


def swap(value, axis):
    count = lax.axis_size(axis)
    return lax.ppermute(value, axis, [(source, source ^ 1) for source in range(count)])


def make_patches(pixel_block):
    channels, pixel_rows, pixel_cols = pixel_block.shape
    grid_rows = pixel_rows // PATCH
    grid_cols = pixel_cols // PATCH
    shaped = pixel_block.reshape(channels, grid_rows, PATCH, grid_cols, PATCH)
    return shaped.transpose(1, 3, 0, 2, 4).reshape(grid_rows, grid_cols, channels * PATCH * PATCH)


def window_split(block):
    rows_all, cols_all, features = block.shape
    shaped = block.reshape(rows_all // WIN, WIN, cols_all // WIN, WIN, features)
    return shaped.transpose(0, 2, 1, 3, 4).reshape(-1, features)


def splice_after(own, borrowed, offset, dim):
    joined = jnp.concatenate([own, borrowed], dim)
    return lax.dynamic_slice_in_dim(joined, offset, own.shape[dim], dim)


def pack_out(rows):
    tall = rows[:16].reshape(16, 8, LANES).transpose(1, 0, 2).reshape(LANES, LANES)
    low = rows[16:].reshape(8, 8, LANES).transpose(1, 0, 2).reshape(64, 2, 64)
    return jnp.concatenate([low.transpose(1, 0, 2).reshape(LANES, 64), tall], axis=1)


def gather_weights(qkv_weight, out_weight, half):
    split = qkv_weight.size // LANES
    line = jnp.concatenate([qkv_weight.reshape(-1, LANES), out_weight.reshape(-1, LANES)])
    lines = spread(line, FAR)
    bands = lax.axis_size("yl")
    cols = lines.shape[0] // bands
    rows_w, rows_o = qkv_weight.shape[0], out_weight.shape[0]
    qkv = lines[:, :split].reshape(bands, cols, *qkv_weight.shape).transpose(0, 2, 1, 3)
    qkv = qkv.reshape(bands * rows_w, 3, -1)
    out = lines[:, split:].reshape(bands, cols, *out_weight.shape).transpose(0, 2, 1, 3)
    out = out.reshape(bands, rows_o, -1)
    features = qkv.shape[2]
    mine = lax.dynamic_slice_in_dim(qkv, half * (features // 2), features // 2, 2)
    out = lax.dynamic_slice_in_dim(out, half * 2, 2, 0)
    group = features // 4
    blocks = []
    for core in range(2):
        part = mine[:, :, core * group : (core + 1) * group]
        pieces = [part[:, i, :LANES] for i in range(3)] + [part[:, i, LANES:] for i in range(3)]
        blocks.append(jnp.concatenate([*pieces, pack_out(out[core])], axis=1))
    both = jnp.stack(blocks)
    chips = lax.axis_size("x")
    sent = jnp.broadcast_to(both[None], (chips, *both.shape)).reshape(2 * chips, *both.shape[1:])
    arrived = exchange(sent, CHIP_ROW)
    return arrived


def on_device(
    pixels,
    cotangent,
    embed_weight,
    embed_bias,
    layer_norm_gain,
    qkv_weight,
    out_weight,
    bias_table,
    rel_index,
    shifts,
):
    cotangent, pixels = cotangent[0], pixels[0]
    rows_dev, cols_dev, width = cotangent.shape
    all_heads, table_size = bias_table.shape
    heads = all_heads // 4
    grid_rows = rows_dev * lax.axis_size(ROW)
    grid_cols = cols_dev * lax.axis_size("col")
    row_shift, col_shift = shifts[0, 0], shifts[0, 1]
    row_at, col_at, core = lax.axis_index(ROW), lax.axis_index("col"), lax.axis_index("core")
    half = col_at % 2
    group = 2 * half + core

    depth = embed_weight.shape[0]
    patches = make_patches(pixels)
    patches = jnp.pad(patches, ((0, 0), (0, 0), (0, LANES - depth)))
    block = jnp.concatenate([cotangent, patches], axis=-1)
    below = from_behind(block[: WIN - 1], ROW)
    block = splice_after(block, below, row_shift, 0)
    block = splice_after(block, from_behind(block[:, :WIN], "col"), col_shift, 1)
    own = window_split(block)
    arrived = gather_weights(qkv_weight, out_weight, half)
    beside = swap(own, "col")
    two = jnp.concatenate([own, beside])
    other = swap(two, "core")
    cells = 2 * two.shape[0]

    labels = []
    for row_flip, col_flip in ((0, 0), (0, 1), (1, 0), (1, 1)):
        row_ids = (row_at ^ row_flip) * rows_dev + jnp.arange(rows_dev, dtype=jnp.int32)
        col_ids = (col_at ^ col_flip) * cols_dev + jnp.arange(cols_dev, dtype=jnp.int32)
        row_part = (row_ids >= grid_rows - row_shift).astype(jnp.int32)
        col_part = (col_ids >= grid_cols - col_shift).astype(jnp.int32)
        region = 2 * row_part[:, None] + col_part[None, :]
        labels.append(window_split(region[:, :, None])[:, 0])
    label = jnp.concatenate(labels) + 4 * (jnp.arange(cells, dtype=jnp.int32) // CELLS)
    label = label.astype(jnp.float32).reshape(-1, PAIR)
    selector = (
        rel_index.reshape(-1)[:, None] == jnp.arange(table_size, dtype=jnp.int32)[None, :]
    ).astype(jnp.float32)
    my_table = lax.dynamic_slice_in_dim(bias_table, group * heads, heads, 0)
    bias = jnp.dot(selector, my_table.T, precision=lax.Precision.HIGHEST).T
    bias = bias.reshape(heads, CELLS, CELLS)
    embed_w = jnp.pad(embed_weight, ((0, LANES - depth), (0, 0)))
    gain = layer_norm_gain[None]

    normed, xhat, inv = run_tokens(two, other, embed_w, embed_bias[None], gain)
    proj, prob, out_grad = run_forward(two, other, normed, arrived, bias, label)
    count = lax.axis_size(CHIP_ROW)
    held = exchange(out_grad.reshape(count, -1, width), CHIP_ROW)
    dproj, table_part = run_scores(two, other, proj, prob, arrived, width)
    held = held.reshape(count // 2, 2, -1, width).astype(jnp.float32).sum(axis=0)
    held = held.astype(jnp.bfloat16)
    rows_o, deep = held.shape[1], lax.axis_size("col")
    ring = lax.axis_size(RING)
    held = held.reshape(2, rows_o, deep, ring // 4, -1).transpose(0, 3, 2, 1, 4)
    held = held.reshape(2, ring // 4, -1, LANES)
    none = jnp.zeros_like(held)
    bands = jnp.concatenate([jnp.where(half == i, held, none) for i in range(2)])
    bands = exchange(bands.reshape(ring, -1, LANES), RING)
    line = run_norm(two, other, dproj, xhat, inv, gain, arrived)
    my_grad = jnp.dot(table_part.reshape(heads, -1), selector, precision=lax.Precision.HIGHEST)
    wide = 256
    my_grad = jnp.pad(my_grad, ((0, 0), (0, wide - table_size)))
    table_grad = lax.dynamic_update_slice_in_dim(
        jnp.zeros((all_heads, wide), jnp.float32), my_grad, group * heads, 0
    )
    table_rows = table_grad.astype(jnp.bfloat16).reshape(-1, width)
    line = lax.dynamic_update_slice(line, table_rows, (depth + 2, 0))
    line, bands = lax.optimization_barrier((line, bands))
    chunks = lax.axis_size(ROW)
    tall = line.shape[0]
    tiles = line.reshape(tall // 8, 8, width // LANES, LANES).transpose(0, 2, 1, 3)
    tiles = tiles.reshape(chunks, -1, LANES)
    mine = exchange(tiles, ROW)
    mine = mine.astype(jnp.float32).sum(axis=0)
    mine = mine + swap(mine, "dp")
    mine = mine.astype(jnp.bfloat16)
    bands = bands.astype(jnp.float32).sum(axis=0).astype(jnp.bfloat16)
    bands = bands.reshape(deep, -1, LANES)
    held = mine.shape[0]
    mine = jnp.broadcast_to(mine[None], (deep, held, LANES))
    both = exchange(jnp.concatenate([mine, bands], axis=1), "col")
    both = both.astype(jnp.float32).sum(axis=0)
    out_weight_grad = both[held:].reshape(rows_o, -1)
    total = spread(both[:held].astype(jnp.bfloat16), ROW)
    total = total.reshape(tall // 8, width // LANES, 8, LANES).transpose(0, 2, 1, 3)
    total = total.reshape(tall, width).astype(jnp.float32)
    table_grad = total[depth + 2 : depth + 5].reshape(all_heads, wide)[:, :table_size]
    return (out_weight_grad, total[:depth], total[depth], total[depth + 1], table_grad)


def solution(mesh):
    sizes = mesh.devices.shape
    names = ("yl", "x", "core", "col", "dp")
    fine = Mesh(mesh.devices.reshape(-1, 4, 2, *sizes[1:]), names)
    return jax.shard_map(
        on_device,
        mesh=fine,
        in_specs=(
            P("dp", None, ROW, "col"),
            P("dp", ROW, "col", None),
            P(),
            P(),
            P(),
            P(ROW, COL),
            P(ROW, COL),
            P(),
            P(),
            P("dp", None),
        ),
        out_specs=(P(ROW, COL), P(), P(), P(), P()),
        check_vma=False,
    )
```

```python
import jax
import jax.numpy as jnp
from jax import lax
from jax.experimental import pallas as pl
from jax.experimental.pallas import tpu as pltpu
from jax.sharding import Mesh, PartitionSpec as P

WIN = 8
PATCH = 4
CELLS = WIN * WIN
norm_epsilon = 1e-05

STEP = 256
PAIR = 128
HEAD = 64
LANES = 128
SCALE = HEAD ** (-0.5)
UNITS = ((0, 128, 256, 0, 2), (384, 448, 512, 128, 1))
QKV = 640


def dot_nn(a, b):
    return lax.dot_general(a, b, (((1,), (0,)), ((), ())), preferred_element_type=jnp.float32)


def dot_nt(a, b):
    return lax.dot_general(a, b, (((1,), (1,)), ((), ())), preferred_element_type=jnp.float32)


def dot_tn(a, b):
    return lax.dot_general(a, b, (((0,), (0,)), ((), ())), preferred_element_type=jnp.float32)


def half_masks(count):
    lane = lax.broadcasted_iota(jnp.int32, (PAIR, count * HEAD), 1)
    return [(lane // HEAD) == i for i in range(count)]


def choose(masks, parts):
    return parts[0] if len(parts) == 1 else jnp.where(masks[0], parts[0], parts[1])


def only(masks, i, x):
    return x if len(masks) == 1 else jnp.where(masks[i], x, jnp.zeros_like(x))


def work():
    for pair in range(STEP // PAIR):
        for unit in UNITS:
            yield (pair, slice(pair * PAIR, (pair + 1) * PAIR), *unit)


def assemble(arrived, out):
    sources, rows, _ = arrived.shape
    band = rows // 4
    for source in range(sources):
        for i in range(4):
            at = (i * sources + source) * band
            out[at : at + band, :] = arrived[source, i * band : (i + 1) * band, :QKV]


def assemble_out(arrived, wide, out):
    sources = arrived.shape[0]
    for source in range(sources):
        at = source * 24
        for tile in range(8):
            cols = slice(tile * LANES, (tile + 1) * LANES)
            tall = arrived[source, tile * 16 : (tile + 1) * 16, QKV:]
            wide[at : at + 16, cols] = tall.astype(jnp.float32)
            for i in range(2):
                low = arrived[source, i * 64 + tile * 8 : i * 64 + tile * 8 + 8, QKV - 64 : QKV]
                low = low.astype(jnp.float32)
                low = jnp.concatenate([low[:4], low[4:]], axis=1)
                wide[at + 16 + 4 * i : at + 20 + 4 * i, cols] = low
    out[...] = wide[...].astype(jnp.bfloat16)


def tokens_kernel(two, other, embed_w, embed_b, gain, normed_out, xhat_out, inv_out):
    step = pl.program_id(0)
    patches = jnp.where(step < 2, two[...], other[...])
    tokens = dot_nn(patches, embed_w[...]) + embed_b[...]
    tokens = tokens.astype(jnp.bfloat16).astype(jnp.float32)
    centered = tokens - jnp.mean(tokens, axis=-1, keepdims=True)
    inv = lax.rsqrt(jnp.mean(centered * centered, axis=-1, keepdims=True) + norm_epsilon)
    xhat = centered * inv
    xhat_out[...] = xhat
    inv_out[...] = jnp.broadcast_to(inv, inv_out.shape)
    normed_out[...] = (xhat * gain[...]).astype(jnp.bfloat16)


def forward_kernel(
    two, other, normed, arrived, bias, label,
    proj_out, prob_out, grad_out, weights, bias_pair, scores, att, grad_acc
):
    step = pl.program_id(0)

    @pl.when(step == 0)
    def _():
        assemble(arrived, weights)
        for head in range(bias.shape[0]):
            row = jnp.concatenate([bias[head], bias[head]], axis=1)
            bias_pair[head] = jnp.concatenate([row, row], axis=0)

    cot = jnp.where(step < 2, two[...], other[...])
    proj_out[...] = dot_nn(normed[...], weights[...]).astype(jnp.bfloat16)
    heads = bias.shape[0]
    for pair, rows, q_at, k_at, v_at, at, count in work():
        q = proj_out[rows, q_at : q_at + count * HEAD]
        k = proj_out[rows, k_at : k_at + count * HEAD]
        for i in range(count):
            scores[pair * heads + at // HEAD + i] = dot_nt(only(half_masks(count), i, q), k)
    for pair in range(STEP // PAIR):
        line = label[pl.ds(step * (STEP // PAIR) + pair, 1), :]
        wide = jnp.broadcast_to(line, (PAIR, PAIR))
        same = wide == wide.T
        for head in range(heads):
            values = scores[pair * heads + head] * SCALE + bias_pair[head]
            values = jnp.where(same, values, -1e30)
            e = jnp.exp(values - jnp.max(values, axis=-1, keepdims=True))
            prob_out[pair, head] = e * (1.0 / jnp.sum(e, axis=-1, keepdims=True))
    for pair, rows, q_at, k_at, v_at, at, count in work():
        v = proj_out[rows, v_at : v_at + count * HEAD]
        parts = [
            dot_nn(prob_out[pair, at // HEAD + i].astype(jnp.bfloat16), v) for i in range(count)
        ]
        att[rows, at : at + count * HEAD] = choose(half_masks(count), parts).astype(jnp.bfloat16)
    grad = dot_tn(att[...], cot)

    @pl.when(step == 0)
    def _():
        grad_acc[...] = grad

    @pl.when(step > 0)
    def _():
        grad_acc[...] += grad

    @pl.when(step == pl.num_programs(0) - 1)
    def _():
        grad_out[...] = grad_acc[...].astype(grad_out.dtype)


def scores_kernel(
    two, other, proj, prob_in, arrived, dproj, table_out, wide, wo, table, datt, d_probs, lows
):
    step = pl.program_id(0)
    heads = prob_in.shape[1]

    @pl.when(step == 0)
    def _():
        assemble_out(arrived, wide, wo)
        table[...] = jnp.zeros_like(table)

    cot = jnp.where(step < 2, two[...], other[...])
    datt[...] = dot_nt(cot, wo[...]).astype(jnp.bfloat16)
    dproj[:, QKV - HEAD :] = jnp.zeros((STEP, HEAD), jnp.bfloat16)
    for pair, rows, q_at, k_at, v_at, at, count in work():
        v = proj[rows, v_at : v_at + count * HEAD]
        d_out = datt[rows, at : at + count * HEAD]
        for i in range(count):
            d_probs[pair * heads + at // HEAD + i] = dot_nt(only(half_masks(count), i, d_out), v)
    for head in range(heads):
        total = table[head]
        for pair in range(STEP // PAIR):
            prob, d_prob = prob_in[pair, head], d_probs[pair * heads + head]
            weighted = prob * d_prob
            d_scores = weighted - prob * jnp.sum(weighted, axis=-1, keepdims=True)
            total = total + d_scores
            lows[pair * heads + head] = d_scores.astype(jnp.bfloat16)
        table[head] = total
    for pair, rows, q_at, k_at, v_at, at, count in work():
        width_in = count * HEAD
        masks = half_masks(count)
        q = proj[rows, q_at : q_at + width_in]
        k = proj[rows, k_at : k_at + width_in]
        d_out = datt[rows, at : at + width_in]
        qs, ks, vs = [], [], []
        for i in range(count):
            head = at // HEAD + i
            low = lows[pair * heads + head]
            qs.append(dot_nn(low, k))
            ks.append(dot_tn(low, q))
            vs.append(dot_tn(prob_in[pair, head].astype(jnp.bfloat16), d_out))
        dproj[rows, q_at : q_at + width_in] = (choose(masks, qs) * SCALE).astype(jnp.bfloat16)
        dproj[rows, k_at : k_at + width_in] = (choose(masks, ks) * SCALE).astype(jnp.bfloat16)
        dproj[rows, v_at : v_at + width_in] = choose(masks, vs).astype(jnp.bfloat16)

    @pl.when(step == pl.num_programs(0) - 1)
    def _():
        for head in range(heads):
            full = table[head]
            table_out[head] = full[:CELLS, :CELLS] + full[CELLS:, CELLS:]


def norm_kernel(
    two, other, dproj, xhat, inv, gain, arrived, line_out, weights, dn, branch, embed, bias, gains
):
    step = pl.program_id(0)
    width = gain.shape[1]
    chunk = 32
    cells = jnp.where(step < 2, two[...], other[...])
    patches = cells[:, width:]

    @pl.when(step == 0)
    def _():
        assemble(arrived, weights)
        cot = cells[:, :width]
        embed[...] = dot_tn(patches, cot)
        bias[...] = cot.astype(jnp.float32).reshape(STEP // 8, 8, width).sum(axis=0)
        gains[...] = jnp.zeros_like(gains)

    dn[...] = dot_nt(dproj[...], weights[...])
    bias_sum, gain_sum = bias[...], gains[...]
    for i in range(STEP // chunk):
        rows = slice(i * chunk, (i + 1) * chunk)
        d, x = dn[rows, :], xhat[rows, :]
        gain_sum = gain_sum + (d * x).reshape(chunk // 8, 8, width).sum(axis=0)
        g = d * gain[...]
        mean = jnp.mean(g, axis=-1, keepdims=True)
        along = jnp.mean(g * x, axis=-1, keepdims=True)
        out = (inv[rows, 0:1] * (g - mean - x * along)).astype(jnp.bfloat16)
        branch[rows, :] = out
        bias_sum = bias_sum + out.astype(jnp.float32).reshape(chunk // 8, 8, width).sum(axis=0)
    bias[...] = bias_sum
    gains[...] = gain_sum
    embed[...] += dot_tn(patches, branch[...])

    @pl.when(step == pl.num_programs(0) - 1)
    def _():
        depth = 48
        line_out[:depth, :] = embed[:depth, :].astype(line_out.dtype)
        row = lax.broadcasted_iota(jnp.int32, (16, width), 0)
        sums = jnp.where(row == 0, jnp.sum(bias[...], axis=0, keepdims=True), 0.0)
        sums = jnp.where(row == 1, jnp.sum(gains[...], axis=0, keepdims=True), sums)
        line_out[depth:, :] = sums.astype(line_out.dtype)


def stepped(shape):
    rest = len(shape) - 1
    return pl.BlockSpec(shape, lambda i: (i,) + (0,) * rest)


def whole(shape):
    return pl.BlockSpec(shape, lambda i: (0,) * len(shape))


def cell_specs(width, at=0):
    return [
        pl.BlockSpec((STEP, width), lambda i: (jnp.minimum(i, 1), at)),
        pl.BlockSpec((STEP, width), lambda i: (jnp.maximum(i - 2, 0), at)),
    ]


def call(kernel, cells, in_specs, out_specs, out_shape, scratch, flops):
    return pl.pallas_call(
        kernel,
        grid=(cells // STEP,),
        in_specs=in_specs,
        out_specs=out_specs,
        out_shape=out_shape,
        scratch_shapes=scratch,
        compiler_params=pltpu.CompilerParams(
            dimension_semantics=("arbitrary",), vmem_limit_bytes=56 * 1024 * 1024
        ),
        cost_estimate=pl.CostEstimate(flops=flops, transcendentals=0, bytes_accessed=8 << 20),
    )


def run_tokens(two, other, embed_w, embed_b, gain):
    cells, width = 2 * two.shape[0], gain.shape[1]
    f32, bf16 = jnp.float32, jnp.bfloat16
    return call(
        tokens_kernel, cells,
        [
            *cell_specs(LANES, width // LANES), whole((LANES, width)), whole((1, width)),
            whole((1, width)),
        ],
        [stepped((STEP, width)), stepped((STEP, width)), stepped((STEP, LANES))],
        [
            jax.ShapeDtypeStruct((cells, width), bf16),
            jax.ShapeDtypeStruct((cells, width), f32),
            jax.ShapeDtypeStruct((cells, LANES), f32),
        ],
        [],
        2 << 30,
    )(two, other, embed_w, embed_b, gain)


def run_forward(two, other, normed, arrived, bias, label):
    cells, width = normed.shape
    heads = bias.shape[0]
    features = heads * HEAD
    units = heads * (STEP // PAIR)
    f32, bf16 = jnp.float32, jnp.bfloat16
    return call(
        forward_kernel, cells,
        [
            *cell_specs(width), stepped((STEP, width)),
            whole(arrived.shape), whole(bias.shape), whole(label.shape),
        ],
        [
            stepped((STEP, QKV)), stepped((STEP // PAIR, heads, PAIR, PAIR)),
            whole((features, width)),
        ],
        [
            jax.ShapeDtypeStruct((cells, QKV), bf16),
            jax.ShapeDtypeStruct((cells // PAIR, heads, PAIR, PAIR), f32),
            jax.ShapeDtypeStruct((features, width), bf16),
        ],
        [
            pltpu.VMEM((width, QKV), bf16), pltpu.VMEM((heads, PAIR, PAIR), f32),
            pltpu.VMEM((units, PAIR, PAIR), f32), pltpu.VMEM((STEP, features), bf16),
            pltpu.VMEM((features, width), f32),
        ],
        4 << 30,
    )(two, other, normed, arrived, bias, label)


def run_scores(two, other, proj, prob, arrived, width):
    cells = proj.shape[0]
    heads = prob.shape[1]
    features = heads * HEAD
    units = heads * (STEP // PAIR)
    f32, bf16 = jnp.float32, jnp.bfloat16
    return call(
        scores_kernel, cells,
        [
            *cell_specs(width), stepped((STEP, QKV)),
            stepped((STEP // PAIR, heads, PAIR, PAIR)), whole(arrived.shape),
        ],
        [stepped((STEP, QKV)), whole((heads, CELLS, CELLS))],
        [
            jax.ShapeDtypeStruct((cells, QKV), bf16),
            jax.ShapeDtypeStruct((heads, CELLS, CELLS), f32),
        ],
        [
            pltpu.VMEM((features, width), f32), pltpu.VMEM((features, width), bf16),
            pltpu.VMEM((heads, PAIR, PAIR), f32), pltpu.VMEM((STEP, features), bf16),
            pltpu.VMEM((units, PAIR, PAIR), f32), pltpu.VMEM((units, PAIR, PAIR), bf16),
        ],
        4 << 30,
    )(two, other, proj, prob, arrived)


def run_norm(two, other, dproj, xhat, inv, gain, arrived):
    cells, width = xhat.shape
    f32, bf16 = jnp.float32, jnp.bfloat16
    return call(
        norm_kernel, cells,
        [
            *cell_specs(two.shape[1]), stepped((STEP, QKV)), stepped((STEP, width)),
            stepped((STEP, LANES)), whole((1, width)), whole(arrived.shape),
        ],
        whole((64, width)),
        jax.ShapeDtypeStruct((64, width), bf16),
        [
            pltpu.VMEM((width, QKV), bf16), pltpu.VMEM((STEP, width), f32),
            pltpu.VMEM((STEP, width), bf16), pltpu.VMEM((LANES, width), f32),
            pltpu.VMEM((8, width), f32), pltpu.VMEM((8, width), f32),
        ],
        4 << 30,
    )(two, other, dproj, xhat, inv, gain, arrived)


ROW = ("yl", "x", "core")
COL = ("col", "dp")
CHIP_ROW = ("x", "core")
FAR = ("yl", "col", "dp")


def exchange(blocks, axis):
    return lax.all_to_all(blocks, axis, split_axis=0, concat_axis=0, tiled=True)


def spread(line, axis):
    copies = jnp.broadcast_to(line[None], (lax.axis_size(axis), *line.shape))
    return exchange(copies, axis)


def from_behind(value, axis):
    count = lax.axis_size(axis)
    return lax.ppermute(value, axis, [(source, (source - 1) % count) for source in range(count)])


def swap(value, axis):
    count = lax.axis_size(axis)
    return lax.ppermute(value, axis, [(source, source ^ 1) for source in range(count)])


def make_patches(pixel_block):
    channels, pixel_rows, pixel_cols = pixel_block.shape
    grid_rows = pixel_rows // PATCH
    grid_cols = pixel_cols // PATCH
    shaped = pixel_block.reshape(channels, grid_rows, PATCH, grid_cols, PATCH)
    return shaped.transpose(1, 3, 0, 2, 4).reshape(grid_rows, grid_cols, channels * PATCH * PATCH)


def window_split(block):
    rows_all, cols_all, features = block.shape
    shaped = block.reshape(rows_all // WIN, WIN, cols_all // WIN, WIN, features)
    return shaped.transpose(0, 2, 1, 3, 4).reshape(-1, features)


def splice_after(own, borrowed, offset, dim):
    joined = jnp.concatenate([own, borrowed], dim)
    return lax.dynamic_slice_in_dim(joined, offset, own.shape[dim], dim)


UNIT = 16


def runs_of(units):
    runs = []
    for unit in units:
        shard, i = divmod(unit, 9)
        source = ("rest", 0) if i == 8 else ("main", shard)
        start = shard * UNIT if i == 8 else i * UNIT
        if runs and runs[-1][0] == source and runs[-1][2] == start:
            runs[-1][2] += UNIT
        else:
            runs.append([source, start, start + UNIT])
    return runs


def deal_kernel(lines, rest, out):
    groups = 4
    shards = lines.shape[0] // 4

    def part(source, start, end):
        if source[0] == "rest":
            return rest[:, start:end]
        rows = [lines[band * shards + source[1], 0:32, start:end] for band in range(4)]
        return jnp.concatenate(rows, axis=0)

    def columns(units):
        return [part(*run) for run in runs_of(units)]

    for group in range(groups):
        first = [48 * t + 12 * group for t in range(3)]
        tiles = [columns(range(u, u + 8)) for u in first]
        tiles.append(columns(range(first[0] + 8, first[0] + 12)))
        tiles[-1] += columns(range(first[1] + 8, first[1] + 12))
        low = jnp.concatenate(
            [lines[group * shards + shard, 44:48, :].astype(jnp.float32) for shard in range(shards)]
        )
        low = jnp.concatenate([low[:, :HEAD], low[:, HEAD:]], axis=0).astype(jnp.bfloat16)
        tiles.append(columns(range(first[2] + 8, first[2] + 12)) + [low])
        tall = []
        for shard in range(0, shards, 2):
            left = lines[group * shards + shard, 36:44, :].astype(jnp.float32)
            right = lines[group * shards + shard + 1, 36:44, :].astype(jnp.float32)
            tall.append(jnp.concatenate([left[:, :HEAD], right[:, :HEAD]], axis=1))
            tall.append(jnp.concatenate([left[:, HEAD:], right[:, HEAD:]], axis=1))
        tiles.append([jnp.concatenate(tall, axis=0).astype(jnp.bfloat16)])
        for i, pieces in enumerate(tiles):
            tile = pieces[0] if len(pieces) == 1 else jnp.concatenate(pieces, axis=1)
            for copy in range(out.shape[0] // groups):
                out[copy * groups + group, :, i * LANES : (i + 1) * LANES] = tile


def deal(lines, rest, count):
    return call(
        deal_kernel, STEP,
        [whole(lines.shape), whole(rest.shape)],
        whole((count, LANES, QKV + LANES)),
        jax.ShapeDtypeStruct((count, LANES, QKV + LANES), jnp.bfloat16),
        [],
        1 << 30,
    )(lines, rest)


def gather_weights(qkv_weight, out_weight):
    rows_w = qkv_weight.shape[0]
    last = qkv_weight[:, LANES:].reshape(-1, LANES)
    high = jnp.concatenate([out_weight[:8], out_weight[8:16]], axis=1)
    low = jnp.concatenate([out_weight[16:20], out_weight[20:]], axis=1)
    line = jnp.concatenate([qkv_weight[:, :LANES], last, high, low])
    lines = spread(line, FAR)
    bands = lax.axis_size("yl")
    count = lines.shape[0] // bands
    rest = lines[:, rows_w : rows_w + last.shape[0]].reshape(bands, count, rows_w, UNIT)
    rest = rest.transpose(0, 2, 1, 3).reshape(bands * rows_w, count * UNIT)
    sent = deal(lines, rest, lax.axis_size(CHIP_ROW))
    return exchange(sent, CHIP_ROW)


def on_device(
    pixels,
    cotangent,
    embed_weight,
    embed_bias,
    layer_norm_gain,
    qkv_weight,
    out_weight,
    bias_table,
    rel_index,
    shifts,
):
    cotangent, pixels = cotangent[0], pixels[0]
    rows_dev, cols_dev, width = cotangent.shape
    all_heads, table_size = bias_table.shape
    heads = all_heads // 4
    grid_rows = rows_dev * lax.axis_size(ROW)
    grid_cols = cols_dev * lax.axis_size("col")
    row_shift, col_shift = shifts[0, 0], shifts[0, 1]
    row_at, col_at, core = lax.axis_index(ROW), lax.axis_index("col"), lax.axis_index("core")
    group = 2 * (lax.axis_index("x") % 2) + core

    depth = embed_weight.shape[0]
    patches = make_patches(pixels)
    patches = jnp.pad(patches, ((0, 0), (0, 0), (0, LANES - depth)))
    block = jnp.concatenate([cotangent, patches], axis=-1)
    beside = from_behind(block[:, :WIN], "col")
    block = splice_after(block, beside, col_shift, 1)
    below = from_behind(block[: WIN - 1], ROW)
    own = window_split(splice_after(block, below, row_shift, 0))
    arrived = gather_weights(qkv_weight, out_weight)
    beside = swap(own, "x")
    two = jnp.concatenate([own, beside])
    other = swap(two, "core")
    cells = 2 * two.shape[0]

    labels = []
    for row_flip in (0, 2, 1, 3):
        row_ids = (row_at ^ row_flip) * rows_dev + jnp.arange(rows_dev, dtype=jnp.int32)
        col_ids = col_at * cols_dev + jnp.arange(cols_dev, dtype=jnp.int32)
        row_part = (row_ids >= grid_rows - row_shift).astype(jnp.int32)
        col_part = (col_ids >= grid_cols - col_shift).astype(jnp.int32)
        region = 2 * row_part[:, None] + col_part[None, :]
        labels.append(window_split(region[:, :, None])[:, 0])
    label = jnp.concatenate(labels) + 4 * (jnp.arange(cells, dtype=jnp.int32) // CELLS)
    label = label.astype(jnp.float32).reshape(-1, PAIR)
    selector = (
        rel_index.reshape(-1)[:, None] == jnp.arange(table_size, dtype=jnp.int32)[None, :]
    ).astype(jnp.float32)
    my_table = lax.dynamic_slice_in_dim(bias_table, group * heads, heads, 0)
    bias = jnp.dot(selector, my_table.T, precision=lax.Precision.HIGHEST).T
    bias = bias.reshape(heads, CELLS, CELLS)
    embed_w = jnp.pad(embed_weight, ((0, LANES - depth), (0, 0)))
    gain = layer_norm_gain[None]

    normed, xhat, inv = run_tokens(two, other, embed_w, embed_bias[None], gain)
    proj, prob, out_grad = run_forward(two, other, normed, arrived, bias, label)
    count = lax.axis_size(CHIP_ROW)
    held = exchange(out_grad.reshape(count, -1, width), CHIP_ROW)
    dproj, table_part = run_scores(two, other, proj, prob, arrived, width)
    held = held.reshape(2, count // 2, -1, width).astype(jnp.float32).sum(axis=0)
    bands = exchange(held.astype(jnp.bfloat16), "yl")
    line = run_norm(two, other, dproj, xhat, inv, gain, arrived)
    my_grad = jnp.dot(table_part.reshape(heads, -1), selector, precision=lax.Precision.HIGHEST)
    wide = 256
    my_grad = jnp.pad(my_grad, ((0, 0), (0, wide - table_size)))
    table_grad = lax.dynamic_update_slice_in_dim(
        jnp.zeros((all_heads, wide), jnp.float32), my_grad, group * heads, 0
    )
    table_rows = table_grad.astype(jnp.bfloat16).reshape(-1, width)
    line = lax.dynamic_update_slice(line, table_rows, (depth + 2, 0))
    line, bands = lax.optimization_barrier((line, bands))
    chunks = lax.axis_size(ROW)
    tall = line.shape[0]
    tiles = line.reshape(tall // 8, 8, width // LANES, LANES).transpose(0, 2, 1, 3)
    tiles = tiles.reshape(chunks, -1, LANES)
    mine = exchange(tiles, ROW)
    mine = mine.astype(jnp.float32).sum(axis=0).astype(jnp.bfloat16)
    rows_o = bands.shape[1]
    bands = bands.astype(jnp.float32).sum(axis=0).astype(jnp.bfloat16)
    spans = lax.axis_size(COL)
    bands = bands.reshape(rows_o, spans, -1).transpose(1, 0, 2).reshape(spans, -1, LANES)
    held = mine.shape[0]
    mine = jnp.broadcast_to(mine[None], (spans, held, LANES))
    both = exchange(jnp.concatenate([mine, bands], axis=1), COL)
    both = both.astype(jnp.float32).sum(axis=0)
    out_weight_grad = both[held:].reshape(rows_o, -1)
    total = spread(both[:held].astype(jnp.bfloat16), ROW)
    total = total.reshape(tall // 8, width // LANES, 8, LANES).transpose(0, 2, 1, 3)
    total = total.reshape(tall, width).astype(jnp.float32)
    table_grad = total[depth + 2 : depth + 5].reshape(all_heads, wide)[:, :table_size]
    return (out_weight_grad, total[:depth], total[depth], total[depth + 1], table_grad)


def solution(mesh):
    sizes = mesh.devices.shape
    names = ("yl", "x", "core", "col", "dp")
    fine = Mesh(mesh.devices.reshape(-1, 4, 2, *sizes[1:]), names)
    return jax.shard_map(
        on_device,
        mesh=fine,
        in_specs=(
            P("dp", None, ROW, "col"),
            P("dp", ROW, "col", None),
            P(),
            P(),
            P(),
            P(ROW, COL),
            P(ROW, COL),
            P(),
            P(),
            P("dp", None),
        ),
        out_specs=(P(ROW, COL), P(), P(), P(), P()),
        check_vma=False,
    )
```

```python
import jax
import jax.numpy as jnp
from jax import lax
from jax.experimental import pallas as pl
from jax.experimental.pallas import tpu as pltpu
from jax.sharding import Mesh, PartitionSpec as P

WIN = 8
PATCH = 4
CELLS = WIN * WIN
norm_epsilon = 1e-05

STEP = 512
OWN = 256
HALF = 2 * OWN // STEP
PAIR = 128
HEAD = 64
LANES = 128
SCALE = HEAD ** (-0.5)
UNITS = ((0, 128, 256, 0, 2), (384, 448, 512, 128, 1))
QKV = 640


def dot_nn(a, b):
    return lax.dot_general(a, b, (((1,), (0,)), ((), ())), preferred_element_type=jnp.float32)


def dot_nt(a, b):
    return lax.dot_general(a, b, (((1,), (1,)), ((), ())), preferred_element_type=jnp.float32)


def dot_tn(a, b):
    return lax.dot_general(a, b, (((0,), (0,)), ((), ())), preferred_element_type=jnp.float32)


def half_masks(count):
    lane = lax.broadcasted_iota(jnp.int32, (PAIR, count * HEAD), 1)
    return [(lane // HEAD) == i for i in range(count)]


def choose(masks, parts):
    return parts[0] if len(parts) == 1 else jnp.where(masks[0], parts[0], parts[1])


def only(masks, i, x):
    return x if len(masks) == 1 else jnp.where(masks[i], x, jnp.zeros_like(x))


def work():
    for pair in range(STEP // PAIR):
        for unit in UNITS:
            yield (pair, slice(pair * PAIR, (pair + 1) * PAIR), *unit)


def assemble(arrived, out):
    sources, rows, _ = arrived.shape
    band = rows // 4
    for source in range(sources):
        for i in range(4):
            at = (i * sources + source) * band
            out[at : at + band, :] = arrived[source, i * band : (i + 1) * band, :QKV]


def assemble_out(arrived, wide, out):
    sources = arrived.shape[0]
    for source in range(sources):
        at = source * 24
        for tile in range(8):
            cols = slice(tile * LANES, (tile + 1) * LANES)
            tall = arrived[source, tile * 16 : (tile + 1) * 16, QKV:]
            wide[at : at + 16, cols] = tall.astype(jnp.float32)
            for i in range(2):
                low = arrived[source, i * 64 + tile * 8 : i * 64 + tile * 8 + 8, QKV - 64 : QKV]
                low = low.astype(jnp.float32)
                low = jnp.concatenate([low[:4], low[4:]], axis=1)
                wide[at + 16 + 4 * i : at + 20 + 4 * i, cols] = low
    out[...] = wide[...].astype(jnp.bfloat16)


def tokens_kernel(two, other, embed_w, embed_b, gain, normed_out, xhat_out, inv_out):
    step = pl.program_id(0)
    patches = jnp.where(step < HALF, two[...], other[...])
    tokens = dot_nn(patches, embed_w[...]) + embed_b[...]
    tokens = tokens.astype(jnp.bfloat16).astype(jnp.float32)
    centered = tokens - jnp.mean(tokens, axis=-1, keepdims=True)
    inv = lax.rsqrt(jnp.mean(centered * centered, axis=-1, keepdims=True) + norm_epsilon)
    xhat = centered * inv
    xhat_out[...] = xhat
    inv_out[...] = jnp.broadcast_to(inv, inv_out.shape)
    normed_out[...] = (xhat * gain[...]).astype(jnp.bfloat16)


def forward_kernel(
    two, other, normed, arrived, bias, label,
    proj_out, prob_out, grad_out, weights, wo, bias_pair, scores, att, grad_acc, wide_rows
):
    step = pl.program_id(0)

    @pl.when(step == 0)
    def _():
        assemble(arrived, weights)
        assemble_out(arrived, wide_rows, wo)
        for head in range(bias.shape[0]):
            row = jnp.concatenate([bias[head], bias[head]], axis=1)
            bias_pair[head] = jnp.concatenate([row, row], axis=0)

    cot = jnp.where(step < HALF, two[...], other[...])
    proj_out[...] = dot_nn(normed[...], weights[...]).astype(jnp.bfloat16)
    heads = bias.shape[0]
    for pair, rows, q_at, k_at, v_at, at, count in work():
        q = proj_out[rows, q_at : q_at + count * HEAD]
        k = proj_out[rows, k_at : k_at + count * HEAD]
        for i in range(count):
            scores[pair * heads + at // HEAD + i] = dot_nt(only(half_masks(count), i, q), k)
    for pair in range(STEP // PAIR):
        line = label[pl.ds(step * (STEP // PAIR) + pair, 1), :]
        wide = jnp.broadcast_to(line, (PAIR, PAIR))
        same = wide == wide.T
        for head in range(heads):
            values = scores[pair * heads + head] * SCALE + bias_pair[head]
            values = jnp.where(same, values, -1e30)
            e = jnp.exp(values - jnp.max(values, axis=-1, keepdims=True))
            prob_out[pair, head] = e * (1.0 / jnp.sum(e, axis=-1, keepdims=True))
    for pair, rows, q_at, k_at, v_at, at, count in work():
        v = proj_out[rows, v_at : v_at + count * HEAD]
        parts = [
            dot_nn(prob_out[pair, at // HEAD + i].astype(jnp.bfloat16), v) for i in range(count)
        ]
        att[rows, at : at + count * HEAD] = choose(half_masks(count), parts).astype(jnp.bfloat16)
    grad = dot_tn(att[...], cot)

    @pl.when(step == 0)
    def _():
        grad_acc[...] = grad

    @pl.when(step > 0)
    def _():
        grad_acc[...] += grad

    @pl.when(step == pl.num_programs(0) - 1)
    def _():
        grad_out[...] = grad_acc[...].astype(grad_out.dtype)


def scores_kernel(
    two, other, proj, prob_in, wo, dproj, table_out, table, datt, d_probs, lows
):
    step = pl.program_id(0)
    heads = prob_in.shape[1]

    @pl.when(step == 0)
    def _():
        table[...] = jnp.zeros_like(table)

    cot = jnp.where(step < HALF, two[...], other[...])
    datt[...] = dot_nt(cot, wo[...]).astype(jnp.bfloat16)
    dproj[:, QKV - HEAD :] = jnp.zeros((STEP, HEAD), jnp.bfloat16)
    for pair, rows, q_at, k_at, v_at, at, count in work():
        v = proj[rows, v_at : v_at + count * HEAD]
        d_out = datt[rows, at : at + count * HEAD]
        for i in range(count):
            d_probs[pair * heads + at // HEAD + i] = dot_nt(only(half_masks(count), i, d_out), v)
    for head in range(heads):
        total = table[head]
        for pair in range(STEP // PAIR):
            prob, d_prob = prob_in[pair, head], d_probs[pair * heads + head]
            weighted = prob * d_prob
            d_scores = weighted - prob * jnp.sum(weighted, axis=-1, keepdims=True)
            total = total + d_scores
            lows[pair * heads + head] = d_scores.astype(jnp.bfloat16)
        table[head] = total
    for pair, rows, q_at, k_at, v_at, at, count in work():
        width_in = count * HEAD
        masks = half_masks(count)
        q = proj[rows, q_at : q_at + width_in]
        k = proj[rows, k_at : k_at + width_in]
        d_out = datt[rows, at : at + width_in]
        qs, ks, vs = [], [], []
        for i in range(count):
            head = at // HEAD + i
            low = lows[pair * heads + head]
            qs.append(dot_nn(low, k))
            ks.append(dot_tn(low, q))
            vs.append(dot_tn(prob_in[pair, head].astype(jnp.bfloat16), d_out))
        dproj[rows, q_at : q_at + width_in] = (choose(masks, qs) * SCALE).astype(jnp.bfloat16)
        dproj[rows, k_at : k_at + width_in] = (choose(masks, ks) * SCALE).astype(jnp.bfloat16)
        dproj[rows, v_at : v_at + width_in] = choose(masks, vs).astype(jnp.bfloat16)

    @pl.when(step == pl.num_programs(0) - 1)
    def _():
        for head in range(heads):
            full = table[head]
            full = full[:CELLS, :CELLS] + full[CELLS:, CELLS:]
            for row in range(0, CELLS, 2):
                pair_row = jnp.concatenate([full[row : row + 1], full[row + 1 : row + 2]], axis=1)
                table_out[head : head + 1, row * CELLS : (row + 2) * CELLS] = pair_row


def norm_kernel(
    two, other, own, dproj, xhat, inv, gain, weights, table, line_out, dn, branch, embed, bias, gains
):
    step = pl.program_id(0)
    width = gain.shape[1]
    chunk = 32
    patches = jnp.where(step < HALF, two[...], other[...])

    @pl.when(step == 0)
    def _():
        cot = own[...]
        embed[...] = dot_tn(patches[:OWN], cot)
        bias[...] = cot.astype(jnp.float32).reshape(OWN // 8, 8, width).sum(axis=0)
        gains[...] = jnp.zeros_like(gains)

    dn[...] = dot_nt(dproj[...], weights[...])
    bias_sum, gain_sum = bias[...], gains[...]
    for i in range(STEP // chunk):
        rows = slice(i * chunk, (i + 1) * chunk)
        d, x = dn[rows, :], xhat[rows, :]
        gain_sum = gain_sum + (d * x).reshape(chunk // 8, 8, width).sum(axis=0)
        g = d * gain[...]
        mean = jnp.mean(g, axis=-1, keepdims=True)
        along = jnp.mean(g * x, axis=-1, keepdims=True)
        out = (inv[rows, 0:1] * (g - mean - x * along)).astype(jnp.bfloat16)
        branch[rows, :] = out
        bias_sum = bias_sum + out.astype(jnp.float32).reshape(chunk // 8, 8, width).sum(axis=0)
    bias[...] = bias_sum
    gains[...] = gain_sum
    embed[...] += dot_tn(patches, branch[...])

    @pl.when(step == pl.num_programs(0) - 1)
    def _():
        depth = 48
        line_out[:depth, :] = embed[:depth, :].astype(line_out.dtype)
        row = lax.broadcasted_iota(jnp.int32, (16, width), 0)
        sums = jnp.where(row == 0, jnp.sum(bias[...], axis=0, keepdims=True), 0.0)
        sums = jnp.where(row == 1, jnp.sum(gains[...], axis=0, keepdims=True), sums)
        line_out[depth:, :] = (sums + table[...]).astype(line_out.dtype)


def stepped(shape):
    rest = len(shape) - 1
    return pl.BlockSpec(shape, lambda i: (i,) + (0,) * rest)


def whole(shape):
    return pl.BlockSpec(shape, lambda i: (0,) * len(shape))


def cell_specs(width, at=0):
    return [
        pl.BlockSpec((STEP, width), lambda i: (jnp.minimum(i, HALF - 1), at)),
        pl.BlockSpec((STEP, width), lambda i: (jnp.maximum(i - HALF, 0), at)),
    ]


def call(kernel, cells, in_specs, out_specs, out_shape, scratch, flops):
    return pl.pallas_call(
        kernel,
        grid=(cells // STEP,),
        in_specs=in_specs,
        out_specs=out_specs,
        out_shape=out_shape,
        scratch_shapes=scratch,
        compiler_params=pltpu.CompilerParams(
            dimension_semantics=("arbitrary",), vmem_limit_bytes=20 * 1024 * 1024
        ),
        cost_estimate=pl.CostEstimate(flops=flops, transcendentals=0, bytes_accessed=8 << 20),
    )


def run_tokens(two, other, embed_w, embed_b, gain):
    cells, width = 2 * two.shape[0], gain.shape[1]
    f32, bf16 = jnp.float32, jnp.bfloat16
    return call(
        tokens_kernel, cells,
        [
            *cell_specs(LANES, width // LANES), whole((LANES, width)), whole((1, width)),
            whole((1, width)),
        ],
        [stepped((STEP, width)), stepped((STEP, width)), stepped((STEP, LANES))],
        [
            jax.ShapeDtypeStruct((cells, width), bf16),
            jax.ShapeDtypeStruct((cells, width), f32),
            jax.ShapeDtypeStruct((cells, LANES), f32),
        ],
        [],
        2 << 30,
    )(two, other, embed_w, embed_b, gain)


def run_forward(two, other, normed, arrived, bias, label):
    cells, width = normed.shape
    heads = bias.shape[0]
    features = heads * HEAD
    units = heads * (STEP // PAIR)
    f32, bf16 = jnp.float32, jnp.bfloat16
    return call(
        forward_kernel, cells,
        [
            *cell_specs(width), stepped((STEP, width)),
            whole(arrived.shape), whole(bias.shape), whole(label.shape),
        ],
        [
            stepped((STEP, QKV)), stepped((STEP // PAIR, heads, PAIR, PAIR)),
            whole((features, width)), whole((width, QKV)), whole((features, width)),
        ],
        [
            jax.ShapeDtypeStruct((cells, QKV), bf16),
            jax.ShapeDtypeStruct((cells // PAIR, heads, PAIR, PAIR), f32),
            jax.ShapeDtypeStruct((features, width), bf16),
            jax.ShapeDtypeStruct((width, QKV), bf16),
            jax.ShapeDtypeStruct((features, width), bf16),
        ],
        [
            pltpu.VMEM((heads, PAIR, PAIR), f32),
            pltpu.VMEM((units, PAIR, PAIR), f32), pltpu.VMEM((STEP, features), bf16),
            pltpu.VMEM((features, width), f32), pltpu.VMEM((features, width), f32),
        ],
        4 << 30,
    )(two, other, normed, arrived, bias, label)


def run_scores(two, other, proj, prob, wo):
    cells, width = proj.shape[0], wo.shape[1]
    heads = prob.shape[1]
    features = heads * HEAD
    units = heads * (STEP // PAIR)
    f32, bf16 = jnp.float32, jnp.bfloat16
    return call(
        scores_kernel, cells,
        [
            *cell_specs(width), stepped((STEP, QKV)),
            stepped((STEP // PAIR, heads, PAIR, PAIR)), whole(wo.shape),
        ],
        [stepped((STEP, QKV)), whole((heads, CELLS * CELLS))],
        [
            jax.ShapeDtypeStruct((cells, QKV), bf16),
            jax.ShapeDtypeStruct((heads, CELLS * CELLS), f32),
        ],
        [
            pltpu.VMEM((heads, PAIR, PAIR), f32), pltpu.VMEM((STEP, features), bf16),
            pltpu.VMEM((units, PAIR, PAIR), f32), pltpu.VMEM((units, PAIR, PAIR), bf16),
        ],
        4 << 30,
    )(two, other, proj, prob, wo)


def run_norm(two, other, dproj, xhat, inv, gain, weights, table):
    cells, width = xhat.shape
    f32, bf16 = jnp.float32, jnp.bfloat16
    return call(
        norm_kernel, cells,
        [
            *cell_specs(LANES, width // LANES), whole((OWN, width)), stepped((STEP, QKV)),
            stepped((STEP, width)), stepped((STEP, LANES)), whole((1, width)),
            whole(weights.shape), whole(table.shape),
        ],
        whole((64, width)),
        jax.ShapeDtypeStruct((64, width), bf16),
        [
            pltpu.VMEM((STEP, width), f32),
            pltpu.VMEM((STEP, width), bf16), pltpu.VMEM((LANES, width), f32),
            pltpu.VMEM((8, width), f32), pltpu.VMEM((8, width), f32),
        ],
        4 << 30,
    )(two, other, two, dproj, xhat, inv, gain, weights, table)


ROW = ("yl", "x", "core")
COL = ("col", "dp")
CHIP_ROW = ("x", "core")
FAR = ("yl", "col", "dp")


def exchange(blocks, axis):
    return lax.all_to_all(blocks, axis, split_axis=0, concat_axis=0, tiled=True)


def spread(line, axis):
    copies = jnp.broadcast_to(line[None], (lax.axis_size(axis), *line.shape))
    return exchange(copies, axis)


def from_behind(value, axis):
    count = lax.axis_size(axis)
    return lax.ppermute(value, axis, [(source, (source - 1) % count) for source in range(count)])


def swap(value, axis):
    count = lax.axis_size(axis)
    return lax.ppermute(value, axis, [(source, source ^ 1) for source in range(count)])


def make_patches(pixel_block):
    channels, pixel_rows, pixel_cols = pixel_block.shape
    grid_rows = pixel_rows // PATCH
    grid_cols = pixel_cols // PATCH
    shaped = pixel_block.reshape(channels, grid_rows, PATCH, grid_cols, PATCH)
    return shaped.transpose(1, 3, 0, 2, 4).reshape(grid_rows, grid_cols, channels * PATCH * PATCH)


def window_split(block):
    rows_all, cols_all, features = block.shape
    shaped = block.reshape(rows_all // WIN, WIN, cols_all // WIN, WIN, features)
    return shaped.transpose(0, 2, 1, 3, 4).reshape(-1, features)


def splice_after(own, borrowed, offset, dim):
    joined = jnp.concatenate([own, borrowed], dim)
    return lax.dynamic_slice_in_dim(joined, offset, own.shape[dim], dim)


UNIT = 16


def runs_of(units):
    runs = []
    for unit in units:
        shard, i = divmod(unit, 9)
        source = ("rest", 0) if i == 8 else ("main", shard)
        start = shard * UNIT if i == 8 else i * UNIT
        if runs and runs[-1][0] == source and runs[-1][2] == start:
            runs[-1][2] += UNIT
        else:
            runs.append([source, start, start + UNIT])
    return runs


def deal_kernel(lines, rest, out):
    groups = 4
    shards = lines.shape[0] // 4

    def part(source, start, end):
        if source[0] == "rest":
            return rest[:, start:end]
        rows = [lines[band * shards + source[1], 0:32, start:end] for band in range(4)]
        return jnp.concatenate(rows, axis=0)

    def columns(units):
        return [part(*run) for run in runs_of(units)]

    for group in range(groups):
        first = [48 * t + 12 * group for t in range(3)]
        tiles = [columns(range(u, u + 8)) for u in first]
        tiles.append(columns(range(first[0] + 8, first[0] + 12)))
        tiles[-1] += columns(range(first[1] + 8, first[1] + 12))
        low = jnp.concatenate(
            [lines[group * shards + shard, 44:48, :].astype(jnp.float32) for shard in range(shards)]
        )
        low = jnp.concatenate([low[:, :HEAD], low[:, HEAD:]], axis=0).astype(jnp.bfloat16)
        tiles.append(columns(range(first[2] + 8, first[2] + 12)) + [low])
        tall = []
        for shard in range(0, shards, 2):
            left = lines[group * shards + shard, 36:44, :].astype(jnp.float32)
            right = lines[group * shards + shard + 1, 36:44, :].astype(jnp.float32)
            tall.append(jnp.concatenate([left[:, :HEAD], right[:, :HEAD]], axis=1))
            tall.append(jnp.concatenate([left[:, HEAD:], right[:, HEAD:]], axis=1))
        tiles.append([jnp.concatenate(tall, axis=0).astype(jnp.bfloat16)])
        for i, pieces in enumerate(tiles):
            tile = pieces[0] if len(pieces) == 1 else jnp.concatenate(pieces, axis=1)
            for copy in range(out.shape[0] // groups):
                out[copy * groups + group, :, i * LANES : (i + 1) * LANES] = tile


def deal(lines, rest, count):
    return call(
        deal_kernel, STEP,
        [whole(lines.shape), whole(rest.shape)],
        whole((count, LANES, QKV + LANES)),
        jax.ShapeDtypeStruct((count, LANES, QKV + LANES), jnp.bfloat16),
        [],
        1 << 30,
    )(lines, rest)


def gather_weights(qkv_weight, out_weight):
    rows_w = qkv_weight.shape[0]
    last = qkv_weight[:, LANES:].reshape(-1, LANES)
    high = jnp.concatenate([out_weight[:8], out_weight[8:16]], axis=1)
    low = jnp.concatenate([out_weight[16:20], out_weight[20:]], axis=1)
    line = jnp.concatenate([qkv_weight[:, :LANES], last, high, low])
    lines = spread(line, FAR)
    bands = lax.axis_size("yl")
    count = lines.shape[0] // bands
    rest = lines[:, rows_w : rows_w + last.shape[0]].reshape(bands, count, rows_w, UNIT)
    rest = rest.transpose(0, 2, 1, 3).reshape(bands * rows_w, count * UNIT)
    sent = deal(lines, rest, lax.axis_size(CHIP_ROW))
    return exchange(sent, CHIP_ROW)


def on_device(
    pixels,
    cotangent,
    embed_weight,
    embed_bias,
    layer_norm_gain,
    qkv_weight,
    out_weight,
    bias_table,
    rel_index,
    shifts,
):
    cotangent, pixels = cotangent[0], pixels[0]
    rows_dev, cols_dev, width = cotangent.shape
    all_heads, table_size = bias_table.shape
    heads = all_heads // 4
    grid_rows = rows_dev * lax.axis_size(ROW)
    grid_cols = cols_dev * lax.axis_size("col")
    row_shift, col_shift = shifts[0, 0], shifts[0, 1]
    row_at, col_at, core = lax.axis_index(ROW), lax.axis_index("col"), lax.axis_index("core")
    group = 2 * (lax.axis_index("x") % 2) + core

    depth = embed_weight.shape[0]
    patches = make_patches(pixels)
    patches = jnp.pad(patches, ((0, 0), (0, 0), (0, LANES - depth)))
    block = jnp.concatenate([cotangent, patches], axis=-1)
    beside = from_behind(block[:, :WIN], "col")
    block = splice_after(block, beside, col_shift, 1)
    below = from_behind(block[: WIN - 1], ROW)
    own = window_split(splice_after(block, below, row_shift, 0))
    arrived = gather_weights(qkv_weight, out_weight)
    beside = swap(own, "x")
    two = jnp.concatenate([own, beside])
    other = swap(two, "core")
    cells = 2 * two.shape[0]

    labels = []
    for row_flip in (0, 2, 1, 3):
        row_ids = (row_at ^ row_flip) * rows_dev + jnp.arange(rows_dev, dtype=jnp.int32)
        col_ids = col_at * cols_dev + jnp.arange(cols_dev, dtype=jnp.int32)
        row_part = (row_ids >= grid_rows - row_shift).astype(jnp.int32)
        col_part = (col_ids >= grid_cols - col_shift).astype(jnp.int32)
        region = 2 * row_part[:, None] + col_part[None, :]
        labels.append(window_split(region[:, :, None])[:, 0])
    label = jnp.concatenate(labels) + 4 * (jnp.arange(cells, dtype=jnp.int32) // CELLS)
    label = label.astype(jnp.float32).reshape(-1, PAIR)
    selector = (
        rel_index.reshape(-1)[:, None] == jnp.arange(table_size, dtype=jnp.int32)[None, :]
    ).astype(jnp.float32)
    my_table = lax.dynamic_slice_in_dim(bias_table, group * heads, heads, 0)
    bias = jnp.dot(selector, my_table.T, precision=lax.Precision.HIGHEST).T
    bias = bias.reshape(heads, CELLS, CELLS)
    embed_w = jnp.pad(embed_weight, ((0, LANES - depth), (0, 0)))
    gain = layer_norm_gain[None]

    normed, xhat, inv = run_tokens(two, other, embed_w, embed_bias[None], gain)
    proj, prob, out_grad, weights, wo = run_forward(two, other, normed, arrived, bias, label)
    count = lax.axis_size(CHIP_ROW)
    held = exchange(out_grad.reshape(count, -1, width), CHIP_ROW)
    dproj, table_part = run_scores(two, other, proj, prob, wo)
    held = held.reshape(2, count // 2, -1, width).astype(jnp.float32).sum(axis=0)
    bands = exchange(held.astype(jnp.bfloat16), "yl")
    my_grad = jnp.dot(table_part, selector, precision=lax.Precision.HIGHEST)
    wide = 256
    rows = jnp.zeros((16 * width // wide, wide), jnp.float32)
    first_row = 2 * width // wide + group * heads
    table = lax.dynamic_update_slice(rows, my_grad, (first_row, 0)).reshape(16, width)
    line = run_norm(two, other, dproj, xhat, inv, gain, weights, table)
    line, bands = lax.optimization_barrier((line, bands))
    chunks = lax.axis_size(ROW)
    tall = line.shape[0]
    tiles = line.reshape(tall // 8, 8, width // LANES, LANES).transpose(0, 2, 1, 3)
    tiles = tiles.reshape(chunks, -1, LANES)
    mine = exchange(tiles, ROW)
    mine = mine.astype(jnp.float32).sum(axis=0).astype(jnp.bfloat16)
    rows_o = bands.shape[1]
    bands = bands.astype(jnp.float32).sum(axis=0).astype(jnp.bfloat16)
    spans = lax.axis_size(COL)
    bands = bands.reshape(rows_o, spans, -1).transpose(1, 0, 2).reshape(spans, -1, LANES)
    held = mine.shape[0]
    mine = jnp.broadcast_to(mine[None], (spans, held, LANES))
    both = exchange(jnp.concatenate([mine, bands], axis=1), COL)
    both = both.astype(jnp.float32).sum(axis=0)
    out_weight_grad = both[held:].reshape(rows_o, -1)
    total = spread(both[:held].astype(jnp.bfloat16), ROW)
    total = total.reshape(tall // 8, width // LANES, 8, LANES).transpose(0, 2, 1, 3)
    total = total.reshape(tall, width).astype(jnp.float32)
    table_grad = total[depth + 2 : depth + 5].reshape(all_heads, wide)[:, :table_size]
    return (out_weight_grad, total[:depth], total[depth], total[depth + 1], table_grad)


def solution(mesh):
    sizes = mesh.devices.shape
    names = ("yl", "x", "core", "col", "dp")
    fine = Mesh(mesh.devices.reshape(-1, 4, 2, *sizes[1:]), names)
    return jax.shard_map(
        on_device,
        mesh=fine,
        in_specs=(
            P("dp", None, ROW, "col"),
            P("dp", ROW, "col", None),
            P(),
            P(),
            P(),
            P(ROW, COL),
            P(ROW, COL),
            P(),
            P(),
            P("dp", None),
        ),
        out_specs=(P(ROW, COL), P(), P(), P(), P()),
        check_vma=False,
    )
```

```python
import jax
import jax.numpy as jnp
from jax import lax
from jax.experimental import pallas as pl
from jax.experimental.pallas import tpu as pltpu
from jax.sharding import Mesh, PartitionSpec as P

WIN = 8
PATCH = 4
CELLS = WIN * WIN
norm_epsilon = 1e-05

STEP = 512
OWN = 256
HALF = 2 * OWN // STEP
PAIR = 128
HEAD = 64
LANES = 128
SCALE = HEAD ** (-0.5)
UNITS = ((0, 128, 256, 0, 2), (384, 448, 512, 128, 1))
QKV = 640


def dot_nn(a, b):
    return lax.dot_general(a, b, (((1,), (0,)), ((), ())), preferred_element_type=jnp.float32)


def dot_nt(a, b):
    return lax.dot_general(a, b, (((1,), (1,)), ((), ())), preferred_element_type=jnp.float32)


def dot_tn(a, b):
    return lax.dot_general(a, b, (((0,), (0,)), ((), ())), preferred_element_type=jnp.float32)


def half_masks(count):
    lane = lax.broadcasted_iota(jnp.int32, (PAIR, count * HEAD), 1)
    return [(lane // HEAD) == i for i in range(count)]


def choose(masks, parts):
    return parts[0] if len(parts) == 1 else jnp.where(masks[0], parts[0], parts[1])


def only(masks, i, x):
    return x if len(masks) == 1 else jnp.where(masks[i], x, jnp.zeros_like(x))


def work():
    for pair in range(STEP // PAIR):
        for unit in UNITS:
            yield (pair, slice(pair * PAIR, (pair + 1) * PAIR), *unit)


def assemble(arrived, out):
    sources, rows, _ = arrived.shape
    band = rows // 4
    for source in range(sources):
        for i in range(4):
            at = (i * sources + source) * band
            out[at : at + band, :] = arrived[source, i * band : (i + 1) * band, :QKV]


def assemble_out(arrived, wide, out):
    sources = arrived.shape[0]
    for source in range(sources):
        at = source * 24
        for tile in range(8):
            cols = slice(tile * LANES, (tile + 1) * LANES)
            tall = arrived[source, tile * 16 : (tile + 1) * 16, QKV:]
            wide[at : at + 16, cols] = tall.astype(jnp.float32)
            for i in range(2):
                low = arrived[source, i * 64 + tile * 8 : i * 64 + tile * 8 + 8, QKV - 64 : QKV]
                low = low.astype(jnp.float32)
                low = jnp.concatenate([low[:4], low[4:]], axis=1)
                wide[at + 16 + 4 * i : at + 20 + 4 * i, cols] = low
    out[...] = wide[...].astype(jnp.bfloat16)


def tokens_kernel(two, other, embed_w, embed_b, gain, normed_out, xhat_out, inv_out):
    step = pl.program_id(0)
    patches = jnp.where(step < HALF, two[...], other[...])
    tokens = dot_nn(patches, embed_w[...]) + embed_b[...]
    tokens = tokens.astype(jnp.bfloat16).astype(jnp.float32)
    centered = tokens - jnp.mean(tokens, axis=-1, keepdims=True)
    inv = lax.rsqrt(jnp.mean(centered * centered, axis=-1, keepdims=True) + norm_epsilon)
    xhat = centered * inv
    xhat_out[...] = xhat
    inv_out[...] = jnp.broadcast_to(inv, inv_out.shape)
    normed_out[...] = (xhat * gain[...]).astype(jnp.bfloat16)


def attention_kernel(
    two, other, normed, arrived, bias, label,
    dproj, table_out, grad_out, weights,
    wo, wide_rows, bias_pair, proj, scores, probs, lows, att, grad_acc, datt, table
):
    step = pl.program_id(0)
    heads = bias.shape[0]

    @pl.when(step == 0)
    def _():
        assemble(arrived, weights)
        assemble_out(arrived, wide_rows, wo)
        table[...] = jnp.zeros_like(table)
        for head in range(heads):
            row = jnp.concatenate([bias[head], bias[head]], axis=1)
            bias_pair[head] = jnp.concatenate([row, row], axis=0)

    cot = jnp.where(step < HALF, two[...], other[...])
    proj[...] = dot_nn(normed[...], weights[...]).astype(jnp.bfloat16)
    datt[...] = dot_nt(cot, wo[...]).astype(jnp.bfloat16)
    dproj[:, QKV - HEAD :] = jnp.zeros((STEP, HEAD), jnp.bfloat16)
    for pair, rows, q_at, k_at, v_at, at, count in work():
        q = proj[rows, q_at : q_at + count * HEAD]
        k = proj[rows, k_at : k_at + count * HEAD]
        for i in range(count):
            scores[pair * heads + at // HEAD + i] = dot_nt(only(half_masks(count), i, q), k)
    for pair in range(STEP // PAIR):
        line = label[pl.ds(step * (STEP // PAIR) + pair, 1), :]
        wide = jnp.broadcast_to(line, (PAIR, PAIR))
        same = wide == wide.T
        for head in range(heads):
            values = scores[pair * heads + head] * SCALE + bias_pair[head]
            values = jnp.where(same, values, -1e30)
            e = jnp.exp(values - jnp.max(values, axis=-1, keepdims=True))
            probs[pair * heads + head] = e * (1.0 / jnp.sum(e, axis=-1, keepdims=True))
    for pair, rows, q_at, k_at, v_at, at, count in work():
        v = proj[rows, v_at : v_at + count * HEAD]
        d_out = datt[rows, at : at + count * HEAD]
        parts = []
        for i in range(count):
            unit = pair * heads + at // HEAD + i
            parts.append(dot_nn(probs[unit].astype(jnp.bfloat16), v))
            scores[unit] = dot_nt(only(half_masks(count), i, d_out), v)
        att[rows, at : at + count * HEAD] = choose(half_masks(count), parts).astype(jnp.bfloat16)
    grad = dot_tn(att[...], cot)
    for head in range(heads):
        total = table[head]
        for pair in range(STEP // PAIR):
            unit = pair * heads + head
            prob = probs[unit]
            weighted = prob * scores[unit]
            d_scores = weighted - prob * jnp.sum(weighted, axis=-1, keepdims=True)
            total = total + d_scores
            lows[unit] = d_scores.astype(jnp.bfloat16)
        table[head] = total
    for pair, rows, q_at, k_at, v_at, at, count in work():
        width_in = count * HEAD
        masks = half_masks(count)
        q = proj[rows, q_at : q_at + width_in]
        k = proj[rows, k_at : k_at + width_in]
        d_out = datt[rows, at : at + width_in]
        qs, ks, vs = [], [], []
        for i in range(count):
            unit = pair * heads + at // HEAD + i
            qs.append(dot_nn(lows[unit], k))
            ks.append(dot_tn(lows[unit], q))
            vs.append(dot_tn(probs[unit].astype(jnp.bfloat16), d_out))
        dproj[rows, q_at : q_at + width_in] = (choose(masks, qs) * SCALE).astype(jnp.bfloat16)
        dproj[rows, k_at : k_at + width_in] = (choose(masks, ks) * SCALE).astype(jnp.bfloat16)
        dproj[rows, v_at : v_at + width_in] = choose(masks, vs).astype(jnp.bfloat16)

    @pl.when(step == 0)
    def _():
        grad_acc[...] = grad

    @pl.when(step > 0)
    def _():
        grad_acc[...] += grad

    @pl.when(step == pl.num_programs(0) - 1)
    def _():
        grad_out[...] = grad_acc[...].astype(grad_out.dtype)
        for head in range(heads):
            full = table[head]
            full = full[:CELLS, :CELLS] + full[CELLS:, CELLS:]
            for row in range(0, CELLS, 2):
                pair_row = jnp.concatenate([full[row : row + 1], full[row + 1 : row + 2]], axis=1)
                table_out[head : head + 1, row * CELLS : (row + 2) * CELLS] = pair_row


def norm_kernel(
    two, other, own, dproj, xhat, inv, gain, weights, table, line_out, dn, branch, embed, bias, gains
):
    step = pl.program_id(0)
    width = gain.shape[1]
    chunk = 32
    patches = jnp.where(step < HALF, two[...], other[...])

    @pl.when(step == 0)
    def _():
        cot = own[...]
        embed[...] = dot_tn(patches[:OWN], cot)
        bias[...] = cot.astype(jnp.float32).reshape(OWN // 8, 8, width).sum(axis=0)
        gains[...] = jnp.zeros_like(gains)

    dn[...] = dot_nt(dproj[...], weights[...])
    bias_sum, gain_sum = bias[...], gains[...]
    for i in range(STEP // chunk):
        rows = slice(i * chunk, (i + 1) * chunk)
        d, x = dn[rows, :], xhat[rows, :]
        gain_sum = gain_sum + (d * x).reshape(chunk // 8, 8, width).sum(axis=0)
        g = d * gain[...]
        mean = jnp.mean(g, axis=-1, keepdims=True)
        along = jnp.mean(g * x, axis=-1, keepdims=True)
        out = (inv[rows, 0:1] * (g - mean - x * along)).astype(jnp.bfloat16)
        branch[rows, :] = out
        bias_sum = bias_sum + out.astype(jnp.float32).reshape(chunk // 8, 8, width).sum(axis=0)
    bias[...] = bias_sum
    gains[...] = gain_sum
    embed[...] += dot_tn(patches, branch[...])

    @pl.when(step == pl.num_programs(0) - 1)
    def _():
        depth = 48
        line_out[:depth, :] = embed[:depth, :].astype(line_out.dtype)
        row = lax.broadcasted_iota(jnp.int32, (16, width), 0)
        sums = jnp.where(row == 0, jnp.sum(bias[...], axis=0, keepdims=True), 0.0)
        sums = jnp.where(row == 1, jnp.sum(gains[...], axis=0, keepdims=True), sums)
        line_out[depth:, :] = (sums + table[...]).astype(line_out.dtype)


def stepped(shape):
    rest = len(shape) - 1
    return pl.BlockSpec(shape, lambda i: (i,) + (0,) * rest)


def whole(shape):
    return pl.BlockSpec(shape, lambda i: (0,) * len(shape))


def cell_specs(width, at=0):
    return [
        pl.BlockSpec((STEP, width), lambda i: (jnp.minimum(i, HALF - 1), at)),
        pl.BlockSpec((STEP, width), lambda i: (jnp.maximum(i - HALF, 0), at)),
    ]


def call(kernel, cells, in_specs, out_specs, out_shape, scratch, flops, grant=56):
    return pl.pallas_call(
        kernel,
        grid=(cells // STEP,),
        in_specs=in_specs,
        out_specs=out_specs,
        out_shape=out_shape,
        scratch_shapes=scratch,
        compiler_params=pltpu.CompilerParams(
            dimension_semantics=("arbitrary",), vmem_limit_bytes=grant << 20
        ),
        cost_estimate=pl.CostEstimate(flops=flops, transcendentals=0, bytes_accessed=8 << 20),
    )


def run_tokens(two, other, embed_w, embed_b, gain):
    cells, width = 2 * two.shape[0], gain.shape[1]
    f32, bf16 = jnp.float32, jnp.bfloat16
    return call(
        tokens_kernel, cells,
        [
            *cell_specs(LANES, width // LANES), whole((LANES, width)), whole((1, width)),
            whole((1, width)),
        ],
        [stepped((STEP, width)), stepped((STEP, width)), stepped((STEP, LANES))],
        [
            jax.ShapeDtypeStruct((cells, width), bf16),
            jax.ShapeDtypeStruct((cells, width), f32),
            jax.ShapeDtypeStruct((cells, LANES), f32),
        ],
        [],
        2 << 30,
    )(two, other, embed_w, embed_b, gain)


def run_attention(two, other, normed, arrived, bias, label):
    cells, width = normed.shape
    heads = bias.shape[0]
    features = heads * HEAD
    units = heads * (STEP // PAIR)
    f32, bf16 = jnp.float32, jnp.bfloat16
    return call(
        attention_kernel, cells,
        [
            *cell_specs(width), stepped((STEP, width)),
            whole(arrived.shape), whole(bias.shape), whole(label.shape),
        ],
        [
            stepped((STEP, QKV)), whole((heads, CELLS * CELLS)),
            whole((features, width)), whole((width, QKV)),
        ],
        [
            jax.ShapeDtypeStruct((cells, QKV), bf16),
            jax.ShapeDtypeStruct((heads, CELLS * CELLS), f32),
            jax.ShapeDtypeStruct((features, width), bf16),
            jax.ShapeDtypeStruct((width, QKV), bf16),
        ],
        [
            pltpu.VMEM((features, width), bf16), pltpu.VMEM((features, width), f32),
            pltpu.VMEM((heads, PAIR, PAIR), f32), pltpu.VMEM((STEP, QKV), bf16),
            pltpu.VMEM((units, PAIR, PAIR), f32), pltpu.VMEM((units, PAIR, PAIR), f32),
            pltpu.VMEM((units, PAIR, PAIR), bf16), pltpu.VMEM((STEP, features), bf16),
            pltpu.VMEM((features, width), f32), pltpu.VMEM((STEP, features), bf16),
            pltpu.VMEM((heads, PAIR, PAIR), f32),
        ],
        8 << 30,
    )(two, other, normed, arrived, bias, label)


def run_norm(two, other, dproj, xhat, inv, gain, weights, table):
    cells, width = xhat.shape
    f32, bf16 = jnp.float32, jnp.bfloat16
    return call(
        norm_kernel, cells,
        [
            *cell_specs(LANES, width // LANES), whole((OWN, width)), stepped((STEP, QKV)),
            stepped((STEP, width)), stepped((STEP, LANES)), whole((1, width)),
            whole(weights.shape), whole(table.shape),
        ],
        whole((64, width)),
        jax.ShapeDtypeStruct((64, width), bf16),
        [
            pltpu.VMEM((STEP, width), f32),
            pltpu.VMEM((STEP, width), bf16), pltpu.VMEM((LANES, width), f32),
            pltpu.VMEM((8, width), f32), pltpu.VMEM((8, width), f32),
        ],
        4 << 30,
    )(two, other, two, dproj, xhat, inv, gain, weights, table)


ROW = ("yl", "x", "core")
COL = ("col", "dp")
CHIP_ROW = ("x", "core")
FAR = ("yl", "col", "dp")


def exchange(blocks, axis):
    return lax.all_to_all(blocks, axis, split_axis=0, concat_axis=0, tiled=True)


def spread(line, axis):
    copies = jnp.broadcast_to(line[None], (lax.axis_size(axis), *line.shape))
    return exchange(copies, axis)


def from_behind(value, axis):
    count = lax.axis_size(axis)
    return lax.ppermute(value, axis, [(source, (source - 1) % count) for source in range(count)])


def swap(value, axis):
    count = lax.axis_size(axis)
    return lax.ppermute(value, axis, [(source, source ^ 1) for source in range(count)])


def make_patches(pixel_block):
    channels, pixel_rows, pixel_cols = pixel_block.shape
    grid_rows = pixel_rows // PATCH
    grid_cols = pixel_cols // PATCH
    shaped = pixel_block.reshape(channels, grid_rows, PATCH, grid_cols, PATCH)
    return shaped.transpose(1, 3, 0, 2, 4).reshape(grid_rows, grid_cols, channels * PATCH * PATCH)


def window_split(block):
    rows_all, cols_all, features = block.shape
    shaped = block.reshape(rows_all // WIN, WIN, cols_all // WIN, WIN, features)
    return shaped.transpose(0, 2, 1, 3, 4).reshape(-1, features)


def splice_after(own, borrowed, offset, dim):
    joined = jnp.concatenate([own, borrowed], dim)
    return lax.dynamic_slice_in_dim(joined, offset, own.shape[dim], dim)


UNIT = 16


def runs_of(units):
    runs = []
    for unit in units:
        shard, i = divmod(unit, 9)
        source = ("rest", 0) if i == 8 else ("main", shard)
        start = shard * UNIT if i == 8 else i * UNIT
        if runs and runs[-1][0] == source and runs[-1][2] == start:
            runs[-1][2] += UNIT
        else:
            runs.append([source, start, start + UNIT])
    return runs


def deal_kernel(lines, rest, out):
    groups = 4
    shards = lines.shape[0] // 4

    def part(source, start, end):
        if source[0] == "rest":
            return rest[:, start:end]
        rows = [lines[band * shards + source[1], 0:32, start:end] for band in range(4)]
        return jnp.concatenate(rows, axis=0)

    def columns(units):
        return [part(*run) for run in runs_of(units)]

    for group in range(groups):
        first = [48 * t + 12 * group for t in range(3)]
        tiles = [columns(range(u, u + 8)) for u in first]
        tiles.append(columns(range(first[0] + 8, first[0] + 12)))
        tiles[-1] += columns(range(first[1] + 8, first[1] + 12))
        low = jnp.concatenate(
            [lines[group * shards + shard, 44:48, :].astype(jnp.float32) for shard in range(shards)]
        )
        low = jnp.concatenate([low[:, :HEAD], low[:, HEAD:]], axis=0).astype(jnp.bfloat16)
        tiles.append(columns(range(first[2] + 8, first[2] + 12)) + [low])
        tall = []
        for shard in range(0, shards, 2):
            left = lines[group * shards + shard, 36:44, :].astype(jnp.float32)
            right = lines[group * shards + shard + 1, 36:44, :].astype(jnp.float32)
            tall.append(jnp.concatenate([left[:, :HEAD], right[:, :HEAD]], axis=1))
            tall.append(jnp.concatenate([left[:, HEAD:], right[:, HEAD:]], axis=1))
        tiles.append([jnp.concatenate(tall, axis=0).astype(jnp.bfloat16)])
        for i, pieces in enumerate(tiles):
            tile = pieces[0] if len(pieces) == 1 else jnp.concatenate(pieces, axis=1)
            for copy in range(out.shape[0] // groups):
                out[copy * groups + group, :, i * LANES : (i + 1) * LANES] = tile


def deal(lines, rest, count):
    return call(
        deal_kernel, STEP,
        [whole(lines.shape), whole(rest.shape)],
        whole((count, LANES, QKV + LANES)),
        jax.ShapeDtypeStruct((count, LANES, QKV + LANES), jnp.bfloat16),
        [],
        1 << 30,
        20,
    )(lines, rest)


def gather_weights(qkv_weight, out_weight):
    rows_w = qkv_weight.shape[0]
    last = qkv_weight[:, LANES:].reshape(-1, LANES)
    high = jnp.concatenate([out_weight[:8], out_weight[8:16]], axis=1)
    low = jnp.concatenate([out_weight[16:20], out_weight[20:]], axis=1)
    line = jnp.concatenate([qkv_weight[:, :LANES], last, high, low])
    lines = spread(line, FAR)
    bands = lax.axis_size("yl")
    count = lines.shape[0] // bands
    rest = lines[:, rows_w : rows_w + last.shape[0]].reshape(bands, count, rows_w, UNIT)
    rest = rest.transpose(0, 2, 1, 3).reshape(bands * rows_w, count * UNIT)
    sent = deal(lines, rest, lax.axis_size(CHIP_ROW))
    return exchange(sent, CHIP_ROW)


def on_device(
    pixels,
    cotangent,
    embed_weight,
    embed_bias,
    layer_norm_gain,
    qkv_weight,
    out_weight,
    bias_table,
    rel_index,
    shifts,
):
    cotangent, pixels = cotangent[0], pixels[0]
    rows_dev, cols_dev, width = cotangent.shape
    all_heads, table_size = bias_table.shape
    heads = all_heads // 4
    grid_rows = rows_dev * lax.axis_size(ROW)
    grid_cols = cols_dev * lax.axis_size("col")
    row_shift, col_shift = shifts[0, 0], shifts[0, 1]
    row_at, col_at, core = lax.axis_index(ROW), lax.axis_index("col"), lax.axis_index("core")
    group = 2 * (lax.axis_index("x") % 2) + core

    depth = embed_weight.shape[0]
    patches = make_patches(pixels)
    patches = jnp.pad(patches, ((0, 0), (0, 0), (0, LANES - depth)))
    block = jnp.concatenate([cotangent, patches], axis=-1)
    beside = from_behind(block[:, :WIN], "col")
    block = splice_after(block, beside, col_shift, 1)
    below = from_behind(block[: WIN - 1], ROW)
    own = window_split(splice_after(block, below, row_shift, 0))
    arrived = gather_weights(qkv_weight, out_weight)
    beside = swap(own, "x")
    two = jnp.concatenate([own, beside])
    other = swap(two, "core")
    cells = 2 * two.shape[0]

    labels = []
    for row_flip in (0, 2, 1, 3):
        row_ids = (row_at ^ row_flip) * rows_dev + jnp.arange(rows_dev, dtype=jnp.int32)
        col_ids = col_at * cols_dev + jnp.arange(cols_dev, dtype=jnp.int32)
        row_part = (row_ids >= grid_rows - row_shift).astype(jnp.int32)
        col_part = (col_ids >= grid_cols - col_shift).astype(jnp.int32)
        region = 2 * row_part[:, None] + col_part[None, :]
        labels.append(window_split(region[:, :, None])[:, 0])
    label = jnp.concatenate(labels) + 4 * (jnp.arange(cells, dtype=jnp.int32) // CELLS)
    label = label.astype(jnp.float32).reshape(-1, PAIR)
    selector = (
        rel_index.reshape(-1)[:, None] == jnp.arange(table_size, dtype=jnp.int32)[None, :]
    ).astype(jnp.float32)
    my_table = lax.dynamic_slice_in_dim(bias_table, group * heads, heads, 0)
    bias = jnp.dot(selector, my_table.T, precision=lax.Precision.HIGHEST).T
    bias = bias.reshape(heads, CELLS, CELLS)
    embed_w = jnp.pad(embed_weight, ((0, LANES - depth), (0, 0)))
    gain = layer_norm_gain[None]

    normed, xhat, inv = run_tokens(two, other, embed_w, embed_bias[None], gain)
    dproj, table_part, out_grad, weights = run_attention(
        two, other, normed, arrived, bias, label
    )
    count = lax.axis_size(CHIP_ROW)
    held = exchange(out_grad.reshape(count, -1, width), CHIP_ROW)
    my_grad = jnp.dot(table_part, selector, precision=lax.Precision.HIGHEST)
    wide = 256
    rows = jnp.zeros((16 * width // wide, wide), jnp.float32)
    first_row = 2 * width // wide + group * heads
    table = lax.dynamic_update_slice(rows, my_grad, (first_row, 0)).reshape(16, width)
    line = run_norm(two, other, dproj, xhat, inv, gain, weights, table)
    line, held = lax.optimization_barrier((line, held))
    chunks = lax.axis_size(ROW)
    tall = line.shape[0]
    tiles = line.reshape(tall // 8, 8, width // LANES, LANES).transpose(0, 2, 1, 3)
    tiles = tiles.reshape(chunks, -1, LANES)
    mine = exchange(tiles, ROW)
    bands = held.reshape(2, count // 2, -1, width).astype(jnp.float32).sum(axis=0)
    groups, rows_o, _ = bands.shape
    spans = lax.axis_size(COL)
    bands = bands.astype(jnp.bfloat16).reshape(groups, rows_o, spans, -1).transpose(2, 0, 1, 3)
    bands = bands.reshape(spans, -1, LANES)
    mine = mine.astype(jnp.float32).sum(axis=0).astype(jnp.bfloat16)
    depth_s = mine.shape[0]
    mine = jnp.broadcast_to(mine[None], (spans, depth_s, LANES))
    both = exchange(jnp.concatenate([mine, bands], axis=1), COL)
    both = both.astype(jnp.float32).sum(axis=0).astype(jnp.bfloat16)
    mine = jnp.broadcast_to(both[None, :depth_s], (chunks, depth_s, LANES))
    bands = both[depth_s:].reshape(groups, 1, -1, LANES)
    here = jnp.arange(count, dtype=jnp.int32)[None, :, None, None] == lax.axis_index(CHIP_ROW)
    bands = jnp.where(here, bands, jnp.zeros_like(bands)).reshape(chunks, -1, LANES)
    total = exchange(jnp.concatenate([mine, bands], axis=1), ROW)
    out_weight_grad = total[:, depth_s:].astype(jnp.float32).sum(axis=0).reshape(rows_o, -1)
    total = total[:, :depth_s]
    total = total.reshape(tall // 8, width // LANES, 8, LANES).transpose(0, 2, 1, 3)
    total = total.reshape(tall, width).astype(jnp.float32)
    table_grad = total[depth + 2 : depth + 5].reshape(all_heads, wide)[:, :table_size]
    return (out_weight_grad, total[:depth], total[depth], total[depth + 1], table_grad)


def solution(mesh):
    sizes = mesh.devices.shape
    names = ("yl", "x", "core", "col", "dp")
    fine = Mesh(mesh.devices.reshape(-1, 4, 2, *sizes[1:]), names)
    return jax.shard_map(
        on_device,
        mesh=fine,
        in_specs=(
            P("dp", None, ROW, "col"),
            P("dp", ROW, "col", None),
            P(),
            P(),
            P(),
            P(ROW, COL),
            P(ROW, COL),
            P(),
            P(),
            P("dp", None),
        ),
        out_specs=(P(ROW, COL), P(), P(), P(), P()),
        check_vma=False,
    )
```

```python
import jax
import jax.numpy as jnp
from jax import lax
from jax.experimental import pallas as pl
from jax.experimental.pallas import tpu as pltpu
from jax.sharding import Mesh, PartitionSpec as P

WIN = 8
PATCH = 4
CELLS = WIN * WIN
norm_epsilon = 1e-05

STEP = 512
OWN = 256
HALF = 2 * OWN // STEP
PAIR = 128
HEAD = 64
LANES = 128
SCALE = HEAD ** (-0.5)
UNITS = ((0, 128, 256, 0, 2), (384, 448, 512, 128, 1))
QKV = 640


def dot_nn(a, b):
    return lax.dot_general(a, b, (((1,), (0,)), ((), ())), preferred_element_type=jnp.float32)


def dot_nt(a, b):
    return lax.dot_general(a, b, (((1,), (1,)), ((), ())), preferred_element_type=jnp.float32)


def dot_tn(a, b):
    return lax.dot_general(a, b, (((0,), (0,)), ((), ())), preferred_element_type=jnp.float32)


def half_masks(count):
    lane = lax.broadcasted_iota(jnp.int32, (PAIR, count * HEAD), 1)
    return [(lane // HEAD) == i for i in range(count)]


def choose(masks, parts):
    return parts[0] if len(parts) == 1 else jnp.where(masks[0], parts[0], parts[1])


def only(masks, i, x):
    return x if len(masks) == 1 else jnp.where(masks[i], x, jnp.zeros_like(x))


def work():
    for pair in range(STEP // PAIR):
        for unit in UNITS:
            yield (pair, slice(pair * PAIR, (pair + 1) * PAIR), *unit)


def assemble(arrived, out):
    sources, rows, _ = arrived.shape
    band = rows // 4
    for source in range(sources):
        for i in range(4):
            at = (i * sources + source) * band
            out[at : at + band, :] = arrived[source, i * band : (i + 1) * band, :QKV]


def assemble_out(arrived, wide, out):
    sources = arrived.shape[0]
    for source in range(sources):
        at = source * 24
        for tile in range(8):
            cols = slice(tile * LANES, (tile + 1) * LANES)
            tall = arrived[source, tile * 16 : (tile + 1) * 16, QKV:]
            wide[at : at + 16, cols] = tall.astype(jnp.float32)
            for i in range(2):
                low = arrived[source, i * 64 + tile * 8 : i * 64 + tile * 8 + 8, QKV - 64 : QKV]
                low = low.astype(jnp.float32)
                low = jnp.concatenate([low[:4], low[4:]], axis=1)
                wide[at + 16 + 4 * i : at + 20 + 4 * i, cols] = low
    out[...] = wide[...].astype(jnp.bfloat16)


def tokens_kernel(two, other, embed_w, embed_b, gain, normed_out, xhat_out, inv_out):
    step = pl.program_id(0)
    patches = jnp.where(step < HALF, two[...], other[...])
    tokens = dot_nn(patches, embed_w[...]) + embed_b[...]
    tokens = tokens.astype(jnp.bfloat16).astype(jnp.float32)
    centered = tokens - jnp.mean(tokens, axis=-1, keepdims=True)
    inv = lax.rsqrt(jnp.mean(centered * centered, axis=-1, keepdims=True) + norm_epsilon)
    xhat = centered * inv
    xhat_out[...] = xhat.astype(xhat_out.dtype)
    inv_out[...] = jnp.broadcast_to(inv, inv_out.shape)
    normed_out[...] = (xhat * gain[...]).astype(jnp.bfloat16)


def attention_kernel(
    two, other, normed, arrived, bias, label,
    dproj, table_out, grad_out, weights,
    wo, wide_rows, bias_pair, proj, scores, probs, lows, att, grad_acc, datt, table
):
    step = pl.program_id(0)
    heads = bias.shape[0]

    @pl.when(step == 0)
    def _():
        assemble(arrived, weights)
        assemble_out(arrived, wide_rows, wo)
        table[...] = jnp.zeros_like(table)
        for head in range(heads):
            row = jnp.concatenate([bias[head], bias[head]], axis=1)
            bias_pair[head] = jnp.concatenate([row, row], axis=0)

    cot = jnp.where(step < HALF, two[...], other[...])
    proj[...] = dot_nn(normed[...], weights[...]).astype(jnp.bfloat16)
    datt[...] = dot_nt(cot, wo[...]).astype(jnp.bfloat16)
    dproj[:, QKV - HEAD :] = jnp.zeros((STEP, HEAD), jnp.bfloat16)
    for pair, rows, q_at, k_at, v_at, at, count in work():
        q = proj[rows, q_at : q_at + count * HEAD]
        k = proj[rows, k_at : k_at + count * HEAD]
        for i in range(count):
            scores[pair * heads + at // HEAD + i] = dot_nt(only(half_masks(count), i, q), k)
    for pair in range(STEP // PAIR):
        line = label[pl.ds(step * (STEP // PAIR) + pair, 1), :]
        wide = jnp.broadcast_to(line, (PAIR, PAIR))
        same = wide == wide.T
        for head in range(heads):
            values = scores[pair * heads + head] * SCALE + bias_pair[head]
            values = jnp.where(same, values, -1e30)
            e = jnp.exp(values - jnp.max(values, axis=-1, keepdims=True))
            probs[pair * heads + head] = e * (1.0 / jnp.sum(e, axis=-1, keepdims=True))
    for pair, rows, q_at, k_at, v_at, at, count in work():
        v = proj[rows, v_at : v_at + count * HEAD]
        d_out = datt[rows, at : at + count * HEAD]
        parts = []
        for i in range(count):
            unit = pair * heads + at // HEAD + i
            parts.append(dot_nn(probs[unit].astype(jnp.bfloat16), v))
            scores[unit] = dot_nt(only(half_masks(count), i, d_out), v)
        att[rows, at : at + count * HEAD] = choose(half_masks(count), parts).astype(jnp.bfloat16)
    grad = dot_tn(att[...], cot)
    for head in range(heads):
        total = table[head]
        for pair in range(STEP // PAIR):
            unit = pair * heads + head
            prob = probs[unit]
            weighted = prob * scores[unit]
            d_scores = weighted - prob * jnp.sum(weighted, axis=-1, keepdims=True)
            total = total + d_scores
            lows[unit] = d_scores.astype(jnp.bfloat16)
        table[head] = total
    for pair, rows, q_at, k_at, v_at, at, count in work():
        width_in = count * HEAD
        masks = half_masks(count)
        q = proj[rows, q_at : q_at + width_in]
        k = proj[rows, k_at : k_at + width_in]
        d_out = datt[rows, at : at + width_in]
        qs, ks, vs = [], [], []
        for i in range(count):
            unit = pair * heads + at // HEAD + i
            qs.append(dot_nn(lows[unit], k))
            ks.append(dot_tn(lows[unit], q))
            vs.append(dot_tn(probs[unit].astype(jnp.bfloat16), d_out))
        dproj[rows, q_at : q_at + width_in] = (choose(masks, qs) * SCALE).astype(jnp.bfloat16)
        dproj[rows, k_at : k_at + width_in] = (choose(masks, ks) * SCALE).astype(jnp.bfloat16)
        dproj[rows, v_at : v_at + width_in] = choose(masks, vs).astype(jnp.bfloat16)

    @pl.when(step == 0)
    def _():
        grad_acc[...] = grad

    @pl.when(step > 0)
    def _():
        grad_acc[...] += grad

    @pl.when(step == pl.num_programs(0) - 1)
    def _():
        grad_out[...] = grad_acc[...].astype(grad_out.dtype)
        for head in range(heads):
            full = table[head]
            full = full[:CELLS, :CELLS] + full[CELLS:, CELLS:]
            for row in range(0, CELLS, 2):
                pair_row = jnp.concatenate([full[row : row + 1], full[row + 1 : row + 2]], axis=1)
                table_out[head : head + 1, row * CELLS : (row + 2) * CELLS] = pair_row


def norm_kernel(
    two, other, own, dproj, xhat, inv, gain, weights, table, line_out, dn, branch, embed, bias, gains
):
    step = pl.program_id(0)
    width = gain.shape[1]
    chunk = 32
    patches = jnp.where(step < HALF, two[...], other[...])

    @pl.when(step == 0)
    def _():
        cot = own[...]
        embed[...] = dot_tn(patches[:OWN], cot)
        bias[...] = cot.astype(jnp.float32).reshape(OWN // 8, 8, width).sum(axis=0)
        gains[...] = jnp.zeros_like(gains)

    dn[...] = dot_nt(dproj[...], weights[...])
    bias_sum, gain_sum = bias[...], gains[...]
    for i in range(STEP // chunk):
        rows = slice(i * chunk, (i + 1) * chunk)
        d, x = dn[rows, :], xhat[rows, :].astype(jnp.float32)
        gain_sum = gain_sum + (d * x).reshape(chunk // 8, 8, width).sum(axis=0)
        g = d * gain[...]
        mean = jnp.mean(g, axis=-1, keepdims=True)
        along = jnp.mean(g * x, axis=-1, keepdims=True)
        out = (inv[rows, 0:1] * (g - mean - x * along)).astype(jnp.bfloat16)
        branch[rows, :] = out
        bias_sum = bias_sum + out.astype(jnp.float32).reshape(chunk // 8, 8, width).sum(axis=0)
    bias[...] = bias_sum
    gains[...] = gain_sum
    embed[...] += dot_tn(patches, branch[...])

    @pl.when(step == pl.num_programs(0) - 1)
    def _():
        depth = 48
        line_out[:depth, :] = embed[:depth, :].astype(line_out.dtype)
        row = lax.broadcasted_iota(jnp.int32, (16, width), 0)
        sums = jnp.where(row == 0, jnp.sum(bias[...], axis=0, keepdims=True), 0.0)
        sums = jnp.where(row == 1, jnp.sum(gains[...], axis=0, keepdims=True), sums)
        line_out[depth:, :] = (sums + table[...]).astype(line_out.dtype)


def stepped(shape):
    rest = len(shape) - 1
    return pl.BlockSpec(shape, lambda i: (i,) + (0,) * rest)


def whole(shape):
    return pl.BlockSpec(shape, lambda i: (0,) * len(shape))


def cell_specs(width, at=0):
    return [
        pl.BlockSpec((STEP, width), lambda i: (jnp.minimum(i, HALF - 1), at)),
        pl.BlockSpec((STEP, width), lambda i: (jnp.maximum(i - HALF, 0), at)),
    ]


def call(kernel, cells, in_specs, out_specs, out_shape, scratch, flops, grant=56):
    return pl.pallas_call(
        kernel,
        grid=(cells // STEP,),
        in_specs=in_specs,
        out_specs=out_specs,
        out_shape=out_shape,
        scratch_shapes=scratch,
        compiler_params=pltpu.CompilerParams(
            dimension_semantics=("arbitrary",), vmem_limit_bytes=grant << 20
        ),
        cost_estimate=pl.CostEstimate(flops=flops, transcendentals=0, bytes_accessed=8 << 20),
    )


def run_tokens(two, other, embed_w, embed_b, gain):
    cells, width = 2 * two.shape[0], gain.shape[1]
    f32, bf16 = jnp.float32, jnp.bfloat16
    return call(
        tokens_kernel, cells,
        [
            *cell_specs(LANES, width // LANES), whole((LANES, width)), whole((1, width)),
            whole((1, width)),
        ],
        [stepped((STEP, width)), stepped((STEP, width)), stepped((STEP, LANES))],
        [
            jax.ShapeDtypeStruct((cells, width), bf16),
            jax.ShapeDtypeStruct((cells, width), bf16),
            jax.ShapeDtypeStruct((cells, LANES), f32),
        ],
        [],
        2 << 30,
    )(two, other, embed_w, embed_b, gain)


def run_attention(two, other, normed, arrived, bias, label):
    cells, width = normed.shape
    heads = bias.shape[0]
    features = heads * HEAD
    units = heads * (STEP // PAIR)
    f32, bf16 = jnp.float32, jnp.bfloat16
    return call(
        attention_kernel, cells,
        [
            *cell_specs(width), stepped((STEP, width)),
            whole(arrived.shape), whole(bias.shape), whole(label.shape),
        ],
        [
            stepped((STEP, QKV)), whole((heads, CELLS * CELLS)),
            whole((features, width)), whole((width, QKV)),
        ],
        [
            jax.ShapeDtypeStruct((cells, QKV), bf16),
            jax.ShapeDtypeStruct((heads, CELLS * CELLS), f32),
            jax.ShapeDtypeStruct((features, width), bf16),
            jax.ShapeDtypeStruct((width, QKV), bf16),
        ],
        [
            pltpu.VMEM((features, width), bf16), pltpu.VMEM((features, width), f32),
            pltpu.VMEM((heads, PAIR, PAIR), f32), pltpu.VMEM((STEP, QKV), bf16),
            pltpu.VMEM((units, PAIR, PAIR), f32), pltpu.VMEM((units, PAIR, PAIR), f32),
            pltpu.VMEM((units, PAIR, PAIR), bf16), pltpu.VMEM((STEP, features), bf16),
            pltpu.VMEM((features, width), f32), pltpu.VMEM((STEP, features), bf16),
            pltpu.VMEM((heads, PAIR, PAIR), f32),
        ],
        8 << 30,
        50,
    )(two, other, normed, arrived, bias, label)


def run_norm(two, other, dproj, xhat, inv, gain, weights, table):
    cells, width = xhat.shape
    f32, bf16 = jnp.float32, jnp.bfloat16
    return call(
        norm_kernel, cells,
        [
            *cell_specs(LANES, width // LANES), whole((OWN, width)), stepped((STEP, QKV)),
            stepped((STEP, width)), stepped((STEP, LANES)), whole((1, width)),
            whole(weights.shape), whole(table.shape),
        ],
        whole((64, width)),
        jax.ShapeDtypeStruct((64, width), bf16),
        [
            pltpu.VMEM((STEP, width), f32),
            pltpu.VMEM((STEP, width), bf16), pltpu.VMEM((LANES, width), f32),
            pltpu.VMEM((8, width), f32), pltpu.VMEM((8, width), f32),
        ],
        4 << 30,
    )(two, other, two, dproj, xhat, inv, gain, weights, table)


ROW = ("yl", "x", "core")
COL = ("col", "dp")
CHIP_ROW = ("x", "core")
FAR = ("yl", "col", "dp")


def exchange(blocks, axis):
    return lax.all_to_all(blocks, axis, split_axis=0, concat_axis=0, tiled=True)


def spread(line, axis):
    copies = jnp.broadcast_to(line[None], (lax.axis_size(axis), *line.shape))
    return exchange(copies, axis)


def from_behind(value, axis):
    count = lax.axis_size(axis)
    return lax.ppermute(value, axis, [(source, (source - 1) % count) for source in range(count)])


def swap(value, axis):
    count = lax.axis_size(axis)
    return lax.ppermute(value, axis, [(source, source ^ 1) for source in range(count)])


def make_patches(pixel_block):
    channels, pixel_rows, pixel_cols = pixel_block.shape
    grid_rows = pixel_rows // PATCH
    grid_cols = pixel_cols // PATCH
    shaped = pixel_block.reshape(channels, grid_rows, PATCH, grid_cols, PATCH)
    return shaped.transpose(1, 3, 0, 2, 4).reshape(grid_rows, grid_cols, channels * PATCH * PATCH)


def window_split(block):
    rows_all, cols_all, features = block.shape
    shaped = block.reshape(rows_all // WIN, WIN, cols_all // WIN, WIN, features)
    return shaped.transpose(0, 2, 1, 3, 4).reshape(-1, features)


def splice_after(own, borrowed, offset, dim):
    joined = jnp.concatenate([own, borrowed], dim)
    return lax.dynamic_slice_in_dim(joined, offset, own.shape[dim], dim)


UNIT = 16


def runs_of(units):
    runs = []
    for unit in units:
        shard, i = divmod(unit, 9)
        source = ("rest", 0) if i == 8 else ("main", shard)
        start = shard * UNIT if i == 8 else i * UNIT
        if runs and runs[-1][0] == source and runs[-1][2] == start:
            runs[-1][2] += UNIT
        else:
            runs.append([source, start, start + UNIT])
    return runs


def deal_kernel(lines, rest, out):
    groups = 4
    shards = lines.shape[0] // 4

    def part(source, start, end):
        if source[0] == "rest":
            return rest[:, start:end]
        rows = [lines[band * shards + source[1], 0:32, start:end] for band in range(4)]
        return jnp.concatenate(rows, axis=0)

    def columns(units):
        return [part(*run) for run in runs_of(units)]

    for group in range(groups):
        first = [48 * t + 12 * group for t in range(3)]
        tiles = [columns(range(u, u + 8)) for u in first]
        tiles.append(columns(range(first[0] + 8, first[0] + 12)))
        tiles[-1] += columns(range(first[1] + 8, first[1] + 12))
        low = jnp.concatenate(
            [lines[group * shards + shard, 44:48, :].astype(jnp.float32) for shard in range(shards)]
        )
        low = jnp.concatenate([low[:, :HEAD], low[:, HEAD:]], axis=0).astype(jnp.bfloat16)
        tiles.append(columns(range(first[2] + 8, first[2] + 12)) + [low])
        tall = []
        for shard in range(0, shards, 2):
            left = lines[group * shards + shard, 36:44, :].astype(jnp.float32)
            right = lines[group * shards + shard + 1, 36:44, :].astype(jnp.float32)
            tall.append(jnp.concatenate([left[:, :HEAD], right[:, :HEAD]], axis=1))
            tall.append(jnp.concatenate([left[:, HEAD:], right[:, HEAD:]], axis=1))
        tiles.append([jnp.concatenate(tall, axis=0).astype(jnp.bfloat16)])
        for i, pieces in enumerate(tiles):
            tile = pieces[0] if len(pieces) == 1 else jnp.concatenate(pieces, axis=1)
            for copy in range(out.shape[0] // groups):
                out[copy * groups + group, :, i * LANES : (i + 1) * LANES] = tile


def deal(lines, rest, count):
    return call(
        deal_kernel, STEP,
        [whole(lines.shape), whole(rest.shape)],
        whole((count, LANES, QKV + LANES)),
        jax.ShapeDtypeStruct((count, LANES, QKV + LANES), jnp.bfloat16),
        [],
        1 << 30,
        20,
    )(lines, rest)


def gather_weights(qkv_weight, out_weight):
    rows_w = qkv_weight.shape[0]
    last = qkv_weight[:, LANES:].reshape(-1, LANES)
    high = jnp.concatenate([out_weight[:8], out_weight[8:16]], axis=1)
    low = jnp.concatenate([out_weight[16:20], out_weight[20:]], axis=1)
    line = jnp.concatenate([qkv_weight[:, :LANES], last, high, low])
    lines = spread(line, FAR)
    bands = lax.axis_size("yl")
    count = lines.shape[0] // bands
    rest = lines[:, rows_w : rows_w + last.shape[0]].reshape(bands, count, rows_w, UNIT)
    rest = rest.transpose(0, 2, 1, 3).reshape(bands * rows_w, count * UNIT)
    sent = deal(lines, rest, lax.axis_size(CHIP_ROW))
    return exchange(sent, CHIP_ROW)


def finish_kernel(total, embed, bias, gain, table, out):
    depth = embed.shape[0] // 8
    small = 2 * 8

    def tile(at):
        return total[at // 2, (at % 2) * 8 : (at % 2) * 8 + 8, :].astype(jnp.float32)

    for at in range(8 * depth):
        row, col = divmod(at, 8)
        embed[row * 8 : row * 8 + 8, col * LANES : (col + 1) * LANES] = tile(at)
    columns = table.shape[1] - LANES
    for col in range(8):
        values = tile(8 * depth + col)
        cols = slice(col * LANES, (col + 1) * LANES)
        bias[:, cols] = values[0:1]
        gain[:, cols] = values[1:2]
        for i in range(3):
            row = 4 * i + col // 2
            line = values[2 + i : 3 + i]
            if col % 2 == 0:
                table[row : row + 1, :LANES] = line
            else:
                table[row : row + 1, LANES:] = line[:, :columns]
    sums = total[:, small:, :].astype(jnp.float32).sum(axis=0)
    for row in range(out.shape[0] // 2):
        out[2 * row : 2 * row + 1, :] = sums[row : row + 1, :HEAD]
        out[2 * row + 1 : 2 * row + 2, :] = sums[row : row + 1, HEAD:]


def finish(total, depth, table_shape, out_shape):
    f32, width = jnp.float32, 8 * LANES
    shapes = [(depth, width), (1, width), (1, width), table_shape, out_shape]
    return call(
        finish_kernel, STEP,
        [whole(total.shape)], [whole(shape) for shape in shapes],
        [jax.ShapeDtypeStruct(shape, f32) for shape in shapes], [], 1 << 20, 20,
    )(total)


def on_device(
    pixels,
    cotangent,
    embed_weight,
    embed_bias,
    layer_norm_gain,
    qkv_weight,
    out_weight,
    bias_table,
    rel_index,
    shifts,
):
    cotangent, pixels = cotangent[0], pixels[0]
    rows_dev, cols_dev, width = cotangent.shape
    all_heads, table_size = bias_table.shape
    heads = all_heads // 4
    grid_rows = rows_dev * lax.axis_size(ROW)
    grid_cols = cols_dev * lax.axis_size("col")
    row_shift, col_shift = shifts[0, 0], shifts[0, 1]
    row_at, col_at, core = lax.axis_index(ROW), lax.axis_index("col"), lax.axis_index("core")
    group = 2 * (lax.axis_index("x") % 2) + core

    depth = embed_weight.shape[0]
    patches = make_patches(pixels)
    patches = jnp.pad(patches, ((0, 0), (0, 0), (0, LANES - depth)))
    block = jnp.concatenate([cotangent, patches], axis=-1)
    beside = from_behind(block[:, :WIN], "col")
    block = splice_after(block, beside, col_shift, 1)
    below = from_behind(block[: WIN - 1], ROW)
    own = window_split(splice_after(block, below, row_shift, 0))
    arrived = gather_weights(qkv_weight, out_weight)
    beside = swap(own, "x")
    two = jnp.concatenate([own, beside])
    other = swap(two, "core")
    cells = 2 * two.shape[0]

    labels = []
    for row_flip in (0, 2, 1, 3):
        row_ids = (row_at ^ row_flip) * rows_dev + jnp.arange(rows_dev, dtype=jnp.int32)
        col_ids = col_at * cols_dev + jnp.arange(cols_dev, dtype=jnp.int32)
        row_part = (row_ids >= grid_rows - row_shift).astype(jnp.int32)
        col_part = (col_ids >= grid_cols - col_shift).astype(jnp.int32)
        region = 2 * row_part[:, None] + col_part[None, :]
        labels.append(window_split(region[:, :, None])[:, 0])
    label = jnp.concatenate(labels) + 4 * (jnp.arange(cells, dtype=jnp.int32) // CELLS)
    label = label.astype(jnp.float32).reshape(-1, PAIR)
    selector = (
        rel_index.reshape(-1)[:, None] == jnp.arange(table_size, dtype=jnp.int32)[None, :]
    ).astype(jnp.float32)
    my_table = lax.dynamic_slice_in_dim(bias_table, group * heads, heads, 0)
    bias = jnp.dot(selector, my_table.T, precision=lax.Precision.HIGHEST).T
    bias = bias.reshape(heads, CELLS, CELLS)
    embed_w = jnp.pad(embed_weight, ((0, LANES - depth), (0, 0)))
    gain = layer_norm_gain[None]

    normed, xhat, inv = run_tokens(two, other, embed_w, embed_bias[None], gain)
    dproj, table_part, out_grad, weights = run_attention(
        two, other, normed, arrived, bias, label
    )
    count = lax.axis_size(CHIP_ROW)
    held = exchange(out_grad.reshape(count, -1, width), CHIP_ROW)
    my_grad = jnp.dot(table_part, selector, precision=lax.Precision.HIGH)
    wide = 256
    rows = jnp.zeros((16 * width // wide, wide), jnp.float32)
    first_row = 2 * width // wide + group * heads
    table = lax.dynamic_update_slice(rows, my_grad, (first_row, 0)).reshape(16, width)
    line = run_norm(two, other, dproj, xhat, inv, gain, weights, table)
    line, held = lax.optimization_barrier((line, held))
    chunks = lax.axis_size(ROW)
    tall = line.shape[0]
    tiles = line.reshape(tall // 8, 8, width // LANES, LANES).transpose(0, 2, 1, 3)
    tiles = tiles.reshape(chunks, -1, LANES)
    mine = exchange(tiles, ROW)
    bands = held.reshape(2, count // 2, -1, width).astype(jnp.float32).sum(axis=0)
    groups, rows_o, _ = bands.shape
    spans = lax.axis_size(COL)
    bands = bands.astype(jnp.bfloat16).reshape(groups, rows_o, spans, -1).transpose(2, 0, 1, 3)
    bands = bands.reshape(spans, -1, LANES)
    mine = mine.astype(jnp.float32).sum(axis=0).astype(jnp.bfloat16)
    depth_s = mine.shape[0]
    mine = jnp.broadcast_to(mine[None], (spans, depth_s, LANES))
    both = exchange(jnp.concatenate([mine, bands], axis=1), COL)
    both = both.astype(jnp.float32).sum(axis=0).astype(jnp.bfloat16)
    mine = jnp.broadcast_to(both[None, :depth_s], (chunks, depth_s, LANES))
    bands = both[depth_s:].reshape(groups, 1, -1, LANES)
    here = jnp.arange(count, dtype=jnp.int32)[None, :, None, None] == lax.axis_index(CHIP_ROW)
    bands = jnp.where(here, bands, jnp.zeros_like(bands)).reshape(chunks, -1, LANES)
    total = exchange(jnp.concatenate([mine, bands], axis=1), ROW)
    embed_grad, bias_grad, gain_grad, table_grad, out_weight_grad = finish(
        total, depth, bias_table.shape, out_weight.shape
    )
    return (out_weight_grad, embed_grad, bias_grad[0], gain_grad[0], table_grad)


def solution(mesh):
    sizes = mesh.devices.shape
    names = ("yl", "x", "core", "col", "dp")
    fine = Mesh(mesh.devices.reshape(-1, 4, 2, *sizes[1:]), names)
    return jax.shard_map(
        on_device,
        mesh=fine,
        in_specs=(
            P("dp", None, ROW, "col"),
            P("dp", ROW, "col", None),
            P(),
            P(),
            P(),
            P(ROW, COL),
            P(ROW, COL),
            P(),
            P(),
            P("dp", None),
        ),
        out_specs=(P(ROW, COL), P(), P(), P(), P()),
        check_vma=False,
    )
```
